32 devices in a mesh: gx: 16 (over z, y, x), gy: 2 (over core).
Axes of the slice: x: 2, y: 2, z: 4, core: 2. Of those that a mesh axis runs over, the one named last changes fastest.
Arguments:
- fields: bfloat16 [4, 1, 3072, 3072], P(None, None, 'gx', 'gy'), may hold values from -6 to 6
- x_codes: int32 [1024], replicated, may hold values from 0 to 1024, as said below
- y_codes: int32 [1020], replicated, may hold values from 0 to 1024, as said below
Outputs:
- spectrum: float32 [4, 1, 1024, 1020], P(None, None, 'gx', 'gy')
- lowpass: float32 [4, 1, 3072, 3072], P(None, None, 'gx', 'gy')
The draws below stay inside these ranges and needn't reach their ends.
Inputs may be any that keep to these rules, and one draw needn't show every extreme that they name: `x_codes`: distinct codes in rising order, each naming one real Fourier basis function with wavenumber at most 512. `y_codes`: distinct codes in rising order, each naming one real Fourier basis function with wavenumber at most 512.
All inputs are finite; a program needn't handle non-finite values.
Results may differ from the reference program's by a relative error of at most 0.006.
Values may be sent and summed in bfloat16 or wider, within the bound.
A program may use at most 64 MiB of HBM per device.

```python
import math
import jax
import jax.numpy as jnp
from jax import lax

FIELDS = 4
NX = 3072
NY = 3072
BAND = 512
KX = 1024
KY = 1020
ZW = 1


def draw_x_codes(key, part):
    shuffled = jax.random.permutation(jax.random.fold_in(key, 11), 2 * BAND + 1)
    return jnp.sort(shuffled[:KX]).astype(jnp.int32)


def draw_y_codes(key, part):
    shuffled = jax.random.permutation(jax.random.fold_in(key, 23), 2 * BAND + 1)
    return jnp.sort(shuffled[:KY]).astype(jnp.int32)


def block_scale(own_key, dims, shards, least, top_value):
    def one(dim, parts):
        heights = jax.random.uniform(jax.random.fold_in(jax.random.fold_in(own_key, 6), dim), (parts,), jnp.float32, least / len(shards), top_value / len(shards))
        return jnp.repeat(jnp.exp(heights), dims[dim] // parts).reshape((-1,) + (1,) * (len(dims) - dim - 1))

    level = one(*shards[0])
    for cut in shards[1:]:
        level = level * one(*cut)
    return level


def scatter_about(key, shape, scale, reach, split=(), kind=jnp.bfloat16):
    values = scale * jax.random.normal(key, shape, jnp.float32)
    if split:
        values = values * block_scale(key, shape, split, -0.22, 0.18)
    return jnp.clip(values, -reach, reach).astype(kind)


def setup_inputs(seed: int = 0) -> dict:
    key_of = jax.random.split(jax.random.key(seed), 4)
    fields = scatter_about(key_of[0], (FIELDS, ZW, NX, NY), 1.0, 6.0, ((2, 16), (3, 2)))
    x_codes = draw_x_codes(jax.random.fold_in(key_of[3], 71), 0)
    y_codes = draw_y_codes(jax.random.fold_in(key_of[3], 71), 0)
    return {"fields": fields, "x_codes": x_codes, "y_codes": y_codes}


def mode_table(picked, length):
    position = jnp.arange(length, dtype=jnp.int32)
    frequency = jnp.where(picked <= BAND, picked, picked - BAND).astype(jnp.int32)
    phase_index = frequency[:, None] * position[None, :] % length
    radians = phase_index.astype(jnp.float32) * (2.0 * math.pi / length)
    values = jnp.where(picked[:, None] <= BAND, jnp.cos(radians), jnp.sin(radians))
    norm_factor = jnp.where(picked == 0, 1.0 / math.sqrt(length), math.sqrt(2.0 / length)).astype(jnp.float32)
    return (values * norm_factor[:, None]).astype(jnp.bfloat16)

def reference(fields, x_codes, y_codes):
    highest = lax.Precision.HIGHEST
    x_table = mode_table(x_codes, NX).astype(jnp.float32)
    y_table = mode_table(y_codes, NY).astype(jnp.float32)
    partial_value = jnp.einsum('fzxy,ky->fzxk', fields.astype(jnp.float32), y_table, precision=highest)
    spectrum = jnp.einsum('jx,fzxk->fzjk', x_table, partial_value, precision=highest)
    coarse = spectrum.astype(jnp.bfloat16).astype(jnp.float32)
    synth_x = jnp.einsum('jx,fzjk->fzxk', x_table, coarse, precision=highest)
    lowpass = jnp.einsum('fzxk,ky->fzxy', synth_x, y_table, precision=highest)
    return (spectrum, lowpass)
```

```python
import functools
import math

import jax
import jax.numpy as jnp
from jax import lax
from jax.experimental import pallas as pl
from jax.experimental.pallas import tpu as pltpu
from jax.sharding import PartitionSpec as P

NX = 3072
NY = 3072
BAND = 512
STEP = 64


def angle(freq, position, length):
    phase = freq[None, :] * position[:, None] % length
    return phase.astype(jnp.float32) * (2.0 * math.pi / length)


def mode_parts(picked, first, amount, length, live=None):
    step = 64 if amount % 64 == 0 else 8
    freq = jnp.where(picked <= BAND, picked, picked - BAND)
    coarse_angle = angle(freq, first + step * jnp.arange(amount // step, dtype=jnp.int32), length)
    fine_angle = angle(freq, jnp.arange(step, dtype=jnp.int32), length)
    norm = jnp.where(picked == 0, 1.0 / math.sqrt(length), math.sqrt(2.0 / length)).astype(jnp.float32)
    if live is not None:
        norm = jnp.where(live, norm, 0.0)
    is_cos = (picked <= BAND)[None, :]
    c, s = jnp.cos(coarse_angle), jnp.sin(coarse_angle)
    first_part = jnp.where(is_cos, c, s) * norm[None, :]
    second_part = jnp.where(is_cos, -s, c) * norm[None, :]
    fc, fs = jnp.cos(fine_angle), jnp.sin(fine_angle)
    return lax.optimization_barrier((first_part, second_part, fc, fs))


def mode_table(picked, first, amount, length, live=None):
    first_part, second_part, fc, fs = mode_parts(picked, first, amount, length, live)
    table = first_part[:, None, :] * fc[None] + second_part[:, None, :] * fs[None]
    return table.astype(jnp.bfloat16).reshape(amount, picked.shape[0])


def al(v, m):
    return pl.multiple_of(v, m)


def turn(freq, position, shift, length):
    product = freq * position
    quarter = jnp.floor(product * (4.0 / length) + 0.5)
    x = (product * 4.0 - quarter * length) * (2.0 * math.pi / (4 * length))
    x2 = x * x
    s = x + x * x2 * (-1 / 6 + x2 * (1 / 120 + x2 * (-1 / 5040 + x2 * (1 / 362880))))
    c = 1.0 + x2 * (-0.5 + x2 * (1 / 24 + x2 * (-1 / 720 + x2 * (1 / 40320))))
    quarter = quarter - shift
    q = quarter - 4.0 * jnp.floor(quarter * 0.25)
    odd = (q == 1.0) | (q == 3.0)
    cos_value, sin_value = jnp.where(odd, s, c), jnp.where(odd, c, s)
    cos_value = jnp.where((q == 1.0) | (q == 2.0), -cos_value, cos_value)
    return cos_value, jnp.where(q >= 2.0, -sin_value, sin_value)


LANES = 128


def make_table(code, first, length, table, ta, tb, fc, fs):
    amount, codes = table.shape
    f32 = jnp.float32
    freq = jnp.where(code <= BAND, code, code - BAND).astype(f32)
    shift = jnp.where(code <= BAND, 0, 1).astype(f32)
    norm = jnp.where(code == 0, 1.0 / math.sqrt(length), math.sqrt(2.0 / length)).astype(f32)
    norm = jnp.where(code < 0, 0.0, norm)
    row = lax.broadcasted_iota(jnp.int32, (8, codes), 0)

    @pl.loop(0, amount // STEP // 8)
    def _(i):
        c, s = turn(freq, (first + (row + i * 8) * STEP).astype(f32), shift, length)
        ta[pl.ds(al(i * 8, 8), 8), :] = c * norm
        tb[pl.ds(al(i * 8, 8), 8), :] = s * norm

    @pl.loop(0, STEP // 8)
    def _(i):
        c, s = turn(freq, (row + i * 8).astype(f32), 0.0, length)
        fc[pl.ds(al(i * 8, 8), 8), :] = c
        fs[pl.ds(al(i * 8, 8), 8), :] = s

    @pl.loop(0, amount // STEP)
    def _(h):
        table[pl.ds(al(h * STEP, STEP), STEP), :] = (
            ta[pl.ds(h, 1), :] * fc[...] - tb[pl.ds(h, 1), :] * fs[...]
        ).astype(jnp.bfloat16)


def filter_kernel(
    lead, x_local, kx, ky, kpad,
    grid_in, code_in, spec_ref, low_ref,
    grid_ref, code_ref, y_raw, y_codes, y_ref, yta, ytb, yfc, yfs, own, other, inc, part, lines, turned, xt, xta, xtb, xfc, xfs,
    s_own, s_out, s_in, coarse, blocks, wide,
    gs, gr, s1, r1, s2, r2, s3, r3, s4, r4, in_sem,
):
    me = lax.axis_index("gx")
    half = lax.axis_index("gy")
    peer = 1 - half
    bf, f32 = jnp.bfloat16, jnp.float32
    scope = jax.named_scope
    chunks = kpad // LANES
    members = 2 * lead
    modes = xt.shape[1]
    pieces = r2.shape[0] // chunks
    piece = modes // pieces
    rows = lead * x_local
    block = x_local + kx
    plane, spot = me // lead, lax.rem(me, lead)
    side = plane // 2
    base = side * members
    mine = me - base
    hub_in, end_in = 1 - side, side
    hub_base = base + hub_in * lead
    is_hub = plane == 1 + side
    across = (2 - side) * lead + spot

    grid_copy = pltpu.make_async_copy(grid_in, grid_ref, in_sem.at[0])
    code_copy = pltpu.make_async_copy(code_in, code_ref, in_sem.at[1])
    code_copy.start()
    grid_copy.start()
    barrier = pltpu.get_barrier_semaphore()
    pl.semaphore_signal(barrier, inc=1, device_id={"gy": peer})

    @pl.loop(1, members)
    def _(t):
        pl.semaphore_signal(barrier, inc=1, device_id={"gx": base + lax.rem(mine + t, members)})

    @pl.when(is_hub)
    def _():
        pl.semaphore_signal(barrier, inc=1, device_id={"gx": across})

    def span(i, n):
        return pl.ds(al(i * n, n), n)

    def swap(k):
        return pltpu.make_async_remote_copy(
            src_ref=other.at[k], dst_ref=inc.at[k], send_sem=gs, recv_sem=gr.at[k], device_id={"gy": peer})

    def up(k, f):
        return pltpu.make_async_remote_copy(
            src_ref=part.at[k, span(f, x_local), :], dst_ref=lines.at[k, span(mine, x_local), :],
            send_sem=s1, recv_sem=r1.at[k], device_id={"gx": hub_base + f})

    def up_in(k):
        taken = lines.at[k, pl.ds(0, (members - 1) * x_local), :]
        return pltpu.make_async_remote_copy(
            src_ref=taken, dst_ref=taken, send_sem=s1, recv_sem=r1.at[k], device_id={"gx": hub_base})

    def sent(view, sem):
        pltpu.make_async_remote_copy(
            src_ref=view, dst_ref=view, send_sem=sem, recv_sem=gr.at[0], device_id={"gy": peer}).wait_send()

    def cross(k, m):
        return pltpu.make_async_remote_copy(
            src_ref=s_out.at[k, span(m, piece), :], dst_ref=s_in.at[k, span(m, piece), :],
            send_sem=s2, recv_sem=r2.at[k * pieces + m], device_id={"gx": across})

    def down(k, b):
        return pltpu.make_async_remote_copy(
            src_ref=blocks.at[k, b], dst_ref=wide.at[k, spot, :, span(half, LANES)],
            send_sem=s3, recv_sem=r3.at[k * lead + spot], device_id={"gx": base + b})

    def down_in(k, f):
        return pltpu.make_async_remote_copy(
            src_ref=blocks.at[k, 0], dst_ref=wide.at[k, f, :, span(half, LANES)],
            send_sem=s3, recv_sem=r3.at[k * lead + f], device_id={"gx": hub_base + f})

    def forward(k, f, who):
        place = wide.at[k, f, pl.ds(0, x_local), span(who, LANES)]
        return pltpu.make_async_remote_copy(
            src_ref=place, dst_ref=place, send_sem=s4, recv_sem=r4.at[k * lead + f],
            device_id={"gy": peer})

    def local(f):
        return is_hub & (f == spot)

    width = chunks * LANES * 2
    y_raw[...] = jnp.full(y_raw.shape, -1, jnp.int32)
    with scope("codewait"):
        code_copy.wait()
    y_raw[:, : 2 * ky] = code_ref[:, modes:]
    first_half = jnp.broadcast_to(y_raw[...], (8, width))
    second_half = pltpu.roll(first_half, width - ky, 1)
    live = lax.broadcasted_iota(jnp.int32, (8, width), 1) < ky
    first_half = jnp.where(live, first_half, -1)
    second_half = jnp.where(live, second_half, -1)
    for k in range(chunks):
        y_codes[k, :, :LANES] = first_half[:, k * LANES : (k + 1) * LANES]
        y_codes[k, :, LANES:] = second_half[:, k * LANES : (k + 1) * LANES]

    def y_table(k):
        with scope("ytab"):
            make_table(y_codes[k, :1, :], half * y_ref.shape[1], NY, y_ref.at[k], yta, ytb, yfc, yfs)

    def sums(k):
        if k == 0:
            with scope("gridwait"):
                grid_copy.wait()
        with scope("dotA"):
            both = jnp.dot(grid_ref[...], y_ref[k], preferred_element_type=f32)
            low_part, high_part = both[:, :LANES], both[:, LANES:]
            other[k] = jnp.where(half == 0, high_part, low_part).astype(bf)
            own[k] = jnp.where(half == 0, low_part, high_part)
        if k == 0:
            with scope("barrier"):
                pl.semaphore_wait(barrier, members + jnp.where(is_hub, 1, 0))
        swap(k).start()

    def rise(k):
        with scope("swapwait"):
            swap(k).wait_recv()
        part[k] = (own[k] + inc[k].astype(f32)).astype(bf)

        @pl.loop(0, lead)
        def _(t):
            f = lax.rem(spot + t, lead)

            @pl.when(jnp.logical_not(local(f)))
            def _():
                up(k, f).start()

        @pl.when(is_hub)
        def _():
            lines[k, span(mine, x_local), :] = part[k, span(spot, x_local), :]

    def partial_sum(k):
        with scope("upwait"):
            up_in(k).wait_recv()

        with scope("dotB"):
            turned[...] = lines[k].T

            @pl.loop(0, pieces)
            def _(m):
                got = jnp.dot(turned[...], xt[:, span(m, piece)], preferred_element_type=f32).T
                s_own[k, span(m, piece), :] = got
                s_out[k, span(m, piece), :] = got.astype(bf)
                cross(k, m).start()

    def whole_sum(k):
        @pl.loop(0, pieces)
        def _(m):
            with scope("crosswait"):
                cross(k, m).wait_recv()
            coarse[k, span(m, piece), :] = (
                s_own[k, span(m, piece), :] + s_in[k, span(m, piece), :].astype(f32)
            ).astype(bf)

        for place in (end_in, hub_in):
            with scope("dotC"):
                syn = jnp.dot(xt[span(place, rows), :], coarse[k], preferred_element_type=f32).astype(bf)
                blocks[k, span(place, lead), :x_local, :] = syn.reshape(lead, x_local, LANES)
                blocks[k, span(place, lead), x_local:, :] = coarse[
                    k, span(base // lead + place, lead * kx), :
                ].reshape(lead, kx, LANES)

            @pl.loop(1, lead + 1)
            def _(t):
                b = place * lead + lax.rem(spot + t, lead)

                @pl.when(b != mine)
                def _():
                    down(k, b).start()

        wide[k, spot, :, span(half, LANES)] = blocks[k, mine]

    def take(k):
        @pl.loop(1, lead + 1)
        def _(t):
            f = lax.rem(spot + lead - lax.rem(t, lead), lead)

            @pl.when(jnp.logical_not(local(f)))
            def _():
                with scope("downwait"):
                    down_in(k, f).wait_recv()

            forward(k, f, half).start()
            found = wide[k, f, pl.ds(x_local, kx), span(half, LANES)].astype(f32)
            spec_ref[span(f, kx), pl.ds(k * LANES, min(LANES, ky - k * LANES))] = found[:, : ky - k * LANES]

    def expand(k):
        @pl.loop(1, lead + 1)
        def _(t):
            f = lax.rem(spot + lead - lax.rem(t, lead), lead)
            with scope("fwdwait"):
                forward(k, f, peer).wait_recv()
            with scope("dotD"):
                got = lax.dot_general(
                    wide[k, f, :x_local, :], y_ref[k], (((1,), (1,)), ((), ())), preferred_element_type=f32)
                if k > 0:
                    got = got + low_ref[span(f, x_local), :]
                low_ref[span(f, x_local), :] = got

    y_table(0)
    sums(0)
    y_table(1)

    @pl.when(half == 0)
    def _():
        rise(0)

    sums(1)

    @pl.when(half == 1)
    def _():
        rise(0)

    if chunks > 2:
        y_table(2)
    rise(1)

    def late_sums(k):
        sums(k)
        if k + 1 < chunks:
            y_table(k + 1)
        rise(k)

    @pl.when(is_hub)
    def _():
        with scope("xtab"):
            make_table(code_ref[:, :modes], side * xt.shape[0], NX, xt, xta, xtb, xfc, xfs)
        for k in range(chunks):
            partial_sum(k)
            if k + 2 < chunks:
                late_sums(k + 2)
            if 0 < k < chunks - 1:
                whole_sum(k - 1)
        take(0)
        expand(0)
        for k in range(max(chunks - 2, 0), chunks):
            whole_sum(k)
        for k in range(1, chunks):
            take(k)
            expand(k)

    @pl.when(jnp.logical_not(is_hub))
    def _():
        for k in range(2, chunks):
            late_sums(k)
        for k in range(chunks):
            take(k)
            expand(k)

    with scope("drain"):
        sent(other, gs)
        sent(wide.at[:, :, pl.ds(0, x_local), pl.ds(0, LANES)], s4)

        @pl.when(is_hub)
        def _():
            sent(part.at[:, pl.ds(0, rows - x_local), :], s1)
            sent(s_out, s2)
            sent(blocks.at[:, pl.ds(0, members - 1)], s3)

        @pl.when(jnp.logical_not(is_hub))
        def _():
            sent(part, s1)


def spectral_filter(lead, x_local, kx, ky, kpad, grid, codes):
    bf, f32 = jnp.bfloat16, jnp.float32
    y_local = grid.shape[1]
    rows, members, modes = lead * x_local, 2 * lead, codes.shape[1] - 2 * ky
    chunks, pieces = kpad // LANES, 4
    tall_x, tall_y = members * x_local // STEP, y_local // STEP
    block = x_local + kx
    dma = pltpu.SemaphoreType.DMA
    vmem = pl.BlockSpec(memory_space=pltpu.VMEM)
    return pl.pallas_call(
        functools.partial(filter_kernel, lead, x_local, kx, ky, kpad),
        out_shape=(
            jax.ShapeDtypeStruct((lead * kx, ky), f32),
            jax.ShapeDtypeStruct((rows, y_local), f32),
        ),
        in_specs=[pl.BlockSpec(memory_space=pl.ANY)] * 2,
        out_specs=(vmem, vmem),
        scratch_shapes=[
            pltpu.VMEM((rows, y_local), bf),
            pltpu.VMEM(codes.shape, jnp.int32),
            pltpu.VMEM((1, 2 * kpad), jnp.int32),
            pltpu.VMEM((chunks, 8, 2 * LANES), jnp.int32),
            pltpu.VMEM((chunks, y_local, 2 * LANES), bf),
            pltpu.VMEM((tall_y, 2 * LANES), f32),
            pltpu.VMEM((tall_y, 2 * LANES), f32),
            pltpu.VMEM((STEP, 2 * LANES), f32),
            pltpu.VMEM((STEP, 2 * LANES), f32),
            pltpu.VMEM((chunks, rows, LANES), f32),
            pltpu.VMEM((chunks, rows, LANES), bf),
            pltpu.VMEM((chunks, rows, LANES), bf),
            pltpu.VMEM((chunks, rows, LANES), bf),
            pltpu.VMEM((chunks, members * x_local, LANES), bf),
            pltpu.VMEM((LANES, members * x_local), bf),
            pltpu.VMEM((members * x_local, modes), bf),
            pltpu.VMEM((tall_x, modes), f32),
            pltpu.VMEM((tall_x, modes), f32),
            pltpu.VMEM((STEP, modes), f32),
            pltpu.VMEM((STEP, modes), f32),
            pltpu.VMEM((chunks, modes, LANES), f32),
            pltpu.VMEM((chunks, modes, LANES), bf),
            pltpu.VMEM((chunks, modes, LANES), bf),
            pltpu.VMEM((chunks, modes, LANES), bf),
            pltpu.VMEM((chunks, members, block, LANES), bf),
            pltpu.VMEM((chunks, lead, block, 2 * LANES), bf),
            dma, dma((chunks,)),
            dma, dma((chunks,)),
            dma, dma((chunks * pieces,)),
            dma, dma((chunks * lead,)),
            dma, dma((chunks * lead,)),
            dma((2,)),
        ],
        compiler_params=pltpu.CompilerParams(
            collective_id=0, has_side_effects=True, vmem_limit_bytes=46 * 1024 * 1024
        ),
    )(grid, codes)


def build(gx, gy):
    def local(fields, x_codes, y_codes):
        nf, nz, x_local, y_local = fields.shape
        lead = nf * nz
        ky = y_codes.shape[0] // gy
        kx = x_codes.shape[0] // gx
        unit = 128 * gx // math.gcd(128 * gx, lead)
        if unit > 2 * ky:
            unit = gx // math.gcd(gx, lead)
        kpad = -(-ky // unit) * unit
        cols = lead * kpad // gx
        me_y = lax.axis_index("gy")
        y_first = me_y * y_local
        grid = fields.reshape(lead * x_local, y_local)
        fits = gy == 2 and gx == 4 * lead and kpad % LANES == 0 and kpad >= 4 * LANES and kx % 16 == 0
        fits = fits and x_local % 16 == 0 and 2 * lead * x_local % (8 * STEP) == 0
        fits = fits and y_local % (8 * STEP) == 0 and gx * kx % (4 * LANES) == 0
        if fits:
            spec, low = spectral_filter(
                lead, x_local, kx, ky, kpad, grid, jnp.concatenate([x_codes, y_codes]).reshape(1, -1))
            return spec.reshape(nf, nz, kx, ky), low.reshape(nf, nz, x_local, y_local)
        padded = jnp.pad(y_codes.reshape(gy, ky), ((0, 0), (0, kpad - ky)))
        live = jnp.broadcast_to(jnp.arange(kpad)[None] < ky, (gy, kpad)).reshape(-1)
        x_tab = mode_table(x_codes, 0, x_local * gx, NX)
        y_tab = mode_table(padded.reshape(-1), y_first, y_local, NY, live)
        part = jnp.dot(grid, y_tab, preferred_element_type=jnp.float32).reshape(lead * x_local, gy, kpad)
        own = lax.dynamic_index_in_dim(part, me_y, 1, keepdims=False)
        for shift in range(1, gy):
            there = lax.rem(me_y + shift, gy)
            block = lax.dynamic_index_in_dim(part, there, 1, keepdims=False).astype(jnp.bfloat16)
            got = lax.ppermute(block, "gy", [(i, (i + shift) % gy) for i in range(gy)])
            own = own + got.astype(jnp.float32)
        send = own.astype(jnp.bfloat16).reshape(lead, x_local, kpad)
        if cols <= kpad:
            def spread(a):
                n = a.shape[1]
                return a.reshape(lead, n, kpad // cols, cols).transpose(0, 2, 1, 3).reshape(gx, n, cols)

            def merge(a):
                n = a.shape[1]
                return a.reshape(lead, kpad // cols, n, cols).transpose(0, 2, 1, 3).reshape(lead, n, kpad)
        else:
            def spread(a):
                n = a.shape[1]
                return a.transpose(1, 0, 2).reshape(n, gx, cols).transpose(1, 0, 2)

            def merge(a):
                n = a.shape[1]
                return a.transpose(1, 0, 2).reshape(n, lead, kpad).transpose(1, 0, 2)
        lines = lax.all_to_all(spread(send), "gx", split_axis=0, concat_axis=0, tiled=True)
        lines = lines.reshape(gx * x_local, cols)
        modes = lax.dot_general(x_tab, lines, (((0,), (0,)), ((), ())), preferred_element_type=jnp.float32)
        coarse = modes.astype(jnp.bfloat16)
        synth = jnp.dot(x_tab, coarse, preferred_element_type=jnp.float32).astype(jnp.bfloat16)
        back = lax.all_to_all(synth.reshape(gx, x_local, cols), "gx", split_axis=0, concat_axis=0, tiled=True)
        spec = lax.all_to_all(coarse.reshape(gx, kx, cols), "gx", split_axis=0, concat_axis=0, tiled=True)
        spectrum = merge(spec)[:, :, :ky].astype(jnp.float32).reshape(nf, nz, kx, ky)
        mine = merge(back).reshape(lead * x_local, kpad)
        y_parts = y_tab.reshape(y_local, gy, kpad)
        whole = jnp.zeros((gy, lead * x_local, kpad), jnp.bfloat16)
        whole = lax.dynamic_update_index_in_dim(whole, mine, me_y, 0)
        for shift in range(1, gy):
            got = lax.ppermute(mine, "gy", [(i, (i + shift) % gy) for i in range(gy)])
            whole = lax.dynamic_update_index_in_dim(whole, got, lax.rem(me_y + gy - shift, gy), 0)
        wide = whole.transpose(1, 0, 2).reshape(lead * x_local, gy * kpad)
        low = lax.dot_general(wide, y_tab, (((1,), (1,)), ((), ())), preferred_element_type=jnp.float32)
        return spectrum, low.reshape(nf, nz, x_local, y_local)

    return local


def solution(mesh):
    return jax.shard_map(
        build(mesh.shape["gx"], mesh.shape["gy"]),
        mesh=mesh,
        in_specs=(P(None, None, "gx", "gy"), P(), P()),
        out_specs=(P(None, None, "gx", "gy"), P(None, None, "gx", "gy")),
        check_vma=False,
    )
```

```python
import functools
import math

import jax
import jax.numpy as jnp
from jax import lax
from jax.experimental import pallas as pl
from jax.experimental.pallas import tpu as pltpu
from jax.sharding import PartitionSpec as P

NX = 3072
NY = 3072
BAND = 512
STEP = 64


def angle(freq, position, length):
    phase = freq[None, :] * position[:, None] % length
    return phase.astype(jnp.float32) * (2.0 * math.pi / length)


def mode_parts(picked, first, amount, length, live=None):
    step = 64 if amount % 64 == 0 else 8
    freq = jnp.where(picked <= BAND, picked, picked - BAND)
    coarse_angle = angle(freq, first + step * jnp.arange(amount // step, dtype=jnp.int32), length)
    fine_angle = angle(freq, jnp.arange(step, dtype=jnp.int32), length)
    norm = jnp.where(picked == 0, 1.0 / math.sqrt(length), math.sqrt(2.0 / length)).astype(jnp.float32)
    if live is not None:
        norm = jnp.where(live, norm, 0.0)
    is_cos = (picked <= BAND)[None, :]
    c, s = jnp.cos(coarse_angle), jnp.sin(coarse_angle)
    first_part = jnp.where(is_cos, c, s) * norm[None, :]
    second_part = jnp.where(is_cos, -s, c) * norm[None, :]
    fc, fs = jnp.cos(fine_angle), jnp.sin(fine_angle)
    return lax.optimization_barrier((first_part, second_part, fc, fs))


def mode_table(picked, first, amount, length, live=None):
    first_part, second_part, fc, fs = mode_parts(picked, first, amount, length, live)
    table = first_part[:, None, :] * fc[None] + second_part[:, None, :] * fs[None]
    return table.astype(jnp.bfloat16).reshape(amount, picked.shape[0])


def al(v, m):
    return pl.multiple_of(v, m)


def turn(freq, position, shift, length):
    product = freq * position
    quarter = jnp.floor(product * (4.0 / length) + 0.5)
    x = (product * 4.0 - quarter * length) * (2.0 * math.pi / (4 * length))
    x2 = x * x
    s = x + x * x2 * (-1 / 6 + x2 * (1 / 120 + x2 * (-1 / 5040 + x2 * (1 / 362880))))
    c = 1.0 + x2 * (-0.5 + x2 * (1 / 24 + x2 * (-1 / 720 + x2 * (1 / 40320))))
    quarter = quarter - shift
    q = quarter - 4.0 * jnp.floor(quarter * 0.25)
    odd = (q == 1.0) | (q == 3.0)
    cos_value, sin_value = jnp.where(odd, s, c), jnp.where(odd, c, s)
    cos_value = jnp.where((q == 1.0) | (q == 2.0), -cos_value, cos_value)
    return cos_value, jnp.where(q >= 2.0, -sin_value, sin_value)


LANES = 128


def make_table(code, first, length, table, ta, tb, fc, fs):
    amount, codes = table.shape
    f32 = jnp.float32
    freq = jnp.where(code <= BAND, code, code - BAND).astype(f32)
    shift = jnp.where(code <= BAND, 0, 1).astype(f32)
    norm = jnp.where(code == 0, 1.0 / math.sqrt(length), math.sqrt(2.0 / length)).astype(f32)
    norm = jnp.where(code < 0, 0.0, norm)
    row = lax.broadcasted_iota(jnp.int32, (8, codes), 0)

    @pl.loop(0, amount // STEP // 8)
    def _(i):
        c, s = turn(freq, (first + (row + i * 8) * STEP).astype(f32), shift, length)
        ta[pl.ds(al(i * 8, 8), 8), :] = c * norm
        tb[pl.ds(al(i * 8, 8), 8), :] = s * norm

    @pl.loop(0, STEP // 8)
    def _(i):
        c, s = turn(freq, (row + i * 8).astype(f32), 0.0, length)
        fc[pl.ds(al(i * 8, 8), 8), :] = c
        fs[pl.ds(al(i * 8, 8), 8), :] = s

    @pl.loop(0, amount // STEP)
    def _(h):
        table[pl.ds(al(h * STEP, STEP), STEP), :] = (
            ta[pl.ds(h, 1), :] * fc[...] - tb[pl.ds(h, 1), :] * fs[...]
        ).astype(jnp.bfloat16)


def flipped(spot, t, lead):
    f = spot
    for bit in range(lead.bit_length()):
        if t >> bit & 1:
            f = f + (1 << bit) - (2 << bit) * lax.rem(f // (1 << bit), 2)
    return f


def near_first(lead):
    return sorted(range(lead - 1, 0, -1), key=lambda t: bin(t).count("1"))


def filter_kernel(
    lead, x_local, kx, ky, kpad,
    grid_in, xcode_in, ycode_in, spec_ref, low_ref, wide_last, y_last,
    grid_ref, xcode_ref, ycode_ref, y_raw, y_codes, y_ref, yta, ytb, yfc, yfs, own, other, inc, part, lines, turned, xt, xta, xtb, xfc, xfs,
    s_own, s_out, s_in, coarse, blocks, wide, found,
    gs, gr, s1, r1, s2, r2, s3, r3, s4, r4, s5, r5, s6, r6, in_sem,
):
    me = lax.axis_index("gx")
    half = lax.axis_index("gy")
    peer = 1 - half
    bf, f32 = jnp.bfloat16, jnp.float32
    scope = jax.named_scope
    chunks = kpad // LANES
    members = 2 * lead
    modes = xt.shape[1]
    pieces = r2.shape[0] // chunks
    piece = modes // pieces
    rows = lead * x_local
    plane, spot = me // lead, lax.rem(me, lead)
    side = plane // 2
    base = side * members
    mine = me - base
    hub_base = base + (1 - side) * lead
    end_base = base + side * lead
    own_base = plane * lead
    is_hub = plane == 1 + side
    across = (2 - side) * lead + spot

    grid_copy = pltpu.make_async_copy(grid_in, grid_ref, in_sem.at[0])
    ycode_copy = pltpu.make_async_copy(ycode_in, ycode_ref, in_sem.at[1])
    xcode_copy = pltpu.make_async_copy(xcode_in, xcode_ref, in_sem.at[2])
    ycode_copy.start()
    grid_copy.start()
    xcode_copy.start()
    barrier = pltpu.get_barrier_semaphore()
    pl.semaphore_signal(barrier, inc=1, device_id={"gy": peer})

    @pl.loop(1, members)
    def _(t):
        pl.semaphore_signal(barrier, inc=1, device_id={"gx": base + lax.rem(mine + t, members)})

    @pl.when(is_hub)
    def _():
        pl.semaphore_signal(barrier, inc=1, device_id={"gx": across})

    def mate(t):
        return flipped(spot, t, lead)

    far_first = near_first(lead)[::-1]

    def wide_at(k):
        return wide_last if k == chunks - 1 else wide.at[k]

    def y_at(k):
        return y_last if k == chunks - 1 else y_ref.at[k]

    def span(i, n):
        return pl.ds(al(i * n, n), n)

    def swap(k):
        return pltpu.make_async_remote_copy(
            src_ref=other.at[k], dst_ref=inc.at[k], send_sem=gs, recv_sem=gr.at[k], device_id={"gy": peer})

    def up(k, f):
        return pltpu.make_async_remote_copy(
            src_ref=part.at[k, span(f, x_local), :], dst_ref=lines.at[k, span(mine, x_local), :],
            send_sem=s1, recv_sem=r1.at[k], device_id={"gx": hub_base + f})

    def up_in(k):
        taken = lines.at[k, pl.ds(0, (members - 1) * x_local), :]
        return pltpu.make_async_remote_copy(
            src_ref=taken, dst_ref=taken, send_sem=s1, recv_sem=r1.at[k], device_id={"gx": hub_base})

    def sent(view, sem):
        pltpu.make_async_remote_copy(
            src_ref=view, dst_ref=view, send_sem=sem, recv_sem=gr.at[0], device_id={"gy": peer}).wait_send()

    def cross(k, m):
        return pltpu.make_async_remote_copy(
            src_ref=s_out.at[k, span(m, piece), :], dst_ref=s_in.at[k, span(m, piece), :],
            send_sem=s2, recv_sem=r2.at[k * pieces + m], device_id={"gx": across})

    def relay(k, m):
        view = coarse.at[k, span(m, piece), :]
        return pltpu.make_async_remote_copy(
            src_ref=view, dst_ref=view, send_sem=s5, recv_sem=r5.at[k * pieces + m],
            device_id={"gx": end_base + spot})

    def down(k, f):
        return pltpu.make_async_remote_copy(
            src_ref=blocks.at[k, f], dst_ref=wide_at(k).at[spot, :, span(half, LANES)],
            send_sem=s3, recv_sem=r3.at[k * lead + spot], device_id={"gx": own_base + f})

    def show(k, f):
        return pltpu.make_async_remote_copy(
            src_ref=coarse.at[k, span(own_base + f, kx), :], dst_ref=found.at[k, spot],
            send_sem=s6, recv_sem=r6.at[k], device_id={"gx": own_base + f})

    def show_in(k):
        view = found.at[k, pl.ds(0, lead - 1)]
        return pltpu.make_async_remote_copy(
            src_ref=view, dst_ref=view, send_sem=s6, recv_sem=r6.at[k], device_id={"gx": own_base})

    def down_in(k, f):
        return pltpu.make_async_remote_copy(
            src_ref=blocks.at[k, 0], dst_ref=wide_at(k).at[f, :, span(half, LANES)],
            send_sem=s3, recv_sem=r3.at[k * lead + f], device_id={"gx": own_base + f})

    def forward(k, f, who):
        place = wide_at(k).at[f, :, span(who, LANES)]
        return pltpu.make_async_remote_copy(
            src_ref=place, dst_ref=place, send_sem=s4, recv_sem=r4.at[k * lead + f],
            device_id={"gy": peer})

    def local(f):
        return is_hub & (f == spot)

    width = chunks * LANES * 2
    y_raw[...] = jnp.full(y_raw.shape, -1, jnp.int32)
    with scope("codewait"):
        ycode_copy.wait()
    y_raw[:, : 2 * ky] = ycode_ref[...]
    first_half = jnp.broadcast_to(y_raw[...], (8, width))
    second_half = pltpu.roll(first_half, width - ky, 1)
    live = lax.broadcasted_iota(jnp.int32, (8, width), 1) < ky
    first_half = jnp.where(live, first_half, -1)
    second_half = jnp.where(live, second_half, -1)
    for k in range(chunks):
        y_codes[k, :, :LANES] = first_half[:, k * LANES : (k + 1) * LANES]
        y_codes[k, :, LANES:] = second_half[:, k * LANES : (k + 1) * LANES]

    def y_table(k):
        with scope("ytab"):
            make_table(y_codes[k, :1, :], half * grid_ref.shape[1], NY, y_at(k), yta, ytb, yfc, yfs)

    def sums(k):
        if k == 0:
            with scope("gridwait"):
                grid_copy.wait()
        with scope("dotA"):
            both = jnp.dot(grid_ref[...], y_at(k)[...], preferred_element_type=f32)
            low_part, high_part = both[:, :LANES], both[:, LANES:]
            other[k] = jnp.where(half == 0, high_part, low_part).astype(bf)
            own[k] = jnp.where(half == 0, low_part, high_part)
        if k == 0:
            with scope("barrier"):
                pl.semaphore_wait(barrier, members + jnp.where(is_hub, 1, 0))
        swap(k).start()

    def rise(k):
        with scope("swapwait"):
            swap(k).wait_recv()
        part[k] = (own[k] + inc[k].astype(f32)).astype(bf)

        for t in far_first:
            up(k, mate(t)).start()

        @pl.when(jnp.logical_not(is_hub))
        def _():
            up(k, spot).start()

        @pl.when(is_hub)
        def _():
            lines[k, span(mine, x_local), :] = part[k, span(spot, x_local), :]

    def partial_sum(k, held=1):
        with scope("upwait"):
            up_in(k).wait_recv()

        with scope("dotB"):
            turned[...] = lines[k].T

            @pl.loop(0, pieces)
            def _(m):
                got = jnp.dot(turned[...], xt[:, span(m, piece)], preferred_element_type=f32).T
                s_own[k, span(m, piece), :] = got
                s_out[k, span(m, piece), :] = got.astype(bf)

                @pl.when(half <= held)
                def _():
                    cross(k, m).start()

    mine_x = span(plane - 2 * side, rows)

    def share(k):
        for t in far_first:
            show(k, mate(t)).start()
        found[k, spot] = coarse[k, span(me, kx), :]

    def absorb(k, m):
        if m < pieces - 1:
            @pl.when(plane == m)
            def _():
                share(k)

        if k == chunks - 1:
            with scope("dotC"):
                got = jnp.dot(
                    xt[mine_x, pl.ds(m * piece, piece)], coarse[k, pl.ds(m * piece, piece), :],
                    preferred_element_type=f32)
                own[0] = got if m == 0 else own[0] + got

    def meet(k, m):
        with scope("crosswait"):
            cross(k, m).wait_recv()
        part_of = pl.ds(m * piece, piece)
        coarse[k, part_of, :] = (s_own[k, part_of, :] + s_in[k, part_of, :].astype(f32)).astype(bf)
        relay(k, m).start()
        absorb(k, m)

    def receive(k, m):
        with scope("relaywait"):
            relay(k, m).wait_recv()
        absorb(k, m)

    def synthesis(k):
        if k < chunks - 1:
            with scope("dotC"):
                syn = jnp.dot(xt[mine_x, :], coarse[k], preferred_element_type=f32)
        else:
            syn = own[0]
        blocks[k] = syn.astype(bf).reshape(lead, x_local, LANES)

        for t in far_first:
            down(k, mate(t)).start()

        wide_at(k)[spot, :, span(half, LANES)] = blocks[k, spot]

        @pl.when(plane == pieces - 1)
        def _():
            share(k)

    def pass_on(k, f):
        @pl.when(f != spot)
        def _():
            with scope("downwait"):
                down_in(k, f).wait_recv()

        forward(k, f, half).start()

    def reveal(k):
        with scope("showwait"):
            show_in(k).wait_recv()
        columns = min(LANES, ky - k * LANES)
        spec_ref[:, pl.ds(k * LANES, columns)] = (
            found[k].reshape(lead * kx, LANES)[:, :columns].astype(f32))

    def add_field(k, f):
        with scope("fwdwait"):
            forward(k, f, peer).wait_recv()
        with scope("dotD"):
            got = lax.dot_general(
                wide_at(k)[f], y_at(k)[...], (((1,), (1,)), ((), ())), preferred_element_type=f32)
            if k > 0:
                got = got + low_ref[span(f, x_local), :]
            low_ref[span(f, x_local), :] = got

    def turn_of(t):
        return lax.rem(spot + lead - lax.rem(t, lead), lead)

    def take(k):
        @pl.loop(1, lead + 1)
        def _(t):
            pass_on(k, turn_of(t))

        reveal(k)

    def expand(k):
        @pl.loop(1, lead + 1)
        def _(t):
            add_field(k, turn_of(t))

    def finish():
        k = chunks - 1
        add_field(k, spot)
        for t in reversed(far_first):
            pass_on(k, mate(t))
        reveal(k)
        with scope("fwdwait"):
            for t in reversed(far_first):
                forward(k, mate(t), peer).wait_recv()

    y_table(0)
    sums(0)
    y_table(1)

    @pl.when(half == 0)
    def _():
        rise(0)

    sums(1)
    y_table(2)

    @pl.when(half == 1)
    def _():
        rise(0)

    def x_table():
        with scope("xtab"):
            xcode_copy.wait()
            make_table(xcode_ref[...], side * xt.shape[0], NX, xt, xta, xtb, xfc, xfs)

    @pl.when(is_hub)
    def _():
        x_table()
        rise(1)
        sums(2)
        y_table(3)

        @pl.when(half == 1)
        def _():
            sums(3)

        partial_sum(0)

        @pl.when(half == 0)
        def _():
            sums(3)

        rise(2)
        rise(3)
        partial_sum(1)
        for k in range(chunks):
            ahead = pieces - 1 - k
            for m in range(ahead):
                meet(k, m)
            if k + 2 < chunks:
                partial_sum(k + 2, 0 if k + 3 == chunks else 1)
            for m in range(ahead, pieces):
                meet(k, m)
            synthesis(k)
            if k == chunks - 2:
                @pl.when(half == 1)
                def _():
                    @pl.loop(0, pieces)
                    def _(m):
                        cross(chunks - 1, m).start()

        forward(chunks - 1, spot, half).start()
        for k in range(chunks - 1):
            take(k)
            expand(k)
        finish()

    @pl.when(jnp.logical_not(is_hub))
    def _():
        sums(2)
        y_table(3)

        rise(1)
        sums(3)
        rise(2)
        rise(3)
        x_table()
        for k in range(chunks):
            for m in range(pieces):
                receive(k, m)
            synthesis(k)
            if k == chunks - 1:
                forward(k, spot, half).start()
            if k > 0:
                take(k - 1)
                expand(k - 1)
        finish()

    with scope("drain"):
        sent(other, gs)
        sent(wide.at[:, :, :, pl.ds(0, LANES)], s4)
        sent(wide_last.at[:, :, pl.ds(0, LANES)], s4)
        sent(found.at[:, pl.ds(0, lead - 1)], s6)
        sent(blocks.at[:, pl.ds(0, lead - 1)], s3)

        @pl.when(is_hub)
        def _():
            sent(part.at[:, pl.ds(0, rows - x_local), :], s1)
            sent(s_out, s2)
            sent(coarse, s5)

        @pl.when(jnp.logical_not(is_hub))
        def _():
            sent(part, s1)


def spectral_filter(lead, x_local, kx, ky, kpad, *operands):
    bf, f32 = jnp.bfloat16, jnp.float32
    operands = [pltpu.with_memory_space_constraint(a, pltpu.HBM) for a in operands]
    grid, x_codes, y_codes = operands
    y_local = grid.shape[1]
    rows, members, modes = lead * x_local, 2 * lead, x_codes.shape[1]
    chunks, pieces = kpad // LANES, 4
    tall_x, tall_y = members * x_local // STEP, y_local // STEP
    dma = pltpu.SemaphoreType.DMA
    vmem = pl.BlockSpec(memory_space=pltpu.VMEM)
    return pl.pallas_call(
        functools.partial(filter_kernel, lead, x_local, kx, ky, kpad),
        out_shape=(
            jax.ShapeDtypeStruct((lead * kx, ky), f32),
            jax.ShapeDtypeStruct((rows, y_local), f32),
            jax.ShapeDtypeStruct((lead, x_local, 2 * LANES), bf),
            jax.ShapeDtypeStruct((y_local, 2 * LANES), bf),
        ),
        in_specs=[pl.BlockSpec(memory_space=pltpu.HBM)] * 3,
        out_specs=(vmem,) * 4,
        scratch_shapes=[
            pltpu.VMEM((rows, y_local), bf),
            pltpu.VMEM(x_codes.shape, jnp.int32),
            pltpu.VMEM(y_codes.shape, jnp.int32),
            pltpu.VMEM((1, 2 * kpad), jnp.int32),
            pltpu.VMEM((chunks, 8, 2 * LANES), jnp.int32),
            pltpu.VMEM((chunks - 1, y_local, 2 * LANES), bf),
            pltpu.VMEM((tall_y, 2 * LANES), f32),
            pltpu.VMEM((tall_y, 2 * LANES), f32),
            pltpu.VMEM((STEP, 2 * LANES), f32),
            pltpu.VMEM((STEP, 2 * LANES), f32),
            pltpu.VMEM((chunks, rows, LANES), f32),
            pltpu.VMEM((chunks, rows, LANES), bf),
            pltpu.VMEM((chunks, rows, LANES), bf),
            pltpu.VMEM((chunks, rows, LANES), bf),
            pltpu.VMEM((chunks, members * x_local, LANES), bf),
            pltpu.VMEM((LANES, members * x_local), bf),
            pltpu.VMEM((members * x_local, modes), bf),
            pltpu.VMEM((tall_x, modes), f32),
            pltpu.VMEM((tall_x, modes), f32),
            pltpu.VMEM((STEP, modes), f32),
            pltpu.VMEM((STEP, modes), f32),
            pltpu.VMEM((chunks, modes, LANES), f32),
            pltpu.VMEM((chunks, modes, LANES), bf),
            pltpu.VMEM((chunks, modes, LANES), bf),
            pltpu.VMEM((chunks, modes, LANES), bf),
            pltpu.VMEM((chunks, lead, x_local, LANES), bf),
            pltpu.VMEM((chunks - 1, lead, x_local, 2 * LANES), bf),
            pltpu.VMEM((chunks, lead, kx, LANES), bf),
            dma, dma((chunks,)),
            dma, dma((chunks,)),
            dma, dma((chunks * pieces,)),
            dma, dma((chunks * lead,)),
            dma, dma((chunks * lead,)),
            dma, dma((chunks * pieces,)),
            dma, dma((chunks,)),
            dma((3,)),
        ],
        compiler_params=pltpu.CompilerParams(
            collective_id=0, has_side_effects=True, vmem_limit_bytes=46 * 1024 * 1024
        ),
    )(*operands)


def last_sum_kernel(order, spec_in, low_in, wide_in, y_in, spec_out, low_out, total, sem):
    lead, x_local, _ = wide_in.shape
    spot = lax.rem(lax.axis_index("gx"), lead)
    spec_copy = pltpu.make_async_copy(spec_in, spec_out, sem.at[lead])

    def field(source, t):
        part = pl.ds(al(flipped(spot, t, lead) * x_local, x_local), x_local)
        return pltpu.make_async_copy(source.at[part, :], low_out.at[part, :], sem.at[t])

    field(low_in, 0).start()
    spec_copy.start()
    for t in order:
        f = flipped(spot, t, lead)
        part = pl.ds(al(f * x_local, x_local), x_local)
        total[part, :] = low_in[part, :] + lax.dot_general(
            wide_in[f], y_in[...], (((1,), (1,)), ((), ())), preferred_element_type=jnp.float32)
        field(total, t).start()
    field(low_in, 0).wait()
    for t in order:
        field(total, t).wait()
    spec_copy.wait()


def last_sum(spec, low, wide, y_table):
    lead = wide.shape[0]
    vmem, anywhere = pl.BlockSpec(memory_space=pltpu.VMEM), pl.BlockSpec(memory_space=pl.ANY)
    return pl.pallas_call(
        functools.partial(last_sum_kernel, near_first(lead)),
        out_shape=(jax.ShapeDtypeStruct(spec.shape, spec.dtype), jax.ShapeDtypeStruct(low.shape, low.dtype)),
        in_specs=[vmem] * 4,
        out_specs=(anywhere, anywhere),
        scratch_shapes=[pltpu.VMEM(low.shape, low.dtype), pltpu.SemaphoreType.DMA((lead + 1,))],
        compiler_params=pltpu.CompilerParams(vmem_limit_bytes=12 * 1024 * 1024),
    )(spec, low, wide, y_table)


def build(gx, gy):
    def local(fields, x_codes, y_codes):
        nf, nz, x_local, y_local = fields.shape
        lead = nf * nz
        ky = y_codes.shape[0] // gy
        kx = x_codes.shape[0] // gx
        unit = 128 * gx // math.gcd(128 * gx, lead)
        if unit > 2 * ky:
            unit = gx // math.gcd(gx, lead)
        kpad = -(-ky // unit) * unit
        cols = lead * kpad // gx
        me_y = lax.axis_index("gy")
        y_first = me_y * y_local
        grid = fields.reshape(lead * x_local, y_local)
        fits = gy == 2 and gx == 4 * lead and lead & (lead - 1) == 0 and kpad == 4 * LANES and kx % 16 == 0
        fits = fits and x_local % 16 == 0 and 2 * lead * x_local % (8 * STEP) == 0
        fits = fits and y_local % (8 * STEP) == 0 and gx * kx % (4 * LANES) == 0
        if fits:
            spec, low = last_sum(*spectral_filter(
                lead, x_local, kx, ky, kpad, grid, x_codes.reshape(1, -1), y_codes.reshape(1, -1)))
            return spec.reshape(nf, nz, kx, ky), low.reshape(nf, nz, x_local, y_local)
        padded = jnp.pad(y_codes.reshape(gy, ky), ((0, 0), (0, kpad - ky)))
        live = jnp.broadcast_to(jnp.arange(kpad)[None] < ky, (gy, kpad)).reshape(-1)
        x_tab = mode_table(x_codes, 0, x_local * gx, NX)
        y_tab = mode_table(padded.reshape(-1), y_first, y_local, NY, live)
        part = jnp.dot(grid, y_tab, preferred_element_type=jnp.float32).reshape(lead * x_local, gy, kpad)
        own = lax.dynamic_index_in_dim(part, me_y, 1, keepdims=False)
        for shift in range(1, gy):
            there = lax.rem(me_y + shift, gy)
            block = lax.dynamic_index_in_dim(part, there, 1, keepdims=False).astype(jnp.bfloat16)
            got = lax.ppermute(block, "gy", [(i, (i + shift) % gy) for i in range(gy)])
            own = own + got.astype(jnp.float32)
        send = own.astype(jnp.bfloat16).reshape(lead, x_local, kpad)
        if cols <= kpad:
            def spread(a):
                n = a.shape[1]
                return a.reshape(lead, n, kpad // cols, cols).transpose(0, 2, 1, 3).reshape(gx, n, cols)

            def merge(a):
                n = a.shape[1]
                return a.reshape(lead, kpad // cols, n, cols).transpose(0, 2, 1, 3).reshape(lead, n, kpad)
        else:
            def spread(a):
                n = a.shape[1]
                return a.transpose(1, 0, 2).reshape(n, gx, cols).transpose(1, 0, 2)

            def merge(a):
                n = a.shape[1]
                return a.transpose(1, 0, 2).reshape(n, lead, kpad).transpose(1, 0, 2)
        lines = lax.all_to_all(spread(send), "gx", split_axis=0, concat_axis=0, tiled=True)
        lines = lines.reshape(gx * x_local, cols)
        modes = lax.dot_general(x_tab, lines, (((0,), (0,)), ((), ())), preferred_element_type=jnp.float32)
        coarse = modes.astype(jnp.bfloat16)
        synth = jnp.dot(x_tab, coarse, preferred_element_type=jnp.float32).astype(jnp.bfloat16)
        back = lax.all_to_all(synth.reshape(gx, x_local, cols), "gx", split_axis=0, concat_axis=0, tiled=True)
        spec = lax.all_to_all(coarse.reshape(gx, kx, cols), "gx", split_axis=0, concat_axis=0, tiled=True)
        spectrum = merge(spec)[:, :, :ky].astype(jnp.float32).reshape(nf, nz, kx, ky)
        mine = merge(back).reshape(lead * x_local, kpad)
        y_parts = y_tab.reshape(y_local, gy, kpad)
        whole = jnp.zeros((gy, lead * x_local, kpad), jnp.bfloat16)
        whole = lax.dynamic_update_index_in_dim(whole, mine, me_y, 0)
        for shift in range(1, gy):
            got = lax.ppermute(mine, "gy", [(i, (i + shift) % gy) for i in range(gy)])
            whole = lax.dynamic_update_index_in_dim(whole, got, lax.rem(me_y + gy - shift, gy), 0)
        wide = whole.transpose(1, 0, 2).reshape(lead * x_local, gy * kpad)
        low = lax.dot_general(wide, y_tab, (((1,), (1,)), ((), ())), preferred_element_type=jnp.float32)
        return spectrum, low.reshape(nf, nz, x_local, y_local)

    return local


def solution(mesh):
    return jax.shard_map(
        build(mesh.shape["gx"], mesh.shape["gy"]),
        mesh=mesh,
        in_specs=(P(None, None, "gx", "gy"), P(), P()),
        out_specs=(P(None, None, "gx", "gy"), P(None, None, "gx", "gy")),
        check_vma=False,
    )
```

```python
import functools
import math

import jax
import jax.numpy as jnp
from jax import lax
from jax.experimental import pallas as pl
from jax.experimental.pallas import tpu as pltpu
from jax.sharding import PartitionSpec as P

NX = 3072
NY = 3072
BAND = 512
STEP = 64


def angle(freq, position, length):
    phase = freq[None, :] * position[:, None] % length
    return phase.astype(jnp.float32) * (2.0 * math.pi / length)


def mode_parts(picked, first, amount, length, live=None):
    step = 64 if amount % 64 == 0 else 8
    freq = jnp.where(picked <= BAND, picked, picked - BAND)
    coarse_angle = angle(freq, first + step * jnp.arange(amount // step, dtype=jnp.int32), length)
    fine_angle = angle(freq, jnp.arange(step, dtype=jnp.int32), length)
    norm = jnp.where(picked == 0, 1.0 / math.sqrt(length), math.sqrt(2.0 / length)).astype(jnp.float32)
    if live is not None:
        norm = jnp.where(live, norm, 0.0)
    is_cos = (picked <= BAND)[None, :]
    c, s = jnp.cos(coarse_angle), jnp.sin(coarse_angle)
    first_part = jnp.where(is_cos, c, s) * norm[None, :]
    second_part = jnp.where(is_cos, -s, c) * norm[None, :]
    fc, fs = jnp.cos(fine_angle), jnp.sin(fine_angle)
    return lax.optimization_barrier((first_part, second_part, fc, fs))


def mode_table(picked, first, amount, length, live=None):
    first_part, second_part, fc, fs = mode_parts(picked, first, amount, length, live)
    table = first_part[:, None, :] * fc[None] + second_part[:, None, :] * fs[None]
    return table.astype(jnp.bfloat16).reshape(amount, picked.shape[0])


def al(v, m):
    return pl.multiple_of(v, m)


def turn(freq, position, shift, length):
    product = freq * position
    quarter = jnp.floor(product * (4.0 / length) + 0.5)
    x = (product * 4.0 - quarter * length) * (2.0 * math.pi / (4 * length))
    x2 = x * x
    s = x + x * x2 * (-1 / 6 + x2 * (1 / 120 + x2 * (-1 / 5040 + x2 * (1 / 362880))))
    c = 1.0 + x2 * (-0.5 + x2 * (1 / 24 + x2 * (-1 / 720 + x2 * (1 / 40320))))
    quarter = quarter - shift
    q = quarter - 4.0 * jnp.floor(quarter * 0.25)
    odd = (q == 1.0) | (q == 3.0)
    cos_value, sin_value = jnp.where(odd, s, c), jnp.where(odd, c, s)
    cos_value = jnp.where((q == 1.0) | (q == 2.0), -cos_value, cos_value)
    return cos_value, jnp.where(q >= 2.0, -sin_value, sin_value)


LANES = 128


def make_table(code, first, length, table, ta, tb, fc, fs):
    amount, codes = table.shape
    f32 = jnp.float32
    freq = jnp.where(code <= BAND, code, code - BAND).astype(f32)
    shift = jnp.where(code <= BAND, 0, 1).astype(f32)
    norm = jnp.where(code == 0, 1.0 / math.sqrt(length), math.sqrt(2.0 / length)).astype(f32)
    norm = jnp.where(code < 0, 0.0, norm)
    row = lax.broadcasted_iota(jnp.int32, (8, codes), 0)

    @pl.loop(0, amount // STEP // 8)
    def _(i):
        c, s = turn(freq, (first + (row + i * 8) * STEP).astype(f32), shift, length)
        ta[pl.ds(al(i * 8, 8), 8), :] = c * norm
        tb[pl.ds(al(i * 8, 8), 8), :] = s * norm

    @pl.loop(0, STEP // 8)
    def _(i):
        c, s = turn(freq, (row + i * 8).astype(f32), 0.0, length)
        fc[pl.ds(al(i * 8, 8), 8), :] = c
        fs[pl.ds(al(i * 8, 8), 8), :] = s

    @pl.loop(0, amount // STEP)
    def _(h):
        table[pl.ds(al(h * STEP, STEP), STEP), :] = (
            ta[pl.ds(h, 1), :] * fc[...] - tb[pl.ds(h, 1), :] * fs[...]
        ).astype(jnp.bfloat16)


def flipped(spot, t, lead):
    f = spot
    for bit in range(lead.bit_length()):
        if t >> bit & 1:
            f = f + (1 << bit) - (2 << bit) * lax.rem(f // (1 << bit), 2)
    return f


def near_first(lead):
    return sorted(range(lead - 1, 0, -1), key=lambda t: bin(t).count("1"))


def filter_kernel(
    lead, x_local, kx, ky, kpad,
    grid_in, xcode_in, ycode_in, spec_ref, low_ref, wide_last, y_last,
    grid_ref, xcode_ref, ycode_ref, y_raw, y_codes, y_ref, yta, ytb, yfc, yfs, own, other, inc, part, lines, turned, xt, xta, xtb, xfc, xfs,
    s_own, s_out, s_in, coarse, blocks, wide, found,
    gs, gr, s1, r1, s2, r2, s3, r3, s4, r4, s5, r5, s6, r6, in_sem,
):
    me = lax.axis_index("gx")
    half = lax.axis_index("gy")
    peer = 1 - half
    bf, f32 = jnp.bfloat16, jnp.float32
    scope = jax.named_scope
    chunks = kpad // LANES
    members = 2 * lead
    modes = xt.shape[1]
    pieces = r2.shape[0] // chunks
    piece = modes // pieces
    rows = lead * x_local
    plane, spot = me // lead, lax.rem(me, lead)
    side = plane // 2
    base = side * members
    mine = me - base
    hub_base = base + (1 - side) * lead
    end_base = base + side * lead
    own_base = plane * lead
    is_hub = plane == 1 + side
    across = (2 - side) * lead + spot

    def grid_copy(f):
        part = pl.ds(al(f * x_local, x_local), x_local)
        return pltpu.make_async_copy(grid_in.at[part, :], grid_ref.at[part, :], in_sem.at[2 + f])

    ycode_copy = pltpu.make_async_copy(ycode_in, ycode_ref, in_sem.at[0])
    xcode_copy = pltpu.make_async_copy(xcode_in, xcode_ref, in_sem.at[1])
    ycode_copy.start()
    for f in range(lead):
        grid_copy(f).start()
    xcode_copy.start()
    barrier = pltpu.get_barrier_semaphore()
    pl.semaphore_signal(barrier, inc=1, device_id={"gy": peer})

    @pl.loop(1, members)
    def _(t):
        pl.semaphore_signal(barrier, inc=1, device_id={"gx": base + lax.rem(mine + t, members)})

    @pl.when(is_hub)
    def _():
        pl.semaphore_signal(barrier, inc=1, device_id={"gx": across})

    def mate(t):
        return flipped(spot, t, lead)

    far_first = near_first(lead)[::-1]
    last = chunks - 1

    def slot(k, i):
        return k if k < last else last + i

    def wide_at(k):
        return wide_last if k == chunks - 1 else wide.at[k]

    def y_at(k):
        return y_last if k == chunks - 1 else y_ref.at[k]

    def span(i, n):
        return pl.ds(al(i * n, n), n)

    def swap(k):
        return pltpu.make_async_remote_copy(
            src_ref=other.at[k], dst_ref=inc.at[k], send_sem=gs, recv_sem=gr.at[k], device_id={"gy": peer})

    def up(k, f):
        return pltpu.make_async_remote_copy(
            src_ref=part.at[k, span(f, x_local), :], dst_ref=lines.at[k, span(mine, x_local), :],
            send_sem=s1, recv_sem=r1.at[k], device_id={"gx": hub_base + f})

    def up_in(k):
        taken = lines.at[k, pl.ds(0, (members - 1) * x_local), :]
        return pltpu.make_async_remote_copy(
            src_ref=taken, dst_ref=taken, send_sem=s1, recv_sem=r1.at[k], device_id={"gx": hub_base})

    def sent(view, sem):
        pltpu.make_async_remote_copy(
            src_ref=view, dst_ref=view, send_sem=sem, recv_sem=gr.at[0], device_id={"gy": peer}).wait_send()

    def cross(k, m):
        return pltpu.make_async_remote_copy(
            src_ref=s_out.at[k, span(m, piece), :], dst_ref=s_in.at[k, span(m, piece), :],
            send_sem=s2, recv_sem=r2.at[k * pieces + m], device_id={"gx": across})

    def relay(k, m):
        view = coarse.at[k, span(m, piece), :]
        return pltpu.make_async_remote_copy(
            src_ref=view, dst_ref=view, send_sem=s5, recv_sem=r5.at[slot(k, m)],
            device_id={"gx": end_base + spot})

    def down(k, f):
        return pltpu.make_async_remote_copy(
            src_ref=blocks.at[k, f], dst_ref=wide_at(k).at[spot, :, span(half, LANES)],
            send_sem=s3, recv_sem=r3.at[slot(k, spot)], device_id={"gx": own_base + f})

    def show(k, f):
        return pltpu.make_async_remote_copy(
            src_ref=coarse.at[k, span(own_base + f, kx), :], dst_ref=found.at[k, spot],
            send_sem=s6, recv_sem=r6.at[k], device_id={"gx": own_base + f})

    def show_in(k):
        view = found.at[k, pl.ds(0, lead - 1)]
        return pltpu.make_async_remote_copy(
            src_ref=view, dst_ref=view, send_sem=s6, recv_sem=r6.at[k], device_id={"gx": own_base})

    def down_in(k, f):
        return pltpu.make_async_remote_copy(
            src_ref=blocks.at[k, 0], dst_ref=wide_at(k).at[f, :, span(half, LANES)],
            send_sem=s3, recv_sem=r3.at[slot(k, f)], device_id={"gx": own_base + f})

    def all_down(k):
        view = wide.at[k, pl.ds(0, lead - 1), :, span(half, LANES)]
        return pltpu.make_async_remote_copy(
            src_ref=view, dst_ref=view, send_sem=s3, recv_sem=r3.at[k], device_id={"gx": own_base})

    def all_forward(k, who):
        place = wide.at[k, :, :, span(who, LANES)]
        return pltpu.make_async_remote_copy(
            src_ref=place, dst_ref=place, send_sem=s4, recv_sem=r4.at[k], device_id={"gy": peer})

    def all_relayed(k):
        view = coarse.at[k]
        return pltpu.make_async_remote_copy(
            src_ref=view, dst_ref=view, send_sem=s5, recv_sem=r5.at[k], device_id={"gx": hub_base})

    def forward(k, f, who):
        place = wide_at(k).at[f, :, span(who, LANES)]
        return pltpu.make_async_remote_copy(
            src_ref=place, dst_ref=place, send_sem=s4, recv_sem=r4.at[slot(k, f)],
            device_id={"gy": peer})

    def local(f):
        return is_hub & (f == spot)

    width = chunks * LANES * 2
    y_raw[...] = jnp.full(y_raw.shape, -1, jnp.int32)
    with scope("codewait"):
        ycode_copy.wait()
    y_raw[:, : 2 * ky] = ycode_ref[...]
    first_half = jnp.broadcast_to(y_raw[...], (8, width))
    second_half = pltpu.roll(first_half, width - ky, 1)
    live = lax.broadcasted_iota(jnp.int32, (8, width), 1) < ky
    first_half = jnp.where(live, first_half, -1)
    second_half = jnp.where(live, second_half, -1)
    for k in range(chunks):
        y_codes[k, :, :LANES] = first_half[:, k * LANES : (k + 1) * LANES]
        y_codes[k, :, LANES:] = second_half[:, k * LANES : (k + 1) * LANES]

    def y_table(k):
        with scope("ytab"):
            make_table(y_codes[k, :1, :], half * grid_ref.shape[1], NY, y_at(k), yta, ytb, yfc, yfs)

    def field_sums(k, part):
        both = jnp.dot(grid_ref[part, :], y_at(k)[...], preferred_element_type=f32)
        low_part, high_part = both[:, :LANES], both[:, LANES:]
        other[k, part, :] = jnp.where(half == 0, high_part, low_part).astype(bf)
        own[k, part, :] = jnp.where(half == 0, low_part, high_part)

    def sums(k):
        if k == 0:
            @pl.loop(0, lead)
            def _(f):
                with scope("gridwait"):
                    grid_copy(f).wait()
                with scope("dotA"):
                    field_sums(k, span(f, x_local))
        else:
            with scope("dotA"):
                field_sums(k, pl.ds(0, rows))
        if k == 0:
            with scope("barrier"):
                pl.semaphore_wait(barrier, members + jnp.where(is_hub, 1, 0))
        swap(k).start()

    def rise(k):
        with scope("swapwait"):
            swap(k).wait_recv()
        part[k] = (own[k] + inc[k].astype(f32)).astype(bf)

        for t in far_first:
            up(k, mate(t)).start()

        @pl.when(jnp.logical_not(is_hub))
        def _():
            up(k, spot).start()

        @pl.when(is_hub)
        def _():
            lines[k, span(mine, x_local), :] = part[k, span(spot, x_local), :]

    def gather(k):
        with scope("upwait"):
            up_in(k).wait_recv()

        with scope("dotB"):
            turned[...] = lines[k].T

    def partial_sum(k, m, held=1):
        with scope("dotB"):
            got = jnp.dot(turned[...], xt[:, pl.ds(m * piece, piece)], preferred_element_type=f32).T
            s_own[k, pl.ds(m * piece, piece), :] = got
            s_out[k, pl.ds(m * piece, piece), :] = got.astype(bf)

        @pl.when(half <= held)
        def _():
            cross(k, m).start()

    mine_x = span(plane - 2 * side, rows)

    def share(k):
        for t in far_first:
            show(k, mate(t)).start()
        found[k, spot] = coarse[k, span(me, kx), :]

    def absorb(k, m):
        if m < pieces - 1:
            @pl.when(plane == m)
            def _():
                share(k)

        if k == chunks - 1:
            with scope("dotC"):
                got = jnp.dot(
                    xt[mine_x, pl.ds(m * piece, piece)], coarse[k, pl.ds(m * piece, piece), :],
                    preferred_element_type=f32)
                own[0] = got if m == 0 else own[0] + got

    def meet(k, m):
        with scope("crosswait"):
            cross(k, m).wait_recv()
        part_of = pl.ds(m * piece, piece)
        coarse[k, part_of, :] = (s_own[k, part_of, :] + s_in[k, part_of, :].astype(f32)).astype(bf)
        relay(k, m).start()
        absorb(k, m)

    def receive(k):
        if k < last:
            with scope("relaywait"):
                all_relayed(k).wait_recv()
        for m in range(pieces):
            if k == last:
                with scope("relaywait"):
                    relay(k, m).wait_recv()
            absorb(k, m)

    def synthesis(k):
        if k < chunks - 1:
            with scope("dotC"):
                syn = jnp.dot(xt[mine_x, :], coarse[k], preferred_element_type=f32)
        else:
            syn = own[0]
        blocks[k] = syn.astype(bf).reshape(lead, x_local, LANES)

        for t in far_first:
            down(k, mate(t)).start()

        wide_at(k)[spot, :, span(half, LANES)] = blocks[k, spot]

        @pl.when(plane == pieces - 1)
        def _():
            share(k)

    def reveal(k):
        with scope("showwait"):
            show_in(k).wait_recv()
        columns = min(LANES, ky - k * LANES)
        spec_ref[:, pl.ds(k * LANES, columns)] = (
            found[k].reshape(lead * kx, LANES)[:, :columns].astype(f32))

    def add_field(k, f):
        with scope("dotD"):
            got = lax.dot_general(
                wide_at(k)[f], y_at(k)[...], (((1,), (1,)), ((), ())), preferred_element_type=f32)
            if k > 0:
                got = got + low_ref[span(f, x_local), :]
            low_ref[span(f, x_local), :] = got

    def take(k):
        with scope("downwait"):
            all_down(k).wait_recv()
        all_forward(k, half).start()
        reveal(k)

    def expand(k):
        with scope("fwdwait"):
            all_forward(k, peer).wait_recv()

        @pl.loop(0, lead)
        def _(f):
            add_field(k, f)

    def finish():
        with scope("fwdwait"):
            forward(last, spot, peer).wait_recv()
        add_field(last, spot)
        for t in reversed(far_first):
            with scope("downwait"):
                down_in(last, mate(t)).wait_recv()
            forward(last, mate(t), half).start()
        reveal(last)
        with scope("fwdwait"):
            for t in reversed(far_first):
                forward(last, mate(t), peer).wait_recv()

    y_table(0)
    sums(0)
    y_table(1)

    @pl.when(half == 0)
    def _():
        rise(0)

    sums(1)
    y_table(2)
    y_table(3)

    @pl.when(half == 1)
    def _():
        rise(0)

    def x_table():
        with scope("xtab"):
            xcode_copy.wait()
            make_table(xcode_ref[...], side * xt.shape[0], NX, xt, xta, xtb, xfc, xfs)

    @pl.when(is_hub)
    def _():
        x_table()
        rise(1)
        sums(2)

        @pl.when(half == 1)
        def _():
            sums(3)

        gather(0)
        for m in range(pieces):
            partial_sum(0, m)

        @pl.when(half == 0)
        def _():
            sums(3)

        rise(2)
        rise(3)
        for k in range(chunks):
            more = k + 1 < chunks
            held = 0 if k + 2 == chunks else 1
            meet(k, 0)
            if more:
                gather(k + 1)
                for m in range(pieces // 2):
                    partial_sum(k + 1, m, held)
            meet(k, 1)
            if more:
                for m in range(pieces // 2, pieces):
                    partial_sum(k + 1, m, held)
            for m in range(2, pieces):
                meet(k, m)
            if k == chunks - 2:
                @pl.when(half == 1)
                def _():
                    @pl.loop(0, pieces)
                    def _(m):
                        cross(chunks - 1, m).start()

            synthesis(k)
            if k == chunks - 2:
                for early in range(chunks - 2):
                    take(early)

                @pl.when(half == 1)
                def _():
                    expand(0)

        forward(chunks - 1, spot, half).start()

        @pl.when(half == 0)
        def _():
            for k in range(chunks - 2):
                expand(k)

        take(chunks - 2)

        @pl.when(half == 1)
        def _():
            for k in range(1, chunks - 2):
                expand(k)

        expand(chunks - 2)
        finish()

    @pl.when(jnp.logical_not(is_hub))
    def _():
        sums(2)
        sums(3)
        rise(1)
        rise(2)
        rise(3)
        x_table()
        for k in range(last):
            receive(k)
            synthesis(k)
            if k > 0:
                take(k - 1)
                if k < last - 1:
                    expand(k - 1)

        @pl.when(half == 1)
        def _():
            expand(last - 2)

        receive(last)
        synthesis(last)
        forward(last, spot, half).start()

        @pl.when(half == 0)
        def _():
            expand(last - 2)

        take(last - 1)
        expand(last - 1)
        finish()

    with scope("drain"):
        sent(other, gs)
        sent(wide.at[:, :, :, pl.ds(0, LANES)], s4)
        sent(wide_last.at[:, :, pl.ds(0, LANES)], s4)
        sent(found.at[:, pl.ds(0, lead - 1)], s6)
        sent(blocks.at[:, pl.ds(0, lead - 1)], s3)

        @pl.when(is_hub)
        def _():
            sent(part.at[:, pl.ds(0, rows - x_local), :], s1)
            sent(s_out, s2)
            sent(coarse, s5)

        @pl.when(jnp.logical_not(is_hub))
        def _():
            sent(part, s1)


def spectral_filter(lead, x_local, kx, ky, kpad, *operands):
    bf, f32 = jnp.bfloat16, jnp.float32
    operands = [pltpu.with_memory_space_constraint(a, pltpu.HBM) for a in operands]
    grid, x_codes, y_codes = operands
    y_local = grid.shape[1]
    rows, members, modes = lead * x_local, 2 * lead, x_codes.shape[1]
    chunks, pieces = kpad // LANES, 4
    tall_x, tall_y = members * x_local // STEP, y_local // STEP
    dma = pltpu.SemaphoreType.DMA
    vmem = pl.BlockSpec(memory_space=pltpu.VMEM)
    return pl.pallas_call(
        functools.partial(filter_kernel, lead, x_local, kx, ky, kpad),
        out_shape=(
            jax.ShapeDtypeStruct((lead * kx, ky), f32),
            jax.ShapeDtypeStruct((rows, y_local), f32),
            jax.ShapeDtypeStruct((lead, x_local, 2 * LANES), bf),
            jax.ShapeDtypeStruct((y_local, 2 * LANES), bf),
        ),
        in_specs=[pl.BlockSpec(memory_space=pltpu.HBM)] * 3,
        out_specs=(vmem,) * 4,
        scratch_shapes=[
            pltpu.VMEM((rows, y_local), bf),
            pltpu.VMEM(x_codes.shape, jnp.int32),
            pltpu.VMEM(y_codes.shape, jnp.int32),
            pltpu.VMEM((1, 2 * kpad), jnp.int32),
            pltpu.VMEM((chunks, 8, 2 * LANES), jnp.int32),
            pltpu.VMEM((chunks - 1, y_local, 2 * LANES), bf),
            pltpu.VMEM((tall_y, 2 * LANES), f32),
            pltpu.VMEM((tall_y, 2 * LANES), f32),
            pltpu.VMEM((STEP, 2 * LANES), f32),
            pltpu.VMEM((STEP, 2 * LANES), f32),
            pltpu.VMEM((chunks, rows, LANES), f32),
            pltpu.VMEM((chunks, rows, LANES), bf),
            pltpu.VMEM((chunks, rows, LANES), bf),
            pltpu.VMEM((chunks, rows, LANES), bf),
            pltpu.VMEM((chunks, members * x_local, LANES), bf),
            pltpu.VMEM((LANES, members * x_local), bf),
            pltpu.VMEM((members * x_local, modes), bf),
            pltpu.VMEM((tall_x, modes), f32),
            pltpu.VMEM((tall_x, modes), f32),
            pltpu.VMEM((STEP, modes), f32),
            pltpu.VMEM((STEP, modes), f32),
            pltpu.VMEM((chunks, modes, LANES), f32),
            pltpu.VMEM((chunks, modes, LANES), bf),
            pltpu.VMEM((chunks, modes, LANES), bf),
            pltpu.VMEM((chunks, modes, LANES), bf),
            pltpu.VMEM((chunks, lead, x_local, LANES), bf),
            pltpu.VMEM((chunks - 1, lead, x_local, 2 * LANES), bf),
            pltpu.VMEM((chunks, lead, kx, LANES), bf),
            dma, dma((chunks,)),
            dma, dma((chunks,)),
            dma, dma((chunks * pieces,)),
            dma, dma((chunks - 1 + lead,)),
            dma, dma((chunks - 1 + lead,)),
            dma, dma((chunks - 1 + pieces,)),
            dma, dma((chunks,)),
            dma((2 + lead,)),
        ],
        compiler_params=pltpu.CompilerParams(
            collective_id=0, has_side_effects=True, vmem_limit_bytes=46 * 1024 * 1024
        ),
    )(*operands)


def last_sum_kernel(order, spec_in, low_in, wide_in, y_in, spec_out, low_out, total, sem):
    lead, x_local, _ = wide_in.shape
    spot = lax.rem(lax.axis_index("gx"), lead)
    spec_copy = pltpu.make_async_copy(spec_in, spec_out, sem.at[lead])

    def field(source, t):
        part = pl.ds(al(flipped(spot, t, lead) * x_local, x_local), x_local)
        return pltpu.make_async_copy(source.at[part, :], low_out.at[part, :], sem.at[t])

    field(low_in, 0).start()
    spec_copy.start()
    for t in order:
        f = flipped(spot, t, lead)
        part = pl.ds(al(f * x_local, x_local), x_local)
        total[part, :] = low_in[part, :] + lax.dot_general(
            wide_in[f], y_in[...], (((1,), (1,)), ((), ())), preferred_element_type=jnp.float32)
        field(total, t).start()
    field(low_in, 0).wait()
    for t in order:
        field(total, t).wait()
    spec_copy.wait()


def last_sum(spec, low, wide, y_table):
    lead = wide.shape[0]
    vmem, anywhere = pl.BlockSpec(memory_space=pltpu.VMEM), pl.BlockSpec(memory_space=pl.ANY)
    return pl.pallas_call(
        functools.partial(last_sum_kernel, near_first(lead)),
        out_shape=(jax.ShapeDtypeStruct(spec.shape, spec.dtype), jax.ShapeDtypeStruct(low.shape, low.dtype)),
        in_specs=[vmem] * 4,
        out_specs=(anywhere, anywhere),
        scratch_shapes=[pltpu.VMEM(low.shape, low.dtype), pltpu.SemaphoreType.DMA((lead + 1,))],
        compiler_params=pltpu.CompilerParams(vmem_limit_bytes=12 * 1024 * 1024),
    )(spec, low, wide, y_table)


def build(gx, gy):
    def local(fields, x_codes, y_codes):
        nf, nz, x_local, y_local = fields.shape
        lead = nf * nz
        ky = y_codes.shape[0] // gy
        kx = x_codes.shape[0] // gx
        unit = 128 * gx // math.gcd(128 * gx, lead)
        if unit > 2 * ky:
            unit = gx // math.gcd(gx, lead)
        kpad = -(-ky // unit) * unit
        cols = lead * kpad // gx
        me_y = lax.axis_index("gy")
        y_first = me_y * y_local
        grid = fields.reshape(lead * x_local, y_local)
        fits = gy == 2 and gx == 4 * lead and lead & (lead - 1) == 0 and kpad == 4 * LANES and kx % 16 == 0
        fits = fits and x_local % 16 == 0 and 2 * lead * x_local % (8 * STEP) == 0
        fits = fits and y_local % (8 * STEP) == 0 and gx * kx % (4 * LANES) == 0
        if fits:
            spec, low = last_sum(*spectral_filter(
                lead, x_local, kx, ky, kpad, grid, x_codes.reshape(1, -1), y_codes.reshape(1, -1)))
            return spec.reshape(nf, nz, kx, ky), low.reshape(nf, nz, x_local, y_local)
        padded = jnp.pad(y_codes.reshape(gy, ky), ((0, 0), (0, kpad - ky)))
        live = jnp.broadcast_to(jnp.arange(kpad)[None] < ky, (gy, kpad)).reshape(-1)
        x_tab = mode_table(x_codes, 0, x_local * gx, NX)
        y_tab = mode_table(padded.reshape(-1), y_first, y_local, NY, live)
        part = jnp.dot(grid, y_tab, preferred_element_type=jnp.float32).reshape(lead * x_local, gy, kpad)
        own = lax.dynamic_index_in_dim(part, me_y, 1, keepdims=False)
        for shift in range(1, gy):
            there = lax.rem(me_y + shift, gy)
            block = lax.dynamic_index_in_dim(part, there, 1, keepdims=False).astype(jnp.bfloat16)
            got = lax.ppermute(block, "gy", [(i, (i + shift) % gy) for i in range(gy)])
            own = own + got.astype(jnp.float32)
        send = own.astype(jnp.bfloat16).reshape(lead, x_local, kpad)
        if cols <= kpad:
            def spread(a):
                n = a.shape[1]
                return a.reshape(lead, n, kpad // cols, cols).transpose(0, 2, 1, 3).reshape(gx, n, cols)

            def merge(a):
                n = a.shape[1]
                return a.reshape(lead, kpad // cols, n, cols).transpose(0, 2, 1, 3).reshape(lead, n, kpad)
        else:
            def spread(a):
                n = a.shape[1]
                return a.transpose(1, 0, 2).reshape(n, gx, cols).transpose(1, 0, 2)

            def merge(a):
                n = a.shape[1]
                return a.transpose(1, 0, 2).reshape(n, lead, kpad).transpose(1, 0, 2)
        lines = lax.all_to_all(spread(send), "gx", split_axis=0, concat_axis=0, tiled=True)
        lines = lines.reshape(gx * x_local, cols)
        modes = lax.dot_general(x_tab, lines, (((0,), (0,)), ((), ())), preferred_element_type=jnp.float32)
        coarse = modes.astype(jnp.bfloat16)
        synth = jnp.dot(x_tab, coarse, preferred_element_type=jnp.float32).astype(jnp.bfloat16)
        back = lax.all_to_all(synth.reshape(gx, x_local, cols), "gx", split_axis=0, concat_axis=0, tiled=True)
        spec = lax.all_to_all(coarse.reshape(gx, kx, cols), "gx", split_axis=0, concat_axis=0, tiled=True)
        spectrum = merge(spec)[:, :, :ky].astype(jnp.float32).reshape(nf, nz, kx, ky)
        mine = merge(back).reshape(lead * x_local, kpad)
        y_parts = y_tab.reshape(y_local, gy, kpad)
        whole = jnp.zeros((gy, lead * x_local, kpad), jnp.bfloat16)
        whole = lax.dynamic_update_index_in_dim(whole, mine, me_y, 0)
        for shift in range(1, gy):
            got = lax.ppermute(mine, "gy", [(i, (i + shift) % gy) for i in range(gy)])
            whole = lax.dynamic_update_index_in_dim(whole, got, lax.rem(me_y + gy - shift, gy), 0)
        wide = whole.transpose(1, 0, 2).reshape(lead * x_local, gy * kpad)
        low = lax.dot_general(wide, y_tab, (((1,), (1,)), ((), ())), preferred_element_type=jnp.float32)
        return spectrum, low.reshape(nf, nz, x_local, y_local)

    return local


def solution(mesh):
    return jax.shard_map(
        build(mesh.shape["gx"], mesh.shape["gy"]),
        mesh=mesh,
        in_specs=(P(None, None, "gx", "gy"), P(), P()),
        out_specs=(P(None, None, "gx", "gy"), P(None, None, "gx", "gy")),
        check_vma=False,
    )
```

```python
import functools
import math

import jax
import jax.numpy as jnp
from jax import lax
from jax.experimental import pallas as pl
from jax.experimental.pallas import tpu as pltpu
from jax.sharding import PartitionSpec as P

NX = 3072
NY = 3072
BAND = 512
STEP = 64


def angle(freq, position, length):
    phase = freq[None, :] * position[:, None] % length
    return phase.astype(jnp.float32) * (2.0 * math.pi / length)


def mode_parts(picked, first, amount, length, live=None):
    step = 64 if amount % 64 == 0 else 8
    freq = jnp.where(picked <= BAND, picked, picked - BAND)
    coarse_angle = angle(freq, first + step * jnp.arange(amount // step, dtype=jnp.int32), length)
    fine_angle = angle(freq, jnp.arange(step, dtype=jnp.int32), length)
    norm = jnp.where(picked == 0, 1.0 / math.sqrt(length), math.sqrt(2.0 / length)).astype(jnp.float32)
    if live is not None:
        norm = jnp.where(live, norm, 0.0)
    is_cos = (picked <= BAND)[None, :]
    c, s = jnp.cos(coarse_angle), jnp.sin(coarse_angle)
    first_part = jnp.where(is_cos, c, s) * norm[None, :]
    second_part = jnp.where(is_cos, -s, c) * norm[None, :]
    fc, fs = jnp.cos(fine_angle), jnp.sin(fine_angle)
    return lax.optimization_barrier((first_part, second_part, fc, fs))


def mode_table(picked, first, amount, length, live=None):
    first_part, second_part, fc, fs = mode_parts(picked, first, amount, length, live)
    table = first_part[:, None, :] * fc[None] + second_part[:, None, :] * fs[None]
    return table.astype(jnp.bfloat16).reshape(amount, picked.shape[0])


def al(v, m):
    return pl.multiple_of(v, m)


def turn(freq, position, shift, length):
    product = freq * position
    quarter = jnp.floor(product * (4.0 / length) + 0.5)
    x = (product * 4.0 - quarter * length) * (2.0 * math.pi / (4 * length))
    x2 = x * x
    s = x + x * x2 * (-1 / 6 + x2 * (1 / 120 + x2 * (-1 / 5040 + x2 * (1 / 362880))))
    c = 1.0 + x2 * (-0.5 + x2 * (1 / 24 + x2 * (-1 / 720 + x2 * (1 / 40320))))
    quarter = quarter - shift
    q = quarter - 4.0 * jnp.floor(quarter * 0.25)
    odd = (q == 1.0) | (q == 3.0)
    cos_value, sin_value = jnp.where(odd, s, c), jnp.where(odd, c, s)
    cos_value = jnp.where((q == 1.0) | (q == 2.0), -cos_value, cos_value)
    return cos_value, jnp.where(q >= 2.0, -sin_value, sin_value)


LANES = 128


def make_table(code, first, length, table, ta, tb, fc, fs):
    amount, codes = table.shape
    f32 = jnp.float32
    freq = jnp.where(code <= BAND, code, code - BAND).astype(f32)
    shift = jnp.where(code <= BAND, 0, 1).astype(f32)
    norm = jnp.where(code == 0, 1.0 / math.sqrt(length), math.sqrt(2.0 / length)).astype(f32)
    norm = jnp.where(code < 0, 0.0, norm)
    row = lax.broadcasted_iota(jnp.int32, (8, codes), 0)

    @pl.loop(0, amount // STEP // 8)
    def _(i):
        c, s = turn(freq, (first + (row + i * 8) * STEP).astype(f32), shift, length)
        ta[pl.ds(al(i * 8, 8), 8), :] = c * norm
        tb[pl.ds(al(i * 8, 8), 8), :] = s * norm

    @pl.loop(0, STEP // 8)
    def _(i):
        c, s = turn(freq, (row + i * 8).astype(f32), 0.0, length)
        fc[pl.ds(al(i * 8, 8), 8), :] = c
        fs[pl.ds(al(i * 8, 8), 8), :] = s

    @pl.loop(0, amount // STEP)
    def _(h):
        table[pl.ds(al(h * STEP, STEP), STEP), :] = (
            ta[pl.ds(h, 1), :] * fc[...] - tb[pl.ds(h, 1), :] * fs[...]
        ).astype(jnp.bfloat16)


def flipped(spot, t, lead):
    f = spot
    for bit in range(lead.bit_length()):
        if t >> bit & 1:
            f = f + (1 << bit) - (2 << bit) * lax.rem(f // (1 << bit), 2)
    return f


def near_first(lead):
    return sorted(range(lead - 1, 0, -1), key=lambda t: bin(t).count("1"))


def filter_kernel(
    lead, x_local, kx, ky, kpad,
    grid_in, xcode_in, ycode_in, spec_ref, low_ref, wide_last, y_last,
    grid_ref, xcode_ref, ycode_ref, y_raw, y_codes, y_ref, yta, ytb, yfc, yfs, own, other, inc, part, lines, turned, xt, xta, xtb, xfc, xfs,
    s_own, s_out, s_in, coarse, blocks, wide, found, far,
    gs, gr, s1, r1, s2, r2, s3, r3, s4, r4, s5, r5, s6, r6, s7, in_sem,
):
    me = lax.axis_index("gx")
    half = lax.axis_index("gy")
    peer = 1 - half
    bf, f32 = jnp.bfloat16, jnp.float32
    scope = jax.named_scope
    chunks = kpad // LANES
    members = 2 * lead
    modes = xt.shape[1]
    pieces = r2.shape[0] // chunks
    piece = modes // pieces
    rows = lead * x_local
    plane, spot = me // lead, lax.rem(me, lead)
    side = plane // 2
    base = side * members
    mine = me - base
    hub_base = base + (1 - side) * lead
    end_base = base + side * lead
    own_base = plane * lead
    is_hub = plane == 1 + side
    across = (2 - side) * lead + spot

    def grid_copy(f):
        part = pl.ds(al(f * x_local, x_local), x_local)
        return pltpu.make_async_copy(grid_in.at[part, :], grid_ref.at[part, :], in_sem.at[2 + f])

    ycode_copy = pltpu.make_async_copy(ycode_in, ycode_ref, in_sem.at[0])
    xcode_copy = pltpu.make_async_copy(xcode_in, xcode_ref, in_sem.at[1])
    ycode_copy.start()
    for f in range(lead):
        grid_copy(f).start()
    xcode_copy.start()
    barrier = pltpu.get_barrier_semaphore()
    pl.semaphore_signal(barrier, inc=1, device_id={"gy": peer})

    @pl.loop(1, members)
    def _(t):
        pl.semaphore_signal(barrier, inc=1, device_id={"gx": base + lax.rem(mine + t, members)})

    @pl.when(is_hub)
    def _():
        pl.semaphore_signal(barrier, inc=1, device_id={"gx": across})

    def mate(t):
        return flipped(spot, t, lead)

    far_first = near_first(lead)[::-1]
    last = chunks - 1

    def slot(k, i):
        return k if k < last else last + i

    def wide_at(k):
        return wide_last if k == chunks - 1 else wide.at[k]

    def y_at(k):
        return y_last if k == chunks - 1 else y_ref.at[k]

    def span(i, n):
        return pl.ds(al(i * n, n), n)

    def swap(k):
        return pltpu.make_async_remote_copy(
            src_ref=other.at[k], dst_ref=inc.at[k], send_sem=gs, recv_sem=gr.at[k], device_id={"gy": peer})

    def up(k, f):
        return pltpu.make_async_remote_copy(
            src_ref=part.at[k, span(f, x_local), :], dst_ref=lines.at[k, span(mine, x_local), :],
            send_sem=s1, recv_sem=r1.at[k], device_id={"gx": hub_base + f})

    def up_in(k):
        taken = lines.at[k, pl.ds(0, (members - 1) * x_local), :]
        return pltpu.make_async_remote_copy(
            src_ref=taken, dst_ref=taken, send_sem=s1, recv_sem=r1.at[k], device_id={"gx": hub_base})

    def sent(view, sem):
        pltpu.make_async_remote_copy(
            src_ref=view, dst_ref=view, send_sem=sem, recv_sem=gr.at[0], device_id={"gy": peer}).wait_send()

    def cross(k, m):
        return pltpu.make_async_remote_copy(
            src_ref=s_out.at[k, span(m, piece), :], dst_ref=s_in.at[k, span(m, piece), :],
            send_sem=s2, recv_sem=r2.at[k * pieces + m], device_id={"gx": across})

    def relay(k, m):
        view = coarse.at[k, span(m, piece), :]
        return pltpu.make_async_remote_copy(
            src_ref=view, dst_ref=view, send_sem=s5, recv_sem=r5.at[slot(k, m)],
            device_id={"gx": end_base + spot})

    def down(k, f):
        return pltpu.make_async_remote_copy(
            src_ref=blocks.at[k, f], dst_ref=wide_at(k).at[spot, :, span(half, LANES)],
            send_sem=s3, recv_sem=r3.at[slot(k, spot)], device_id={"gx": own_base + f})

    def show(k, f):
        return pltpu.make_async_remote_copy(
            src_ref=coarse.at[k, span(own_base + f, kx), :], dst_ref=found.at[k, spot],
            send_sem=s6, recv_sem=r6.at[k], device_id={"gx": own_base + f})

    def show_in(k):
        view = found.at[k, pl.ds(0, lead - 1)]
        return pltpu.make_async_remote_copy(
            src_ref=view, dst_ref=view, send_sem=s6, recv_sem=r6.at[k], device_id={"gx": own_base})

    def down_in(k, f):
        return pltpu.make_async_remote_copy(
            src_ref=blocks.at[k, 0], dst_ref=wide_at(k).at[f, :, span(half, LANES)],
            send_sem=s3, recv_sem=r3.at[slot(k, f)], device_id={"gx": own_base + f})

    def all_down(k):
        view = wide.at[k, pl.ds(0, lead - 1), :, span(half, LANES)]
        return pltpu.make_async_remote_copy(
            src_ref=view, dst_ref=view, send_sem=s3, recv_sem=r3.at[k], device_id={"gx": own_base})

    def all_forward(k, who):
        place = wide.at[k, :, :, span(who, LANES)]
        return pltpu.make_async_remote_copy(
            src_ref=place, dst_ref=place, send_sem=s4, recv_sem=r4.at[k], device_id={"gy": peer})

    def all_relayed(k):
        view = coarse.at[k]
        return pltpu.make_async_remote_copy(
            src_ref=view, dst_ref=view, send_sem=s5, recv_sem=r5.at[k], device_id={"gx": hub_base})

    def forward(k, f, who):
        place = wide_at(k).at[f, :, span(who, LANES)]
        return pltpu.make_async_remote_copy(
            src_ref=place, dst_ref=place, send_sem=s4, recv_sem=r4.at[slot(k, f)],
            device_id={"gy": peer})

    def local(f):
        return is_hub & (f == spot)

    width = chunks * LANES * 2
    y_raw[...] = jnp.full(y_raw.shape, -1, jnp.int32)
    with scope("codewait"):
        ycode_copy.wait()
    y_raw[:, : 2 * ky] = ycode_ref[...]
    first_half = jnp.broadcast_to(y_raw[...], (8, width))
    second_half = pltpu.roll(first_half, width - ky, 1)
    live = lax.broadcasted_iota(jnp.int32, (8, width), 1) < ky
    first_half = jnp.where(live, first_half, -1)
    second_half = jnp.where(live, second_half, -1)
    for k in range(chunks):
        y_codes[k, :, :LANES] = first_half[:, k * LANES : (k + 1) * LANES]
        y_codes[k, :, LANES:] = second_half[:, k * LANES : (k + 1) * LANES]

    def y_table(k):
        with scope("ytab"):
            make_table(y_codes[k, :1, :], half * grid_ref.shape[1], NY, y_at(k), yta, ytb, yfc, yfs)

    def field_sums(k, part):
        both = jnp.dot(grid_ref[part, :], y_at(k)[...], preferred_element_type=f32)
        low_part, high_part = both[:, :LANES], both[:, LANES:]
        other[k, part, :] = jnp.where(half == 0, high_part, low_part).astype(bf)
        own[k, part, :] = jnp.where(half == 0, low_part, high_part)

    def sums(k):
        if k == 0:
            @pl.loop(0, lead)
            def _(f):
                with scope("gridwait"):
                    grid_copy(f).wait()
                with scope("dotA"):
                    field_sums(k, span(f, x_local))
        else:
            with scope("dotA"):
                field_sums(k, pl.ds(0, rows))
        if k == 0:
            with scope("barrier"):
                pl.semaphore_wait(barrier, members + jnp.where(is_hub, 1, 0))
        swap(k).start()

    def rise(k):
        with scope("swapwait"):
            swap(k).wait_recv()
        part[k] = (own[k] + inc[k].astype(f32)).astype(bf)

        for t in far_first:
            up(k, mate(t)).start()

        @pl.when(jnp.logical_not(is_hub))
        def _():
            up(k, spot).start()

        @pl.when(is_hub)
        def _():
            lines[k, span(mine, x_local), :] = part[k, span(spot, x_local), :]

    def gather(k):
        with scope("upwait"):
            up_in(k).wait_recv()

        with scope("dotB"):
            turned[...] = lines[k].T

    def partial_sum(k, m, held=1):
        with scope("dotB"):
            got = jnp.dot(turned[...], xt[:, pl.ds(m * piece, piece)], preferred_element_type=f32).T
            s_own[k, pl.ds(m * piece, piece), :] = got
            s_out[k, pl.ds(m * piece, piece), :] = got.astype(bf)

        @pl.when(half <= held)
        def _():
            cross(k, m).start()

    mine_x = span(plane - 2 * side, rows)

    def share(k):
        for t in far_first:
            show(k, mate(t)).start()
        found[k, spot] = coarse[k, span(me, kx), :]

    far_plane = 3 * side
    far_x = span(far_plane - 2 * side, rows)

    def throw(f):
        return pltpu.make_async_remote_copy(
            src_ref=far.at[f], dst_ref=wide_last.at[spot, :, span(half, LANES)],
            send_sem=s7.at[0], recv_sem=r3.at[slot(last, spot)], device_id={"gx": far_plane * lead + f})

    def throw_modes():
        for t in far_first + [0]:
            f = mate(t)
            pltpu.make_async_remote_copy(
                src_ref=coarse.at[last, span(far_plane * lead + f, kx), :], dst_ref=found.at[last, spot],
                send_sem=s7.at[1], recv_sem=r6.at[last], device_id={"gx": far_plane * lead + f}).start()

    def absorb_far(m):
        if m < pieces - 1:
            @pl.when(far_plane == m)
            def _():
                throw_modes()

        with scope("dotF"):
            got = jnp.dot(
                xt[far_x, pl.ds(m * piece, piece)], coarse[last, pl.ds(m * piece, piece), :],
                preferred_element_type=f32)
            if m < pieces - 1:
                own[1] = got if m == 0 else own[1] + got
            else:
                far[...] = (own[1] + got).astype(bf).reshape(lead, x_local, LANES)
                for t in far_first + [0]:
                    throw(mate(t)).start()

                @pl.when(far_plane == m)
                def _():
                    throw_modes()

    def absorb(k, m):
        if m < pieces - 1:
            @pl.when(plane == m)
            def _():
                share(k)

        if k == chunks - 1:
            with scope("dotC"):
                got = jnp.dot(
                    xt[mine_x, pl.ds(m * piece, piece)], coarse[k, pl.ds(m * piece, piece), :],
                    preferred_element_type=f32)
                own[0] = got if m == 0 else own[0] + got

    def meet(k, m):
        with scope("crosswait"):
            cross(k, m).wait_recv()
        part_of = pl.ds(m * piece, piece)
        coarse[k, part_of, :] = (s_own[k, part_of, :] + s_in[k, part_of, :].astype(f32)).astype(bf)
        if k < last:
            relay(k, m).start()
        else:
            @pl.when(half == 0)
            def _():
                relay(k, m).start()

            @pl.when(half == 1)
            def _():
                absorb_far(m)

        absorb(k, m)

    def receive(k):
        if k < last:
            with scope("relaywait"):
                all_relayed(k).wait_recv()
        for m in range(pieces):
            if k == last:
                with scope("relaywait"):
                    relay(k, m).wait_recv()
            absorb(k, m)

    def synthesis(k):
        if k < chunks - 1:
            with scope("dotC"):
                syn = jnp.dot(xt[mine_x, :], coarse[k], preferred_element_type=f32)
        else:
            syn = own[0]
        blocks[k] = syn.astype(bf).reshape(lead, x_local, LANES)

        for t in far_first:
            down(k, mate(t)).start()

        wide_at(k)[spot, :, span(half, LANES)] = blocks[k, spot]

        @pl.when(plane == pieces - 1)
        def _():
            share(k)

    def reveal(k):
        with scope("showwait"):
            show_in(k).wait_recv()
        write_modes(k)

    def write_modes(k):
        columns = min(LANES, ky - k * LANES)
        spec_ref[:, pl.ds(k * LANES, columns)] = (
            found[k].reshape(lead * kx, LANES)[:, :columns].astype(f32))

    def add_field(k, f):
        with scope("dotD"):
            got = lax.dot_general(
                wide_at(k)[f], y_at(k)[...], (((1,), (1,)), ((), ())), preferred_element_type=f32)
            if k > 0:
                got = got + low_ref[span(f, x_local), :]
            low_ref[span(f, x_local), :] = got

    def take(k):
        with scope("downwait"):
            all_down(k).wait_recv()
        all_forward(k, half).start()
        reveal(k)

    def expand(k):
        with scope("fwdwait"):
            all_forward(k, peer).wait_recv()

        @pl.loop(0, lead)
        def _(f):
            add_field(k, f)

    def own_first():
        with scope("fwdwait"):
            forward(last, spot, peer).wait_recv()
        add_field(last, spot)

    def pass_on(t):
        with scope("downwait"):
            down_in(last, mate(t)).wait_recv()
        forward(last, mate(t), half).start()

    def others():
        with scope("fwdwait"):
            for t in reversed(far_first):
                forward(last, mate(t), peer).wait_recv()

    def finish():
        @pl.when(half == 0)
        def _():
            for t in reversed(far_first):
                pass_on(t)
            own_first()

        @pl.when(half == 1)
        def _():
            own_first()
            for t in reversed(far_first):
                pass_on(t)

        reveal(last)
        others()

    y_table(0)
    sums(0)
    y_table(1)

    @pl.when(half == 0)
    def _():
        rise(0)

    sums(1)
    y_table(2)
    y_table(3)

    @pl.when(half == 1)
    def _():
        rise(0)

    def x_table():
        with scope("xtab"):
            xcode_copy.wait()
            make_table(xcode_ref[...], side * xt.shape[0], NX, xt, xta, xtb, xfc, xfs)

    @pl.when(is_hub)
    def _():
        x_table()
        rise(1)
        sums(2)

        @pl.when(half == 1)
        def _():
            sums(3)

        gather(0)
        for m in range(pieces):
            partial_sum(0, m)

        @pl.when(half == 0)
        def _():
            sums(3)

        rise(2)
        rise(3)
        for k in range(chunks):
            more = k + 1 < chunks
            held = 0 if k + 2 == chunks else 1
            meet(k, 0)
            if more:
                gather(k + 1)
                for m in range(pieces // 2):
                    partial_sum(k + 1, m, held)
            meet(k, 1)
            if more:
                for m in range(pieces // 2, pieces):
                    partial_sum(k + 1, m, held)
            for m in range(2, pieces):
                meet(k, m)
            if k == chunks - 2:
                @pl.when(half == 1)
                def _():
                    @pl.loop(0, pieces)
                    def _(m):
                        cross(chunks - 1, m).start()

            synthesis(k)
            if k == chunks - 2:
                for early in range(chunks - 2):
                    take(early)

                @pl.when(half == 1)
                def _():
                    expand(0)

        forward(chunks - 1, spot, half).start()

        @pl.when(half == 0)
        def _():
            for k in range(chunks - 2):
                expand(k)

        take(chunks - 2)

        @pl.when(half == 1)
        def _():
            for k in range(1, chunks - 2):
                expand(k)

        expand(chunks - 2)
        finish()

    @pl.when(jnp.logical_not(is_hub))
    def _():
        sums(2)
        sums(3)
        rise(1)
        rise(2)
        rise(3)
        x_table()
        for k in range(last):
            receive(k)
            synthesis(k)
            if k > 0:
                take(k - 1)
                if k < last - 1:
                    expand(k - 1)

        @pl.when(half == 1)
        def _():
            expand(last - 2)

        @pl.when(half == 0)
        def _():
            receive(last)
            synthesis(last)
            forward(last, spot, half).start()
            expand(last - 2)

        take(last - 1)
        expand(last - 1)

        @pl.when(half == 0)
        def _():
            for t in reversed(far_first):
                pass_on(t)
            own_first()
            reveal(last)

        @pl.when(half == 1)
        def _():
            pass_on(0)
            own_first()
            for t in reversed(far_first):
                pass_on(t)
            all_found = found.at[last]
            with scope("showwait"):
                pltpu.make_async_remote_copy(
                    src_ref=all_found, dst_ref=all_found, send_sem=s6, recv_sem=r6.at[last],
                    device_id={"gx": own_base}).wait_recv()
            write_modes(last)

        others()

    with scope("drain"):
        sent(other, gs)
        sent(wide.at[:, :, :, pl.ds(0, LANES)], s4)
        sent(wide_last.at[:, :, pl.ds(0, LANES)], s4)

        @pl.when(is_hub)
        def _():
            sent(part.at[:, pl.ds(0, rows - x_local), :], s1)
            sent(s_out, s2)
            sent(found.at[:, pl.ds(0, lead - 1)], s6)
            sent(blocks.at[:, pl.ds(0, lead - 1)], s3)

            @pl.when(half == 0)
            def _():
                sent(coarse, s5)

            @pl.when(half == 1)
            def _():
                sent(coarse.at[pl.ds(0, last)], s5)
                sent(far, s7.at[0])
                sent(found.at[last], s7.at[1])

        @pl.when(jnp.logical_not(is_hub))
        def _():
            sent(part, s1)

            @pl.when(half == 0)
            def _():
                sent(found.at[:, pl.ds(0, lead - 1)], s6)
                sent(blocks.at[:, pl.ds(0, lead - 1)], s3)

            @pl.when(half == 1)
            def _():
                sent(found.at[pl.ds(0, last), pl.ds(0, lead - 1)], s6)
                sent(blocks.at[pl.ds(0, last), pl.ds(0, lead - 1)], s3)


def spectral_filter(lead, x_local, kx, ky, kpad, *operands):
    bf, f32 = jnp.bfloat16, jnp.float32
    operands = [pltpu.with_memory_space_constraint(a, pltpu.HBM) for a in operands]
    grid, x_codes, y_codes = operands
    y_local = grid.shape[1]
    rows, members, modes = lead * x_local, 2 * lead, x_codes.shape[1]
    chunks, pieces = kpad // LANES, 4
    tall_x, tall_y = members * x_local // STEP, y_local // STEP
    dma = pltpu.SemaphoreType.DMA
    vmem = pl.BlockSpec(memory_space=pltpu.VMEM)
    return pl.pallas_call(
        functools.partial(filter_kernel, lead, x_local, kx, ky, kpad),
        out_shape=(
            jax.ShapeDtypeStruct((lead * kx, ky), f32),
            jax.ShapeDtypeStruct((rows, y_local), f32),
            jax.ShapeDtypeStruct((lead, x_local, 2 * LANES), bf),
            jax.ShapeDtypeStruct((y_local, 2 * LANES), bf),
        ),
        in_specs=[pl.BlockSpec(memory_space=pltpu.HBM)] * 3,
        out_specs=(vmem,) * 4,
        scratch_shapes=[
            pltpu.VMEM((rows, y_local), bf),
            pltpu.VMEM(x_codes.shape, jnp.int32),
            pltpu.VMEM(y_codes.shape, jnp.int32),
            pltpu.VMEM((1, 2 * kpad), jnp.int32),
            pltpu.VMEM((chunks, 8, 2 * LANES), jnp.int32),
            pltpu.VMEM((chunks - 1, y_local, 2 * LANES), bf),
            pltpu.VMEM((tall_y, 2 * LANES), f32),
            pltpu.VMEM((tall_y, 2 * LANES), f32),
            pltpu.VMEM((STEP, 2 * LANES), f32),
            pltpu.VMEM((STEP, 2 * LANES), f32),
            pltpu.VMEM((chunks, rows, LANES), f32),
            pltpu.VMEM((chunks, rows, LANES), bf),
            pltpu.VMEM((chunks, rows, LANES), bf),
            pltpu.VMEM((chunks, rows, LANES), bf),
            pltpu.VMEM((chunks, members * x_local, LANES), bf),
            pltpu.VMEM((LANES, members * x_local), bf),
            pltpu.VMEM((members * x_local, modes), bf),
            pltpu.VMEM((tall_x, modes), f32),
            pltpu.VMEM((tall_x, modes), f32),
            pltpu.VMEM((STEP, modes), f32),
            pltpu.VMEM((STEP, modes), f32),
            pltpu.VMEM((chunks, modes, LANES), f32),
            pltpu.VMEM((chunks, modes, LANES), bf),
            pltpu.VMEM((chunks, modes, LANES), bf),
            pltpu.VMEM((chunks, modes, LANES), bf),
            pltpu.VMEM((chunks, lead, x_local, LANES), bf),
            pltpu.VMEM((chunks - 1, lead, x_local, 2 * LANES), bf),
            pltpu.VMEM((chunks, lead, kx, LANES), bf),
            pltpu.VMEM((lead, x_local, LANES), bf),
            dma, dma((chunks,)),
            dma, dma((chunks,)),
            dma, dma((chunks * pieces,)),
            dma, dma((chunks - 1 + lead,)),
            dma, dma((chunks - 1 + lead,)),
            dma, dma((chunks - 1 + pieces,)),
            dma, dma((chunks,)),
            dma((2,)),
            dma((2 + lead,)),
        ],
        compiler_params=pltpu.CompilerParams(
            collective_id=0, has_side_effects=True, vmem_limit_bytes=46 * 1024 * 1024
        ),
    )(*operands)


def last_sum_kernel(order, spec_in, low_in, wide_in, y_in, spec_out, low_out, total, sem):
    lead, x_local, _ = wide_in.shape
    spot = lax.rem(lax.axis_index("gx"), lead)
    spec_copy = pltpu.make_async_copy(spec_in, spec_out, sem.at[lead])

    def field(source, t):
        part = pl.ds(al(flipped(spot, t, lead) * x_local, x_local), x_local)
        return pltpu.make_async_copy(source.at[part, :], low_out.at[part, :], sem.at[t])

    field(low_in, 0).start()
    spec_copy.start()
    for t in order:
        f = flipped(spot, t, lead)
        part = pl.ds(al(f * x_local, x_local), x_local)
        total[part, :] = low_in[part, :] + lax.dot_general(
            wide_in[f], y_in[...], (((1,), (1,)), ((), ())), preferred_element_type=jnp.float32)
        field(total, t).start()
    field(low_in, 0).wait()
    for t in order:
        field(total, t).wait()
    spec_copy.wait()


def last_sum(spec, low, wide, y_table):
    lead = wide.shape[0]
    vmem, anywhere = pl.BlockSpec(memory_space=pltpu.VMEM), pl.BlockSpec(memory_space=pl.ANY)
    return pl.pallas_call(
        functools.partial(last_sum_kernel, near_first(lead)),
        out_shape=(jax.ShapeDtypeStruct(spec.shape, spec.dtype), jax.ShapeDtypeStruct(low.shape, low.dtype)),
        in_specs=[vmem] * 4,
        out_specs=(anywhere, anywhere),
        scratch_shapes=[pltpu.VMEM(low.shape, low.dtype), pltpu.SemaphoreType.DMA((lead + 1,))],
        compiler_params=pltpu.CompilerParams(vmem_limit_bytes=12 * 1024 * 1024),
    )(spec, low, wide, y_table)


def build(gx, gy):
    def local(fields, x_codes, y_codes):
        nf, nz, x_local, y_local = fields.shape
        lead = nf * nz
        ky = y_codes.shape[0] // gy
        kx = x_codes.shape[0] // gx
        unit = 128 * gx // math.gcd(128 * gx, lead)
        if unit > 2 * ky:
            unit = gx // math.gcd(gx, lead)
        kpad = -(-ky // unit) * unit
        cols = lead * kpad // gx
        me_y = lax.axis_index("gy")
        y_first = me_y * y_local
        grid = fields.reshape(lead * x_local, y_local)
        fits = gy == 2 and gx == 4 * lead and lead & (lead - 1) == 0 and kpad == 4 * LANES and kx % 16 == 0
        fits = fits and x_local % 16 == 0 and 2 * lead * x_local % (8 * STEP) == 0
        fits = fits and y_local % (8 * STEP) == 0 and gx * kx % (4 * LANES) == 0
        if fits:
            spec, low = last_sum(*spectral_filter(
                lead, x_local, kx, ky, kpad, grid, x_codes.reshape(1, -1), y_codes.reshape(1, -1)))
            return spec.reshape(nf, nz, kx, ky), low.reshape(nf, nz, x_local, y_local)
        padded = jnp.pad(y_codes.reshape(gy, ky), ((0, 0), (0, kpad - ky)))
        live = jnp.broadcast_to(jnp.arange(kpad)[None] < ky, (gy, kpad)).reshape(-1)
        x_tab = mode_table(x_codes, 0, x_local * gx, NX)
        y_tab = mode_table(padded.reshape(-1), y_first, y_local, NY, live)
        part = jnp.dot(grid, y_tab, preferred_element_type=jnp.float32).reshape(lead * x_local, gy, kpad)
        own = lax.dynamic_index_in_dim(part, me_y, 1, keepdims=False)
        for shift in range(1, gy):
            there = lax.rem(me_y + shift, gy)
            block = lax.dynamic_index_in_dim(part, there, 1, keepdims=False).astype(jnp.bfloat16)
            got = lax.ppermute(block, "gy", [(i, (i + shift) % gy) for i in range(gy)])
            own = own + got.astype(jnp.float32)
        send = own.astype(jnp.bfloat16).reshape(lead, x_local, kpad)
        if cols <= kpad:
            def spread(a):
                n = a.shape[1]
                return a.reshape(lead, n, kpad // cols, cols).transpose(0, 2, 1, 3).reshape(gx, n, cols)

            def merge(a):
                n = a.shape[1]
                return a.reshape(lead, kpad // cols, n, cols).transpose(0, 2, 1, 3).reshape(lead, n, kpad)
        else:
            def spread(a):
                n = a.shape[1]
                return a.transpose(1, 0, 2).reshape(n, gx, cols).transpose(1, 0, 2)

            def merge(a):
                n = a.shape[1]
                return a.transpose(1, 0, 2).reshape(n, lead, kpad).transpose(1, 0, 2)
        lines = lax.all_to_all(spread(send), "gx", split_axis=0, concat_axis=0, tiled=True)
        lines = lines.reshape(gx * x_local, cols)
        modes = lax.dot_general(x_tab, lines, (((0,), (0,)), ((), ())), preferred_element_type=jnp.float32)
        coarse = modes.astype(jnp.bfloat16)
        synth = jnp.dot(x_tab, coarse, preferred_element_type=jnp.float32).astype(jnp.bfloat16)
        back = lax.all_to_all(synth.reshape(gx, x_local, cols), "gx", split_axis=0, concat_axis=0, tiled=True)
        spec = lax.all_to_all(coarse.reshape(gx, kx, cols), "gx", split_axis=0, concat_axis=0, tiled=True)
        spectrum = merge(spec)[:, :, :ky].astype(jnp.float32).reshape(nf, nz, kx, ky)
        mine = merge(back).reshape(lead * x_local, kpad)
        y_parts = y_tab.reshape(y_local, gy, kpad)
        whole = jnp.zeros((gy, lead * x_local, kpad), jnp.bfloat16)
        whole = lax.dynamic_update_index_in_dim(whole, mine, me_y, 0)
        for shift in range(1, gy):
            got = lax.ppermute(mine, "gy", [(i, (i + shift) % gy) for i in range(gy)])
            whole = lax.dynamic_update_index_in_dim(whole, got, lax.rem(me_y + gy - shift, gy), 0)
        wide = whole.transpose(1, 0, 2).reshape(lead * x_local, gy * kpad)
        low = lax.dot_general(wide, y_tab, (((1,), (1,)), ((), ())), preferred_element_type=jnp.float32)
        return spectrum, low.reshape(nf, nz, x_local, y_local)

    return local


def solution(mesh):
    return jax.shard_map(
        build(mesh.shape["gx"], mesh.shape["gy"]),
        mesh=mesh,
        in_specs=(P(None, None, "gx", "gy"), P(), P()),
        out_specs=(P(None, None, "gx", "gy"), P(None, None, "gx", "gy")),
        check_vma=False,
    )
```

```python
import functools
import math

import jax
import jax.numpy as jnp
from jax import lax
from jax.experimental import pallas as pl
from jax.experimental.pallas import tpu as pltpu
from jax.sharding import PartitionSpec as P

NX = 3072
NY = 3072
BAND = 512
STEP = 64


def angle(freq, position, length):
    phase = freq[None, :] * position[:, None] % length
    return phase.astype(jnp.float32) * (2.0 * math.pi / length)


def mode_parts(picked, first, amount, length, live=None):
    step = 64 if amount % 64 == 0 else 8
    freq = jnp.where(picked <= BAND, picked, picked - BAND)
    coarse_angle = angle(freq, first + step * jnp.arange(amount // step, dtype=jnp.int32), length)
    fine_angle = angle(freq, jnp.arange(step, dtype=jnp.int32), length)
    norm = jnp.where(picked == 0, 1.0 / math.sqrt(length), math.sqrt(2.0 / length)).astype(jnp.float32)
    if live is not None:
        norm = jnp.where(live, norm, 0.0)
    is_cos = (picked <= BAND)[None, :]
    c, s = jnp.cos(coarse_angle), jnp.sin(coarse_angle)
    first_part = jnp.where(is_cos, c, s) * norm[None, :]
    second_part = jnp.where(is_cos, -s, c) * norm[None, :]
    fc, fs = jnp.cos(fine_angle), jnp.sin(fine_angle)
    return lax.optimization_barrier((first_part, second_part, fc, fs))


def mode_table(picked, first, amount, length, live=None):
    first_part, second_part, fc, fs = mode_parts(picked, first, amount, length, live)
    table = first_part[:, None, :] * fc[None] + second_part[:, None, :] * fs[None]
    return table.astype(jnp.bfloat16).reshape(amount, picked.shape[0])


def al(v, m):
    return pl.multiple_of(v, m)


def turn(freq, position, shift, length):
    product = freq * position
    quarter = jnp.floor(product * (4.0 / length) + 0.5)
    x = (product * 4.0 - quarter * length) * (2.0 * math.pi / (4 * length))
    x2 = x * x
    s = x + x * x2 * (-1 / 6 + x2 * (1 / 120 + x2 * (-1 / 5040 + x2 * (1 / 362880))))
    c = 1.0 + x2 * (-0.5 + x2 * (1 / 24 + x2 * (-1 / 720 + x2 * (1 / 40320))))
    quarter = quarter - shift
    q = quarter - 4.0 * jnp.floor(quarter * 0.25)
    odd = (q == 1.0) | (q == 3.0)
    cos_value, sin_value = jnp.where(odd, s, c), jnp.where(odd, c, s)
    cos_value = jnp.where((q == 1.0) | (q == 2.0), -cos_value, cos_value)
    return cos_value, jnp.where(q >= 2.0, -sin_value, sin_value)


LANES = 128


def make_table(code, first, length, table, side, ta, tb, fc, fs):
    amount, codes = table.shape[0], code.shape[1]
    f32 = jnp.float32
    freq = jnp.where(code <= BAND, code, code - BAND).astype(f32)
    shift = jnp.where(code <= BAND, 0, 1).astype(f32)
    norm = jnp.where(code == 0, 1.0 / math.sqrt(length), math.sqrt(2.0 / length)).astype(f32)
    norm = jnp.where(code < 0, 0.0, norm)
    row = lax.broadcasted_iota(jnp.int32, (8, codes), 0)

    @pl.loop(0, amount // STEP // 8)
    def _(i):
        c, s = turn(freq, (first + (row + i * 8) * STEP).astype(f32), shift, length)
        ta[pl.ds(al(i * 8, 8), 8), :] = c * norm
        tb[pl.ds(al(i * 8, 8), 8), :] = s * norm

    @pl.loop(0, STEP // 8)
    def _(i):
        c, s = turn(freq, (row + i * 8).astype(f32), 0.0, length)
        fc[pl.ds(al(i * 8, 8), 8), :] = c
        fs[pl.ds(al(i * 8, 8), 8), :] = s

    @pl.loop(0, amount // STEP)
    def _(h):
        table[pl.ds(al(h * STEP, STEP), STEP), side] = (
            ta[pl.ds(h, 1), :] * fc[...] - tb[pl.ds(h, 1), :] * fs[...]
        ).astype(jnp.bfloat16)


def flipped(spot, t, lead):
    f = spot
    for bit in range(lead.bit_length()):
        if t >> bit & 1:
            f = f + (1 << bit) - (2 << bit) * lax.rem(f // (1 << bit), 2)
    return f


def near_first(lead):
    return sorted(range(lead - 1, 0, -1), key=lambda t: bin(t).count("1"))


def filter_kernel(
    lead, x_local, kx, ky, kpad,
    grid_in, xcode_in, ycode_in, spec_ref, low_ref, wide_last, y_last,
    grid_ref, xcode_ref, ycode_ref, y_raw, y_codes, y_ref, yta, ytb, yfc, yfs, own, other, inc, part, lines, turned, xt, xta, xtb, xfc, xfs,
    s_own, s_out, s_in, coarse, blocks, wide, found, far,
    gs, gr, s1, r1, s2, r2, s3, r3, s4, r4, s5, r5, s6, r6, s7, in_sem,
):
    me = lax.axis_index("gx")
    half = lax.axis_index("gy")
    peer = 1 - half
    bf, f32 = jnp.bfloat16, jnp.float32
    scope = jax.named_scope
    chunks = kpad // LANES
    members = 2 * lead
    modes = xt.shape[1]
    pieces = r2.shape[0] // chunks
    piece = modes // pieces
    rows = lead * x_local
    plane, spot = me // lead, lax.rem(me, lead)
    side = plane // 2
    base = side * members
    mine = me - base
    hub_base = base + (1 - side) * lead
    end_base = base + side * lead
    own_base = plane * lead
    is_hub = plane == 1 + side
    across = (2 - side) * lead + spot

    def grid_copy(f):
        part = pl.ds(al(f * x_local, x_local), x_local)
        return pltpu.make_async_copy(grid_in.at[part, :], grid_ref.at[part, :], in_sem.at[2 + f])

    ycode_copy = pltpu.make_async_copy(ycode_in, ycode_ref, in_sem.at[0])
    xcode_copy = pltpu.make_async_copy(xcode_in, xcode_ref, in_sem.at[1])
    ycode_copy.start()
    for f in range(lead):
        grid_copy(f).start()
    xcode_copy.start()
    barrier = pltpu.get_barrier_semaphore()
    pl.semaphore_signal(barrier, inc=1, device_id={"gy": peer})

    @pl.loop(1, members)
    def _(t):
        pl.semaphore_signal(barrier, inc=1, device_id={"gx": base + lax.rem(mine + t, members)})

    @pl.when(is_hub)
    def _():
        pl.semaphore_signal(barrier, inc=1, device_id={"gx": across})

    def mate(t):
        return flipped(spot, t, lead)

    far_first = near_first(lead)[::-1]
    last = chunks - 1

    def slot(k, i):
        return k if k < last else last + i

    def late(k):
        return pl.ds((k - chunks + 2) * 2 * LANES, 2 * LANES)

    def wide_at(k, who):
        if k >= chunks - 2:
            return wide_last, pl.ds(al((2 * (k - chunks + 2) + who) * LANES, LANES), LANES)
        return wide.at[k], span(who, LANES)

    def wide_row(k, f, who):
        ref, columns = wide_at(k, who)
        return ref.at[f, :, columns]

    def both_halves(k, f):
        return wide_last[f, :, late(k)] if k >= chunks - 2 else wide[k, f]

    def y_place(k):
        return (y_last, late(k)) if k >= chunks - 2 else (y_ref.at[k], slice(None))

    def y_at(k):
        ref, columns = y_place(k)
        return ref[:, columns]

    def span(i, n):
        return pl.ds(al(i * n, n), n)

    def swap(k):
        return pltpu.make_async_remote_copy(
            src_ref=other.at[k], dst_ref=inc.at[k], send_sem=gs, recv_sem=gr.at[k], device_id={"gy": peer})

    def up(k, f):
        return pltpu.make_async_remote_copy(
            src_ref=part.at[k, span(f, x_local), :], dst_ref=lines.at[k, span(mine, x_local), :],
            send_sem=s1, recv_sem=r1.at[k], device_id={"gx": hub_base + f})

    def up_in(k):
        taken = lines.at[k, pl.ds(0, (members - 1) * x_local), :]
        return pltpu.make_async_remote_copy(
            src_ref=taken, dst_ref=taken, send_sem=s1, recv_sem=r1.at[k], device_id={"gx": hub_base})

    def sent(view, sem):
        pltpu.make_async_remote_copy(
            src_ref=view, dst_ref=view, send_sem=sem, recv_sem=gr.at[0], device_id={"gy": peer}).wait_send()

    def cross(k, m):
        return pltpu.make_async_remote_copy(
            src_ref=s_out.at[k, span(m, piece), :], dst_ref=s_in.at[k, span(m, piece), :],
            send_sem=s2, recv_sem=r2.at[k * pieces + m], device_id={"gx": across})

    def relay(k, m):
        view = coarse.at[k, span(m, piece), :]
        return pltpu.make_async_remote_copy(
            src_ref=view, dst_ref=view, send_sem=s5, recv_sem=r5.at[slot(k, m)],
            device_id={"gx": end_base + spot})

    def down(k, f):
        return pltpu.make_async_remote_copy(
            src_ref=blocks.at[k, f], dst_ref=wide_row(k, spot, half),
            send_sem=s3, recv_sem=r3.at[slot(k, spot)], device_id={"gx": own_base + f})

    def show(k, f):
        return pltpu.make_async_remote_copy(
            src_ref=coarse.at[k, span(own_base + f, kx), :], dst_ref=found.at[k, spot],
            send_sem=s6, recv_sem=r6.at[k], device_id={"gx": own_base + f})

    def show_in(k):
        view = found.at[k, pl.ds(0, lead - 1)]
        return pltpu.make_async_remote_copy(
            src_ref=view, dst_ref=view, send_sem=s6, recv_sem=r6.at[k], device_id={"gx": own_base})

    def down_in(k, f):
        return pltpu.make_async_remote_copy(
            src_ref=blocks.at[k, 0], dst_ref=wide_row(k, f, half),
            send_sem=s3, recv_sem=r3.at[slot(k, f)], device_id={"gx": own_base + f})

    def all_down(k):
        ref, columns = wide_at(k, half)
        view = ref.at[pl.ds(0, lead - 1), :, columns]
        return pltpu.make_async_remote_copy(
            src_ref=view, dst_ref=view, send_sem=s3, recv_sem=r3.at[k], device_id={"gx": own_base})

    def all_forward(k, who):
        ref, columns = wide_at(k, who)
        place = ref.at[:, :, columns]
        return pltpu.make_async_remote_copy(
            src_ref=place, dst_ref=place, send_sem=s4, recv_sem=r4.at[k], device_id={"gy": peer})

    def all_relayed(k):
        view = coarse.at[k]
        return pltpu.make_async_remote_copy(
            src_ref=view, dst_ref=view, send_sem=s5, recv_sem=r5.at[k], device_id={"gx": hub_base})

    def forward(k, f, who):
        place = wide_row(k, f, who)
        return pltpu.make_async_remote_copy(
            src_ref=place, dst_ref=place, send_sem=s4, recv_sem=r4.at[slot(k, f)],
            device_id={"gy": peer})

    def local(f):
        return is_hub & (f == spot)

    width = chunks * LANES * 2
    y_raw[...] = jnp.full(y_raw.shape, -1, jnp.int32)
    with scope("codewait"):
        ycode_copy.wait()
    y_raw[:, : 2 * ky] = ycode_ref[...]
    first_half = jnp.broadcast_to(y_raw[...], (8, width))
    second_half = pltpu.roll(first_half, width - ky, 1)
    live = lax.broadcasted_iota(jnp.int32, (8, width), 1) < ky
    first_half = jnp.where(live, first_half, -1)
    second_half = jnp.where(live, second_half, -1)
    for k in range(chunks):
        y_codes[k, :, :LANES] = first_half[:, k * LANES : (k + 1) * LANES]
        y_codes[k, :, LANES:] = second_half[:, k * LANES : (k + 1) * LANES]

    def y_table(k):
        with scope("ytab"):
            make_table(y_codes[k, :1, :], half * grid_ref.shape[1], NY, *y_place(k), yta, ytb, yfc, yfs)

    def field_sums(k, part):
        both = jnp.dot(grid_ref[part, :], y_at(k), preferred_element_type=f32)
        low_part, high_part = both[:, :LANES], both[:, LANES:]
        other[k, part, :] = jnp.where(half == 0, high_part, low_part).astype(bf)
        own[k, part, :] = jnp.where(half == 0, low_part, high_part)

    def sums(k):
        if k == 0:
            @pl.loop(0, lead)
            def _(f):
                with scope("gridwait"):
                    grid_copy(f).wait()
                with scope("dotA"):
                    field_sums(k, span(f, x_local))
        else:
            with scope("dotA"):
                field_sums(k, pl.ds(0, rows))
        if k == 0:
            with scope("barrier"):
                pl.semaphore_wait(barrier, members + jnp.where(is_hub, 1, 0))
        swap(k).start()

    def rise(k):
        with scope("swapwait"):
            swap(k).wait_recv()
        part[k] = (own[k] + inc[k].astype(f32)).astype(bf)

        for t in far_first:
            up(k, mate(t)).start()

        @pl.when(jnp.logical_not(is_hub))
        def _():
            up(k, spot).start()

        @pl.when(is_hub)
        def _():
            lines[k, span(mine, x_local), :] = part[k, span(spot, x_local), :]

    def gather(k):
        with scope("upwait"):
            up_in(k).wait_recv()

        with scope("dotB"):
            turned[...] = lines[k].T

    def partial_sum(k, m, held=1):
        with scope("dotB"):
            got = jnp.dot(turned[...], xt[:, pl.ds(m * piece, piece)], preferred_element_type=f32).T
            s_own[k, pl.ds(m * piece, piece), :] = got
            s_out[k, pl.ds(m * piece, piece), :] = got.astype(bf)

        @pl.when(half <= held)
        def _():
            cross(k, m).start()

    mine_x = span(plane - 2 * side, rows)

    def share(k):
        for t in far_first:
            show(k, mate(t)).start()
        found[k, spot] = coarse[k, span(me, kx), :]

    far_plane = 3 * side
    far_x = span(far_plane - 2 * side, rows)

    def throw(f):
        return pltpu.make_async_remote_copy(
            src_ref=far.at[f], dst_ref=wide_row(last, spot, half),
            send_sem=s7.at[0], recv_sem=r3.at[slot(last, spot)], device_id={"gx": far_plane * lead + f})

    def throw_modes():
        for t in far_first + [0]:
            f = mate(t)
            pltpu.make_async_remote_copy(
                src_ref=coarse.at[last, span(far_plane * lead + f, kx), :], dst_ref=found.at[last, spot],
                send_sem=s7.at[1], recv_sem=r6.at[last], device_id={"gx": far_plane * lead + f}).start()

    def absorb_far(m):
        if m < pieces - 1:
            @pl.when(far_plane == m)
            def _():
                throw_modes()

        with scope("dotF"):
            got = jnp.dot(
                xt[far_x, pl.ds(m * piece, piece)], coarse[last, pl.ds(m * piece, piece), :],
                preferred_element_type=f32)
            if m < pieces - 1:
                own[1] = got if m == 0 else own[1] + got
            else:
                far[...] = (own[1] + got).astype(bf).reshape(lead, x_local, LANES)
                for t in far_first + [0]:
                    throw(mate(t)).start()

                @pl.when(far_plane == m)
                def _():
                    throw_modes()

    def absorb(k, m):
        if m < pieces - 1:
            @pl.when(plane == m)
            def _():
                share(k)

        if k == chunks - 1:
            with scope("dotC"):
                got = jnp.dot(
                    xt[mine_x, pl.ds(m * piece, piece)], coarse[k, pl.ds(m * piece, piece), :],
                    preferred_element_type=f32)
                own[0] = got if m == 0 else own[0] + got

    def meet(k, m):
        with scope("crosswait"):
            cross(k, m).wait_recv()
        part_of = pl.ds(m * piece, piece)
        coarse[k, part_of, :] = (s_own[k, part_of, :] + s_in[k, part_of, :].astype(f32)).astype(bf)
        if k < last:
            relay(k, m).start()
        else:
            @pl.when(half == 0)
            def _():
                relay(k, m).start()

            @pl.when(half == 1)
            def _():
                absorb_far(m)

        absorb(k, m)

    def receive(k):
        if k < last:
            with scope("relaywait"):
                all_relayed(k).wait_recv()
        for m in range(pieces):
            if k == last:
                with scope("relaywait"):
                    relay(k, m).wait_recv()
            absorb(k, m)

    def synthesis(k):
        if k < chunks - 1:
            with scope("dotC"):
                syn = jnp.dot(xt[mine_x, :], coarse[k], preferred_element_type=f32)
        else:
            syn = own[0]
        blocks[k] = syn.astype(bf).reshape(lead, x_local, LANES)

        for t in far_first:
            down(k, mate(t)).start()

        ref, columns = wide_at(k, half)
        ref[spot, :, columns] = blocks[k, spot]

        @pl.when(plane == pieces - 1)
        def _():
            share(k)

    def reveal(k):
        with scope("showwait"):
            show_in(k).wait_recv()
        write_modes(k)

    def write_modes(k):
        columns = min(LANES, ky - k * LANES)
        spec_ref[:, pl.ds(k * LANES, columns)] = (
            found[k].reshape(lead * kx, LANES)[:, :columns].astype(f32))

    def add_field(k, f):
        with scope("dotD"):
            got = lax.dot_general(
                both_halves(k, f), y_at(k), (((1,), (1,)), ((), ())), preferred_element_type=f32)
            if k > 0:
                got = got + low_ref[span(f, x_local), :]
            low_ref[span(f, x_local), :] = got

    def take(k):
        with scope("downwait"):
            all_down(k).wait_recv()
        all_forward(k, half).start()
        reveal(k)

    def expand(k):
        with scope("fwdwait"):
            all_forward(k, peer).wait_recv()

        if k == last - 1:
            add_field(k, spot)
            return

        @pl.loop(0, lead)
        def _(f):
            add_field(k, f)

    def own_first():
        with scope("fwdwait"):
            forward(last, spot, peer).wait_recv()
        add_field(last, spot)

    def pass_on(t):
        with scope("downwait"):
            down_in(last, mate(t)).wait_recv()
        forward(last, mate(t), half).start()

    def others():
        with scope("fwdwait"):
            for t in reversed(far_first):
                forward(last, mate(t), peer).wait_recv()

    def finish():
        @pl.when(half == 0)
        def _():
            for t in reversed(far_first):
                pass_on(t)
            own_first()

        @pl.when(half == 1)
        def _():
            own_first()
            for t in reversed(far_first):
                pass_on(t)

        reveal(last)
        others()

    y_table(0)
    sums(0)
    y_table(1)

    @pl.when(half == 0)
    def _():
        rise(0)

    sums(1)
    y_table(2)
    y_table(3)

    @pl.when(half == 1)
    def _():
        rise(0)

    def x_table():
        with scope("xtab"):
            xcode_copy.wait()
            make_table(xcode_ref[...], side * xt.shape[0], NX, xt, slice(None), xta, xtb, xfc, xfs)

    @pl.when(is_hub)
    def _():
        x_table()
        rise(1)
        sums(2)

        @pl.when(half == 1)
        def _():
            sums(3)

        gather(0)
        for m in range(pieces):
            partial_sum(0, m)

        @pl.when(half == 0)
        def _():
            sums(3)

        rise(2)
        rise(3)
        for k in range(chunks):
            more = k + 1 < chunks
            held = 0 if k + 2 == chunks else 1
            meet(k, 0)
            if more:
                gather(k + 1)
                for m in range(pieces // 2):
                    partial_sum(k + 1, m, held)
            meet(k, 1)
            if more:
                for m in range(pieces // 2, pieces):
                    partial_sum(k + 1, m, held)
            for m in range(2, pieces):
                meet(k, m)
            synthesis(k)
            if k == chunks - 2:
                @pl.when(half == 1)
                def _():
                    @pl.loop(0, pieces)
                    def _(m):
                        cross(chunks - 1, m).start()

            if k == chunks - 2:
                for early in range(chunks - 2):
                    take(early)

                @pl.when(half == 1)
                def _():
                    expand(0)

        forward(chunks - 1, spot, half).start()

        @pl.when(half == 0)
        def _():
            for k in range(chunks - 2):
                expand(k)

        take(chunks - 2)

        @pl.when(half == 1)
        def _():
            for k in range(1, chunks - 2):
                expand(k)

        expand(chunks - 2)
        finish()

    @pl.when(jnp.logical_not(is_hub))
    def _():
        sums(2)
        sums(3)
        rise(1)
        rise(2)
        rise(3)
        x_table()
        for k in range(last):
            receive(k)
            synthesis(k)
            if k > 0:
                take(k - 1)
                if k < last - 1:
                    expand(k - 1)

        @pl.when(half == 1)
        def _():
            expand(last - 2)

        @pl.when(half == 0)
        def _():
            for m in range(pieces):
                with scope("relaywait"):
                    relay(last, m).wait_recv()
                absorb(last, m)
                if m == 0:
                    with scope("fwdwait"):
                        all_forward(last - 2, peer).wait_recv()
                if m < pieces - 1:
                    for f in range(m * lead // (pieces - 1), (m + 1) * lead // (pieces - 1)):
                        add_field(last - 2, f)
            synthesis(last)
            forward(last, spot, half).start()

        take(last - 1)
        @pl.when(half == 0)
        def _():
            expand(last - 1)
            for t in reversed(far_first):
                pass_on(t)
            own_first()
            reveal(last)

        @pl.when(half == 1)
        def _():
            for t in [0] + far_first[::-1]:
                pass_on(t)
            expand(last - 1)
            own_first()
            all_found = found.at[last]
            with scope("showwait"):
                pltpu.make_async_remote_copy(
                    src_ref=all_found, dst_ref=all_found, send_sem=s6, recv_sem=r6.at[last],
                    device_id={"gx": own_base}).wait_recv()
            write_modes(last)

        others()

    with scope("drain"):
        sent(other, gs)
        sent(wide.at[:, :, :, pl.ds(0, LANES)], s4)
        sent(wide_last.at[:, :, pl.ds(0, 2 * LANES)], s4)

        @pl.when(is_hub)
        def _():
            sent(part.at[:, pl.ds(0, rows - x_local), :], s1)
            sent(s_out, s2)
            sent(found.at[:, pl.ds(0, lead - 1)], s6)
            sent(blocks.at[:, pl.ds(0, lead - 1)], s3)

            @pl.when(half == 0)
            def _():
                sent(coarse, s5)

            @pl.when(half == 1)
            def _():
                sent(coarse.at[pl.ds(0, last)], s5)
                sent(far, s7.at[0])
                sent(found.at[last], s7.at[1])

        @pl.when(jnp.logical_not(is_hub))
        def _():
            sent(part, s1)

            @pl.when(half == 0)
            def _():
                sent(found.at[:, pl.ds(0, lead - 1)], s6)
                sent(blocks.at[:, pl.ds(0, lead - 1)], s3)

            @pl.when(half == 1)
            def _():
                sent(found.at[pl.ds(0, last), pl.ds(0, lead - 1)], s6)
                sent(blocks.at[pl.ds(0, last), pl.ds(0, lead - 1)], s3)


def spectral_filter(lead, x_local, kx, ky, kpad, *operands):
    bf, f32 = jnp.bfloat16, jnp.float32
    operands = [pltpu.with_memory_space_constraint(a, pltpu.HBM) for a in operands]
    grid, x_codes, y_codes = operands
    y_local = grid.shape[1]
    rows, members, modes = lead * x_local, 2 * lead, x_codes.shape[1]
    chunks, pieces = kpad // LANES, 4
    tall_x, tall_y = members * x_local // STEP, y_local // STEP
    dma = pltpu.SemaphoreType.DMA
    vmem = pl.BlockSpec(memory_space=pltpu.VMEM)
    return pl.pallas_call(
        functools.partial(filter_kernel, lead, x_local, kx, ky, kpad),
        out_shape=(
            jax.ShapeDtypeStruct((lead * kx, ky), f32),
            jax.ShapeDtypeStruct((rows, y_local), f32),
            jax.ShapeDtypeStruct((lead, x_local, 4 * LANES), bf),
            jax.ShapeDtypeStruct((y_local, 4 * LANES), bf),
        ),
        in_specs=[pl.BlockSpec(memory_space=pltpu.HBM)] * 3,
        out_specs=(vmem,) * 4,
        scratch_shapes=[
            pltpu.VMEM((rows, y_local), bf),
            pltpu.VMEM(x_codes.shape, jnp.int32),
            pltpu.VMEM(y_codes.shape, jnp.int32),
            pltpu.VMEM((1, 2 * kpad), jnp.int32),
            pltpu.VMEM((chunks, 8, 2 * LANES), jnp.int32),
            pltpu.VMEM((chunks - 2, y_local, 2 * LANES), bf),
            pltpu.VMEM((tall_y, 2 * LANES), f32),
            pltpu.VMEM((tall_y, 2 * LANES), f32),
            pltpu.VMEM((STEP, 2 * LANES), f32),
            pltpu.VMEM((STEP, 2 * LANES), f32),
            pltpu.VMEM((chunks, rows, LANES), f32),
            pltpu.VMEM((chunks, rows, LANES), bf),
            pltpu.VMEM((chunks, rows, LANES), bf),
            pltpu.VMEM((chunks, rows, LANES), bf),
            pltpu.VMEM((chunks, members * x_local, LANES), bf),
            pltpu.VMEM((LANES, members * x_local), bf),
            pltpu.VMEM((members * x_local, modes), bf),
            pltpu.VMEM((tall_x, modes), f32),
            pltpu.VMEM((tall_x, modes), f32),
            pltpu.VMEM((STEP, modes), f32),
            pltpu.VMEM((STEP, modes), f32),
            pltpu.VMEM((chunks, modes, LANES), f32),
            pltpu.VMEM((chunks, modes, LANES), bf),
            pltpu.VMEM((chunks, modes, LANES), bf),
            pltpu.VMEM((chunks, modes, LANES), bf),
            pltpu.VMEM((chunks, lead, x_local, LANES), bf),
            pltpu.VMEM((chunks - 2, lead, x_local, 2 * LANES), bf),
            pltpu.VMEM((chunks, lead, kx, LANES), bf),
            pltpu.VMEM((lead, x_local, LANES), bf),
            dma, dma((chunks,)),
            dma, dma((chunks,)),
            dma, dma((chunks * pieces,)),
            dma, dma((chunks - 1 + lead,)),
            dma, dma((chunks - 1 + lead,)),
            dma, dma((chunks - 1 + pieces,)),
            dma, dma((chunks,)),
            dma((2,)),
            dma((2 + lead,)),
        ],
        compiler_params=pltpu.CompilerParams(
            collective_id=0, has_side_effects=True, vmem_limit_bytes=44 * 1024 * 1024
        ),
    )(*operands)


def last_sum_kernel(order, spec_in, low_in, wide_in, y_in, spec_out, low_out, total, sem):
    lead, x_local, _ = wide_in.shape
    spot = lax.rem(lax.axis_index("gx"), lead)
    spec_copy = pltpu.make_async_copy(spec_in, spec_out, sem.at[lead])

    def field(source, t):
        part = pl.ds(al(flipped(spot, t, lead) * x_local, x_local), x_local)
        return pltpu.make_async_copy(source.at[part, :], low_out.at[part, :], sem.at[t])

    field(low_in, 0).start()
    spec_copy.start()
    for t in order:
        f = flipped(spot, t, lead)
        part = pl.ds(al(f * x_local, x_local), x_local)
        total[part, :] = low_in[part, :] + lax.dot_general(
            wide_in[f], y_in[...], (((1,), (1,)), ((), ())), preferred_element_type=jnp.float32)
        field(total, t).start()
    field(low_in, 0).wait()
    for t in order:
        field(total, t).wait()
    spec_copy.wait()


def last_sum(spec, low, wide, y_table):
    lead = wide.shape[0]
    vmem, anywhere = pl.BlockSpec(memory_space=pltpu.VMEM), pl.BlockSpec(memory_space=pl.ANY)
    return pl.pallas_call(
        functools.partial(last_sum_kernel, near_first(lead)),
        out_shape=(jax.ShapeDtypeStruct(spec.shape, spec.dtype), jax.ShapeDtypeStruct(low.shape, low.dtype)),
        in_specs=[vmem] * 4,
        out_specs=(anywhere, anywhere),
        scratch_shapes=[pltpu.VMEM(low.shape, low.dtype), pltpu.SemaphoreType.DMA((lead + 1,))],
        compiler_params=pltpu.CompilerParams(vmem_limit_bytes=12 * 1024 * 1024),
    )(spec, low, wide, y_table)


def build(gx, gy):
    def local(fields, x_codes, y_codes):
        nf, nz, x_local, y_local = fields.shape
        lead = nf * nz
        ky = y_codes.shape[0] // gy
        kx = x_codes.shape[0] // gx
        unit = 128 * gx // math.gcd(128 * gx, lead)
        if unit > 2 * ky:
            unit = gx // math.gcd(gx, lead)
        kpad = -(-ky // unit) * unit
        cols = lead * kpad // gx
        me_y = lax.axis_index("gy")
        y_first = me_y * y_local
        grid = fields.reshape(lead * x_local, y_local)
        fits = gy == 2 and gx == 4 * lead and lead & (lead - 1) == 0 and kpad == 4 * LANES and kx % 16 == 0
        fits = fits and x_local % 16 == 0 and 2 * lead * x_local % (8 * STEP) == 0
        fits = fits and y_local % (8 * STEP) == 0 and gx * kx % (4 * LANES) == 0
        if fits:
            spec, low = last_sum(*spectral_filter(
                lead, x_local, kx, ky, kpad, grid, x_codes.reshape(1, -1), y_codes.reshape(1, -1)))
            return spec.reshape(nf, nz, kx, ky), low.reshape(nf, nz, x_local, y_local)
        padded = jnp.pad(y_codes.reshape(gy, ky), ((0, 0), (0, kpad - ky)))
        live = jnp.broadcast_to(jnp.arange(kpad)[None] < ky, (gy, kpad)).reshape(-1)
        x_tab = mode_table(x_codes, 0, x_local * gx, NX)
        y_tab = mode_table(padded.reshape(-1), y_first, y_local, NY, live)
        part = jnp.dot(grid, y_tab, preferred_element_type=jnp.float32).reshape(lead * x_local, gy, kpad)
        own = lax.dynamic_index_in_dim(part, me_y, 1, keepdims=False)
        for shift in range(1, gy):
            there = lax.rem(me_y + shift, gy)
            block = lax.dynamic_index_in_dim(part, there, 1, keepdims=False).astype(jnp.bfloat16)
            got = lax.ppermute(block, "gy", [(i, (i + shift) % gy) for i in range(gy)])
            own = own + got.astype(jnp.float32)
        send = own.astype(jnp.bfloat16).reshape(lead, x_local, kpad)
        if cols <= kpad:
            def spread(a):
                n = a.shape[1]
                return a.reshape(lead, n, kpad // cols, cols).transpose(0, 2, 1, 3).reshape(gx, n, cols)

            def merge(a):
                n = a.shape[1]
                return a.reshape(lead, kpad // cols, n, cols).transpose(0, 2, 1, 3).reshape(lead, n, kpad)
        else:
            def spread(a):
                n = a.shape[1]
                return a.transpose(1, 0, 2).reshape(n, gx, cols).transpose(1, 0, 2)

            def merge(a):
                n = a.shape[1]
                return a.transpose(1, 0, 2).reshape(n, lead, kpad).transpose(1, 0, 2)
        lines = lax.all_to_all(spread(send), "gx", split_axis=0, concat_axis=0, tiled=True)
        lines = lines.reshape(gx * x_local, cols)
        modes = lax.dot_general(x_tab, lines, (((0,), (0,)), ((), ())), preferred_element_type=jnp.float32)
        coarse = modes.astype(jnp.bfloat16)
        synth = jnp.dot(x_tab, coarse, preferred_element_type=jnp.float32).astype(jnp.bfloat16)
        back = lax.all_to_all(synth.reshape(gx, x_local, cols), "gx", split_axis=0, concat_axis=0, tiled=True)
        spec = lax.all_to_all(coarse.reshape(gx, kx, cols), "gx", split_axis=0, concat_axis=0, tiled=True)
        spectrum = merge(spec)[:, :, :ky].astype(jnp.float32).reshape(nf, nz, kx, ky)
        mine = merge(back).reshape(lead * x_local, kpad)
        y_parts = y_tab.reshape(y_local, gy, kpad)
        whole = jnp.zeros((gy, lead * x_local, kpad), jnp.bfloat16)
        whole = lax.dynamic_update_index_in_dim(whole, mine, me_y, 0)
        for shift in range(1, gy):
            got = lax.ppermute(mine, "gy", [(i, (i + shift) % gy) for i in range(gy)])
            whole = lax.dynamic_update_index_in_dim(whole, got, lax.rem(me_y + gy - shift, gy), 0)
        wide = whole.transpose(1, 0, 2).reshape(lead * x_local, gy * kpad)
        low = lax.dot_general(wide, y_tab, (((1,), (1,)), ((), ())), preferred_element_type=jnp.float32)
        return spectrum, low.reshape(nf, nz, x_local, y_local)

    return local


def solution(mesh):
    return jax.shard_map(
        build(mesh.shape["gx"], mesh.shape["gy"]),
        mesh=mesh,
        in_specs=(P(None, None, "gx", "gy"), P(), P()),
        out_specs=(P(None, None, "gx", "gy"), P(None, None, "gx", "gy")),
        check_vma=False,
    )
```

```python
import functools
import math

import jax
import jax.numpy as jnp
from jax import lax
from jax.experimental import pallas as pl
from jax.experimental.pallas import tpu as pltpu
from jax.sharding import PartitionSpec as P

NX = 3072
NY = 3072
BAND = 512
STEP = 64


def angle(freq, position, length):
    phase = freq[None, :] * position[:, None] % length
    return phase.astype(jnp.float32) * (2.0 * math.pi / length)


def mode_parts(picked, first, amount, length, live=None):
    step = 64 if amount % 64 == 0 else 8
    freq = jnp.where(picked <= BAND, picked, picked - BAND)
    coarse_angle = angle(freq, first + step * jnp.arange(amount // step, dtype=jnp.int32), length)
    fine_angle = angle(freq, jnp.arange(step, dtype=jnp.int32), length)
    norm = jnp.where(picked == 0, 1.0 / math.sqrt(length), math.sqrt(2.0 / length)).astype(jnp.float32)
    if live is not None:
        norm = jnp.where(live, norm, 0.0)
    is_cos = (picked <= BAND)[None, :]
    c, s = jnp.cos(coarse_angle), jnp.sin(coarse_angle)
    first_part = jnp.where(is_cos, c, s) * norm[None, :]
    second_part = jnp.where(is_cos, -s, c) * norm[None, :]
    fc, fs = jnp.cos(fine_angle), jnp.sin(fine_angle)
    return lax.optimization_barrier((first_part, second_part, fc, fs))


def mode_table(picked, first, amount, length, live=None):
    first_part, second_part, fc, fs = mode_parts(picked, first, amount, length, live)
    table = first_part[:, None, :] * fc[None] + second_part[:, None, :] * fs[None]
    return table.astype(jnp.bfloat16).reshape(amount, picked.shape[0])


def al(v, m):
    return pl.multiple_of(v, m)


def turn(freq, position, shift, length):
    product = freq * position
    quarter = jnp.floor(product * (4.0 / length) + 0.5)
    x = (product * 4.0 - quarter * length) * (2.0 * math.pi / (4 * length))
    x2 = x * x
    s = x + x * x2 * (-1 / 6 + x2 * (1 / 120 + x2 * (-1 / 5040 + x2 * (1 / 362880))))
    c = 1.0 + x2 * (-0.5 + x2 * (1 / 24 + x2 * (-1 / 720 + x2 * (1 / 40320))))
    quarter = quarter - shift
    q = quarter - 4.0 * jnp.floor(quarter * 0.25)
    odd = (q == 1.0) | (q == 3.0)
    cos_value, sin_value = jnp.where(odd, s, c), jnp.where(odd, c, s)
    cos_value = jnp.where((q == 1.0) | (q == 2.0), -cos_value, cos_value)
    return cos_value, jnp.where(q >= 2.0, -sin_value, sin_value)


LANES = 128


def make_table(code, first, length, table, side, ta, tb, fc, fs):
    amount, codes = table.shape[0], code.shape[1]
    f32 = jnp.float32
    freq = jnp.where(code <= BAND, code, code - BAND).astype(f32)
    shift = jnp.where(code <= BAND, 0, 1).astype(f32)
    norm = jnp.where(code == 0, 1.0 / math.sqrt(length), math.sqrt(2.0 / length)).astype(f32)
    norm = jnp.where(code < 0, 0.0, norm)
    row = lax.broadcasted_iota(jnp.int32, (8, codes), 0)

    @pl.loop(0, amount // STEP // 8)
    def _(i):
        c, s = turn(freq, (first + (row + i * 8) * STEP).astype(f32), shift, length)
        ta[pl.ds(al(i * 8, 8), 8), :] = c * norm
        tb[pl.ds(al(i * 8, 8), 8), :] = s * norm

    @pl.loop(0, STEP // 8)
    def _(i):
        c, s = turn(freq, (row + i * 8).astype(f32), 0.0, length)
        fc[pl.ds(al(i * 8, 8), 8), :] = c
        fs[pl.ds(al(i * 8, 8), 8), :] = s

    @pl.loop(0, amount // STEP)
    def _(h):
        table[pl.ds(al(h * STEP, STEP), STEP), side] = (
            ta[pl.ds(h, 1), :] * fc[...] - tb[pl.ds(h, 1), :] * fs[...]
        ).astype(jnp.bfloat16)


def flipped(spot, t, lead):
    f = spot
    for bit in range(lead.bit_length()):
        if t >> bit & 1:
            f = f + (1 << bit) - (2 << bit) * lax.rem(f // (1 << bit), 2)
    return f


def near_first(lead):
    return sorted(range(lead - 1, 0, -1), key=lambda t: bin(t).count("1"))


def filter_kernel(
    lead, x_local, kx, ky, kpad,
    grid_in, xcode_in, ycode_in, spec_ref, low_ref, wide_last, y_last,
    grid_ref, xcode_ref, ycode_ref, y_raw, y_codes, y_ref, yta, ytb, yfc, yfs, own, other, inc, part, lines, turned, xt, xta, xtb, xfc, xfs,
    s_own, s_out, s_in, coarse, blocks, wide, found, far,
    gs, gr, s1, r1, s2, r2, s3, r3, s4, r4, s5, r5, s6, r6, s7, in_sem,
):
    me = lax.axis_index("gx")
    half = lax.axis_index("gy")
    peer = 1 - half
    bf, f32 = jnp.bfloat16, jnp.float32
    scope = jax.named_scope
    chunks = kpad // LANES
    members = 2 * lead
    modes = xt.shape[1]
    pieces = r2.shape[0] // chunks
    piece = modes // pieces
    rows = lead * x_local
    plane, spot = me // lead, lax.rem(me, lead)
    side = plane // 2
    base = side * members
    mine = me - base
    hub_base = base + (1 - side) * lead
    end_base = base + side * lead
    own_base = plane * lead
    is_hub = plane == 1 + side
    across = (2 - side) * lead + spot

    def grid_copy(f):
        part = pl.ds(al(f * x_local, x_local), x_local)
        return pltpu.make_async_copy(grid_in.at[part, :], grid_ref.at[part, :], in_sem.at[2 + f])

    ycode_copy = pltpu.make_async_copy(ycode_in, ycode_ref, in_sem.at[0])
    xcode_copy = pltpu.make_async_copy(xcode_in, xcode_ref, in_sem.at[1])
    ycode_copy.start()
    for f in range(lead):
        grid_copy(f).start()
    xcode_copy.start()
    barrier = pltpu.get_barrier_semaphore()
    pl.semaphore_signal(barrier, inc=1, device_id={"gy": peer})

    @pl.loop(1, members)
    def _(t):
        pl.semaphore_signal(barrier, inc=1, device_id={"gx": base + lax.rem(mine + t, members)})

    @pl.when(is_hub)
    def _():
        pl.semaphore_signal(barrier, inc=1, device_id={"gx": across})

    def mate(t):
        return flipped(spot, t, lead)

    far_first = near_first(lead)[::-1]
    last = chunks - 1

    def slot(k, i):
        return k if k < last else last + i

    def late(k):
        return pl.ds((k - chunks + 2) * 2 * LANES, 2 * LANES)

    def wide_at(k, who):
        if k >= chunks - 2:
            return wide_last, pl.ds(al((2 * (k - chunks + 2) + who) * LANES, LANES), LANES)
        return wide.at[k], span(who, LANES)

    def wide_row(k, f, who):
        ref, columns = wide_at(k, who)
        return ref.at[f, :, columns]

    def both_halves(k, f):
        return wide_last[f, :, late(k)] if k >= chunks - 2 else wide[k, f]

    def y_place(k):
        return (y_last, late(k)) if k >= chunks - 2 else (y_ref.at[k], slice(None))

    def y_at(k):
        ref, columns = y_place(k)
        return ref[:, columns]

    def span(i, n):
        return pl.ds(al(i * n, n), n)

    def swap(k):
        return pltpu.make_async_remote_copy(
            src_ref=other.at[k], dst_ref=inc.at[k], send_sem=gs, recv_sem=gr.at[k], device_id={"gy": peer})

    def up(k, f):
        return pltpu.make_async_remote_copy(
            src_ref=part.at[k, span(f, x_local), :], dst_ref=lines.at[k, span(mine, x_local), :],
            send_sem=s1, recv_sem=r1.at[k], device_id={"gx": hub_base + f})

    def up_in(k):
        taken = lines.at[k, pl.ds(0, (members - 1) * x_local), :]
        return pltpu.make_async_remote_copy(
            src_ref=taken, dst_ref=taken, send_sem=s1, recv_sem=r1.at[k], device_id={"gx": hub_base})

    def sent(view, sem):
        pltpu.make_async_remote_copy(
            src_ref=view, dst_ref=view, send_sem=sem, recv_sem=gr.at[0], device_id={"gy": peer}).wait_send()

    def cross(k, m):
        return pltpu.make_async_remote_copy(
            src_ref=s_out.at[k, span(m, piece), :], dst_ref=s_in.at[k, span(m, piece), :],
            send_sem=s2, recv_sem=r2.at[k * pieces + m], device_id={"gx": across})

    def relay(k, m):
        view = coarse.at[k, span(m, piece), :]
        return pltpu.make_async_remote_copy(
            src_ref=view, dst_ref=view, send_sem=s5, recv_sem=r5.at[slot(k, m)],
            device_id={"gx": end_base + spot})

    def down(k, f):
        return pltpu.make_async_remote_copy(
            src_ref=blocks.at[k, f], dst_ref=wide_row(k, spot, half),
            send_sem=s3, recv_sem=r3.at[slot(k, spot)], device_id={"gx": own_base + f})

    def show(k, f):
        return pltpu.make_async_remote_copy(
            src_ref=coarse.at[k, span(own_base + f, kx), :], dst_ref=found.at[k, spot],
            send_sem=s6, recv_sem=r6.at[k], device_id={"gx": own_base + f})

    def show_in(k):
        view = found.at[k, pl.ds(0, lead - 1)]
        return pltpu.make_async_remote_copy(
            src_ref=view, dst_ref=view, send_sem=s6, recv_sem=r6.at[k], device_id={"gx": own_base})

    def down_in(k, f):
        return pltpu.make_async_remote_copy(
            src_ref=blocks.at[k, 0], dst_ref=wide_row(k, f, half),
            send_sem=s3, recv_sem=r3.at[slot(k, f)], device_id={"gx": own_base + f})

    def all_down(k):
        ref, columns = wide_at(k, half)
        view = ref.at[pl.ds(0, lead - 1), :, columns]
        return pltpu.make_async_remote_copy(
            src_ref=view, dst_ref=view, send_sem=s3, recv_sem=r3.at[k], device_id={"gx": own_base})

    def all_forward(k, who):
        ref, columns = wide_at(k, who)
        place = ref.at[:, :, columns]
        return pltpu.make_async_remote_copy(
            src_ref=place, dst_ref=place, send_sem=s4, recv_sem=r4.at[k], device_id={"gy": peer})

    def all_relayed(k):
        view = coarse.at[k]
        return pltpu.make_async_remote_copy(
            src_ref=view, dst_ref=view, send_sem=s5, recv_sem=r5.at[k], device_id={"gx": hub_base})

    def forward(k, f, who):
        place = wide_row(k, f, who)
        return pltpu.make_async_remote_copy(
            src_ref=place, dst_ref=place, send_sem=s4, recv_sem=r4.at[slot(k, f)],
            device_id={"gy": peer})

    def local(f):
        return is_hub & (f == spot)

    width = chunks * LANES * 2
    y_raw[...] = jnp.full(y_raw.shape, -1, jnp.int32)
    with scope("codewait"):
        ycode_copy.wait()
    y_raw[:, : 2 * ky] = ycode_ref[...]
    first_half = jnp.broadcast_to(y_raw[...], (8, width))
    second_half = pltpu.roll(first_half, width - ky, 1)
    live = lax.broadcasted_iota(jnp.int32, (8, width), 1) < ky
    first_half = jnp.where(live, first_half, -1)
    second_half = jnp.where(live, second_half, -1)
    for k in range(chunks):
        y_codes[k, :, :LANES] = first_half[:, k * LANES : (k + 1) * LANES]
        y_codes[k, :, LANES:] = second_half[:, k * LANES : (k + 1) * LANES]

    def y_table(k):
        with scope("ytab"):
            make_table(y_codes[k, :1, :], half * grid_ref.shape[1], NY, *y_place(k), yta, ytb, yfc, yfs)

    def field_sums(k, part):
        both = jnp.dot(grid_ref[part, :], y_at(k), preferred_element_type=f32)
        low_part, high_part = both[:, :LANES], both[:, LANES:]
        other[k, part, :] = jnp.where(half == 0, high_part, low_part).astype(bf)
        own[k, part, :] = jnp.where(half == 0, low_part, high_part)

    def sums(k):
        if k == 0:
            @pl.loop(0, lead)
            def _(f):
                with scope("gridwait"):
                    grid_copy(f).wait()
                with scope("dotA"):
                    field_sums(k, span(f, x_local))
        else:
            with scope("dotA"):
                field_sums(k, pl.ds(0, rows))
        if k == 0:
            with scope("barrier"):
                pl.semaphore_wait(barrier, members + jnp.where(is_hub, 1, 0))
        swap(k).start()

    def rise(k):
        with scope("swapwait"):
            swap(k).wait_recv()
        part[k] = (own[k] + inc[k].astype(f32)).astype(bf)

        for t in far_first:
            up(k, mate(t)).start()

        @pl.when(jnp.logical_not(is_hub))
        def _():
            up(k, spot).start()

        @pl.when(is_hub)
        def _():
            lines[k, span(mine, x_local), :] = part[k, span(spot, x_local), :]

    def gather(k):
        with scope("upwait"):
            up_in(k).wait_recv()

        with scope("dotB"):
            turned[...] = lines[k].T

    def partial_sum(k, m, held=1):
        with scope("dotB"):
            got = jnp.dot(turned[...], xt[:, pl.ds(m * piece, piece)], preferred_element_type=f32).T
            s_own[k, pl.ds(m * piece, piece), :] = got
            s_out[k, pl.ds(m * piece, piece), :] = got.astype(bf)

        @pl.when(half <= held)
        def _():
            cross(k, m).start()

    mine_x = span(plane - 2 * side, rows)

    def share(k):
        for t in far_first:
            show(k, mate(t)).start()
        found[k, spot] = coarse[k, span(me, kx), :]

    far_plane = 3 * side
    far_x = span(far_plane - 2 * side, rows)

    def throw(f):
        return pltpu.make_async_remote_copy(
            src_ref=far.at[f], dst_ref=wide_row(last, spot, half),
            send_sem=s7.at[0], recv_sem=r3.at[slot(last, spot)], device_id={"gx": far_plane * lead + f})

    def throw_modes():
        for t in far_first + [0]:
            f = mate(t)
            pltpu.make_async_remote_copy(
                src_ref=coarse.at[last, span(far_plane * lead + f, kx), :], dst_ref=found.at[last, spot],
                send_sem=s7.at[1], recv_sem=r6.at[last], device_id={"gx": far_plane * lead + f}).start()

    def absorb_far(m):
        if m < pieces - 1:
            @pl.when(far_plane == m)
            def _():
                throw_modes()

        with scope("dotF"):
            got = jnp.dot(
                xt[far_x, pl.ds(m * piece, piece)], coarse[last, pl.ds(m * piece, piece), :],
                preferred_element_type=f32)
            if m < pieces - 1:
                own[1] = got if m == 0 else own[1] + got
            else:
                far[...] = (own[1] + got).astype(bf).reshape(lead, x_local, LANES)
                for t in far_first + [0]:
                    throw(mate(t)).start()

                @pl.when(far_plane == m)
                def _():
                    throw_modes()

    def absorb(k, m):
        if m < pieces - 1:
            @pl.when(plane == m)
            def _():
                share(k)

        if k == chunks - 1:
            with scope("dotC"):
                got = jnp.dot(
                    xt[mine_x, pl.ds(m * piece, piece)], coarse[k, pl.ds(m * piece, piece), :],
                    preferred_element_type=f32)
                own[0] = got if m == 0 else own[0] + got

    def meet(k, m):
        with scope("crosswait"):
            cross(k, m).wait_recv()
        part_of = pl.ds(m * piece, piece)
        coarse[k, part_of, :] = (s_own[k, part_of, :] + s_in[k, part_of, :].astype(f32)).astype(bf)
        if k < last:
            relay(k, m).start()
        else:
            @pl.when(half == 0)
            def _():
                relay(k, m).start()

            @pl.when(half == 1)
            def _():
                absorb_far(m)

        absorb(k, m)

    def receive(k):
        if k < last:
            with scope("relaywait"):
                all_relayed(k).wait_recv()
        for m in range(pieces):
            if k == last:
                with scope("relaywait"):
                    relay(k, m).wait_recv()
            absorb(k, m)

    def synthesis(k):
        if k < chunks - 1:
            with scope("dotC"):
                syn = jnp.dot(xt[mine_x, :], coarse[k], preferred_element_type=f32)
        else:
            syn = own[0]
        blocks[k] = syn.astype(bf).reshape(lead, x_local, LANES)

        for t in far_first:
            down(k, mate(t)).start()

        ref, columns = wide_at(k, half)
        ref[spot, :, columns] = blocks[k, spot]

        @pl.when(plane == pieces - 1)
        def _():
            share(k)

    def reveal(k):
        with scope("showwait"):
            show_in(k).wait_recv()
        write_modes(k)

    def write_modes(k):
        columns = min(LANES, ky - k * LANES)
        spec_ref[:, pl.ds(k * LANES, columns)] = (
            found[k].reshape(lead * kx, LANES)[:, :columns].astype(f32))

    def add_field(k, f):
        with scope("dotD"):
            got = lax.dot_general(
                both_halves(k, f), y_at(k), (((1,), (1,)), ((), ())), preferred_element_type=f32)
            if k > 0:
                got = got + low_ref[span(f, x_local), :]
            low_ref[span(f, x_local), :] = got

    def take(k):
        with scope("downwait"):
            all_down(k).wait_recv()
        all_forward(k, half).start()
        reveal(k)

    def expand(k):
        with scope("fwdwait"):
            all_forward(k, peer).wait_recv()

        if k == last - 1:
            add_field(k, spot)
            return

        @pl.loop(0, lead)
        def _(f):
            add_field(k, f)

    def own_first():
        with scope("fwdwait"):
            forward(last, spot, peer).wait_recv()
        add_field(last, spot)

    def pass_on(t):
        with scope("downwait"):
            down_in(last, mate(t)).wait_recv()
        forward(last, mate(t), half).start()

    def others():
        with scope("fwdwait"):
            for t in reversed(far_first):
                forward(last, mate(t), peer).wait_recv()

    def finish():
        @pl.when(half == 0)
        def _():
            for t in reversed(far_first):
                pass_on(t)
            own_first()

        @pl.when(half == 1)
        def _():
            own_first()
            for t in reversed(far_first):
                pass_on(t)

        reveal(last)
        others()

    y_table(0)
    sums(0)
    y_table(1)

    @pl.when(half == 0)
    def _():
        rise(0)

    sums(1)
    y_table(2)
    y_table(3)

    @pl.when(half == 1)
    def _():
        rise(0)

    def x_table():
        with scope("xtab"):
            xcode_copy.wait()
            make_table(xcode_ref[...], side * xt.shape[0], NX, xt, slice(None), xta, xtb, xfc, xfs)

    @pl.when(is_hub)
    def _():
        x_table()
        rise(1)
        sums(2)

        @pl.when(half == 1)
        def _():
            sums(3)

        rise(2)
        gather(0)
        for m in range(pieces):
            partial_sum(0, m)

        @pl.when(half == 0)
        def _():
            sums(3)

        rise(3)
        for k in range(chunks):
            more = k + 1 < chunks
            held = 0 if k + 2 == chunks else 1
            meet(k, 0)
            if k == 0:
                @pl.when(half == 0)
                def _():
                    meet(0, 1)

            if more:
                gather(k + 1)
                for m in range(pieces // 2):
                    partial_sum(k + 1, m, held)
            if k == 0:
                @pl.when(half == 1)
                def _():
                    meet(0, 1)
            else:
                meet(k, 1)
            if more:
                for m in range(pieces // 2, pieces):
                    partial_sum(k + 1, m, held)
            for m in range(2, pieces):
                meet(k, m)
            synthesis(k)
            if k == chunks - 2:
                @pl.when(half == 1)
                def _():
                    @pl.loop(0, pieces)
                    def _(m):
                        cross(chunks - 1, m).start()

            if k == chunks - 2:
                for early in range(chunks - 2):
                    take(early)

                @pl.when(half == 1)
                def _():
                    expand(0)

        forward(chunks - 1, spot, half).start()

        @pl.when(half == 0)
        def _():
            for k in range(chunks - 2):
                expand(k)

        take(chunks - 2)

        @pl.when(half == 1)
        def _():
            for k in range(1, chunks - 2):
                expand(k)

        expand(chunks - 2)
        finish()

    @pl.when(jnp.logical_not(is_hub))
    def _():
        sums(2)
        sums(3)
        rise(1)
        rise(2)
        rise(3)
        x_table()
        for k in range(last):
            receive(k)
            synthesis(k)
            if k > 0:
                take(k - 1)
                if k < last - 1:
                    expand(k - 1)

        @pl.when(half == 1)
        def _():
            expand(last - 2)

        @pl.when(half == 0)
        def _():
            for m in range(pieces):
                with scope("relaywait"):
                    relay(last, m).wait_recv()
                absorb(last, m)
                if m == 0:
                    with scope("fwdwait"):
                        all_forward(last - 2, peer).wait_recv()
                if m < pieces - 1:
                    for f in range(m * lead // (pieces - 1), (m + 1) * lead // (pieces - 1)):
                        add_field(last - 2, f)
            synthesis(last)
            forward(last, spot, half).start()

        take(last - 1)
        @pl.when(half == 0)
        def _():
            expand(last - 1)
            for t in reversed(far_first):
                pass_on(t)
            own_first()
            reveal(last)

        @pl.when(half == 1)
        def _():
            for t in [0] + far_first[::-1]:
                pass_on(t)
            expand(last - 1)
            own_first()
            all_found = found.at[last]
            with scope("showwait"):
                pltpu.make_async_remote_copy(
                    src_ref=all_found, dst_ref=all_found, send_sem=s6, recv_sem=r6.at[last],
                    device_id={"gx": own_base}).wait_recv()
            write_modes(last)

        others()

    with scope("drain"):
        sent(other, gs)
        sent(wide.at[:, :, :, pl.ds(0, LANES)], s4)
        sent(wide_last.at[:, :, pl.ds(0, 2 * LANES)], s4)

        @pl.when(is_hub)
        def _():
            sent(part.at[:, pl.ds(0, rows - x_local), :], s1)
            sent(s_out, s2)
            sent(found.at[:, pl.ds(0, lead - 1)], s6)
            sent(blocks.at[:, pl.ds(0, lead - 1)], s3)

            @pl.when(half == 0)
            def _():
                sent(coarse, s5)

            @pl.when(half == 1)
            def _():
                sent(coarse.at[pl.ds(0, last)], s5)
                sent(far, s7.at[0])
                sent(found.at[last], s7.at[1])

        @pl.when(jnp.logical_not(is_hub))
        def _():
            sent(part, s1)

            @pl.when(half == 0)
            def _():
                sent(found.at[:, pl.ds(0, lead - 1)], s6)
                sent(blocks.at[:, pl.ds(0, lead - 1)], s3)

            @pl.when(half == 1)
            def _():
                sent(found.at[pl.ds(0, last), pl.ds(0, lead - 1)], s6)
                sent(blocks.at[pl.ds(0, last), pl.ds(0, lead - 1)], s3)


def spectral_filter(lead, x_local, kx, ky, kpad, *operands):
    bf, f32 = jnp.bfloat16, jnp.float32
    operands = [pltpu.with_memory_space_constraint(a, pltpu.HBM) for a in operands]
    grid, x_codes, y_codes = operands
    y_local = grid.shape[1]
    rows, members, modes = lead * x_local, 2 * lead, x_codes.shape[1]
    chunks, pieces = kpad // LANES, 4
    tall_x, tall_y = members * x_local // STEP, y_local // STEP
    dma = pltpu.SemaphoreType.DMA
    vmem = pl.BlockSpec(memory_space=pltpu.VMEM)
    return pl.pallas_call(
        functools.partial(filter_kernel, lead, x_local, kx, ky, kpad),
        out_shape=(
            jax.ShapeDtypeStruct((lead * kx, ky), f32),
            jax.ShapeDtypeStruct((rows, y_local), f32),
            jax.ShapeDtypeStruct((lead, x_local, 4 * LANES), bf),
            jax.ShapeDtypeStruct((y_local, 4 * LANES), bf),
        ),
        in_specs=[pl.BlockSpec(memory_space=pltpu.HBM)] * 3,
        out_specs=(vmem,) * 4,
        scratch_shapes=[
            pltpu.VMEM((rows, y_local), bf),
            pltpu.VMEM(x_codes.shape, jnp.int32),
            pltpu.VMEM(y_codes.shape, jnp.int32),
            pltpu.VMEM((1, 2 * kpad), jnp.int32),
            pltpu.VMEM((chunks, 8, 2 * LANES), jnp.int32),
            pltpu.VMEM((chunks - 2, y_local, 2 * LANES), bf),
            pltpu.VMEM((tall_y, 2 * LANES), f32),
            pltpu.VMEM((tall_y, 2 * LANES), f32),
            pltpu.VMEM((STEP, 2 * LANES), f32),
            pltpu.VMEM((STEP, 2 * LANES), f32),
            pltpu.VMEM((chunks, rows, LANES), f32),
            pltpu.VMEM((chunks, rows, LANES), bf),
            pltpu.VMEM((chunks, rows, LANES), bf),
            pltpu.VMEM((chunks, rows, LANES), bf),
            pltpu.VMEM((chunks, members * x_local, LANES), bf),
            pltpu.VMEM((LANES, members * x_local), bf),
            pltpu.VMEM((members * x_local, modes), bf),
            pltpu.VMEM((tall_x, modes), f32),
            pltpu.VMEM((tall_x, modes), f32),
            pltpu.VMEM((STEP, modes), f32),
            pltpu.VMEM((STEP, modes), f32),
            pltpu.VMEM((chunks, modes, LANES), f32),
            pltpu.VMEM((chunks, modes, LANES), bf),
            pltpu.VMEM((chunks, modes, LANES), bf),
            pltpu.VMEM((chunks, modes, LANES), bf),
            pltpu.VMEM((chunks, lead, x_local, LANES), bf),
            pltpu.VMEM((chunks - 2, lead, x_local, 2 * LANES), bf),
            pltpu.VMEM((chunks, lead, kx, LANES), bf),
            pltpu.VMEM((lead, x_local, LANES), bf),
            dma, dma((chunks,)),
            dma, dma((chunks,)),
            dma, dma((chunks * pieces,)),
            dma, dma((chunks - 1 + lead,)),
            dma, dma((chunks - 1 + lead,)),
            dma, dma((chunks - 1 + pieces,)),
            dma, dma((chunks,)),
            dma((2,)),
            dma((2 + lead,)),
        ],
        compiler_params=pltpu.CompilerParams(
            collective_id=0, has_side_effects=True, vmem_limit_bytes=44 * 1024 * 1024
        ),
    )(*operands)


def last_sum_kernel(order, spec_in, low_in, wide_in, y_in, spec_out, low_out, total, sem):
    lead, x_local, _ = wide_in.shape
    spot = lax.rem(lax.axis_index("gx"), lead)
    spec_copy = pltpu.make_async_copy(spec_in, spec_out, sem.at[lead])

    def field(source, t):
        part = pl.ds(al(flipped(spot, t, lead) * x_local, x_local), x_local)
        return pltpu.make_async_copy(source.at[part, :], low_out.at[part, :], sem.at[t])

    field(low_in, 0).start()
    spec_copy.start()
    for t in order:
        f = flipped(spot, t, lead)
        part = pl.ds(al(f * x_local, x_local), x_local)
        total[part, :] = low_in[part, :] + lax.dot_general(
            wide_in[f], y_in[...], (((1,), (1,)), ((), ())), preferred_element_type=jnp.float32)
        field(total, t).start()
    field(low_in, 0).wait()
    for t in order:
        field(total, t).wait()
    spec_copy.wait()


def last_sum(spec, low, wide, y_table):
    lead = wide.shape[0]
    vmem, anywhere = pl.BlockSpec(memory_space=pltpu.VMEM), pl.BlockSpec(memory_space=pl.ANY)
    return pl.pallas_call(
        functools.partial(last_sum_kernel, near_first(lead)),
        out_shape=(jax.ShapeDtypeStruct(spec.shape, spec.dtype), jax.ShapeDtypeStruct(low.shape, low.dtype)),
        in_specs=[vmem] * 4,
        out_specs=(anywhere, anywhere),
        scratch_shapes=[pltpu.VMEM(low.shape, low.dtype), pltpu.SemaphoreType.DMA((lead + 1,))],
        compiler_params=pltpu.CompilerParams(vmem_limit_bytes=12 * 1024 * 1024),
    )(spec, low, wide, y_table)


def build(gx, gy):
    def local(fields, x_codes, y_codes):
        nf, nz, x_local, y_local = fields.shape
        lead = nf * nz
        ky = y_codes.shape[0] // gy
        kx = x_codes.shape[0] // gx
        unit = 128 * gx // math.gcd(128 * gx, lead)
        if unit > 2 * ky:
            unit = gx // math.gcd(gx, lead)
        kpad = -(-ky // unit) * unit
        cols = lead * kpad // gx
        me_y = lax.axis_index("gy")
        y_first = me_y * y_local
        grid = fields.reshape(lead * x_local, y_local)
        fits = gy == 2 and gx == 4 * lead and lead & (lead - 1) == 0 and kpad == 4 * LANES and kx % 16 == 0
        fits = fits and x_local % 16 == 0 and 2 * lead * x_local % (8 * STEP) == 0
        fits = fits and y_local % (8 * STEP) == 0 and gx * kx % (4 * LANES) == 0
        if fits:
            spec, low = last_sum(*spectral_filter(
                lead, x_local, kx, ky, kpad, grid, x_codes.reshape(1, -1), y_codes.reshape(1, -1)))
            return spec.reshape(nf, nz, kx, ky), low.reshape(nf, nz, x_local, y_local)
        padded = jnp.pad(y_codes.reshape(gy, ky), ((0, 0), (0, kpad - ky)))
        live = jnp.broadcast_to(jnp.arange(kpad)[None] < ky, (gy, kpad)).reshape(-1)
        x_tab = mode_table(x_codes, 0, x_local * gx, NX)
        y_tab = mode_table(padded.reshape(-1), y_first, y_local, NY, live)
        part = jnp.dot(grid, y_tab, preferred_element_type=jnp.float32).reshape(lead * x_local, gy, kpad)
        own = lax.dynamic_index_in_dim(part, me_y, 1, keepdims=False)
        for shift in range(1, gy):
            there = lax.rem(me_y + shift, gy)
            block = lax.dynamic_index_in_dim(part, there, 1, keepdims=False).astype(jnp.bfloat16)
            got = lax.ppermute(block, "gy", [(i, (i + shift) % gy) for i in range(gy)])
            own = own + got.astype(jnp.float32)
        send = own.astype(jnp.bfloat16).reshape(lead, x_local, kpad)
        if cols <= kpad:
            def spread(a):
                n = a.shape[1]
                return a.reshape(lead, n, kpad // cols, cols).transpose(0, 2, 1, 3).reshape(gx, n, cols)

            def merge(a):
                n = a.shape[1]
                return a.reshape(lead, kpad // cols, n, cols).transpose(0, 2, 1, 3).reshape(lead, n, kpad)
        else:
            def spread(a):
                n = a.shape[1]
                return a.transpose(1, 0, 2).reshape(n, gx, cols).transpose(1, 0, 2)

            def merge(a):
                n = a.shape[1]
                return a.transpose(1, 0, 2).reshape(n, lead, kpad).transpose(1, 0, 2)
        lines = lax.all_to_all(spread(send), "gx", split_axis=0, concat_axis=0, tiled=True)
        lines = lines.reshape(gx * x_local, cols)
        modes = lax.dot_general(x_tab, lines, (((0,), (0,)), ((), ())), preferred_element_type=jnp.float32)
        coarse = modes.astype(jnp.bfloat16)
        synth = jnp.dot(x_tab, coarse, preferred_element_type=jnp.float32).astype(jnp.bfloat16)
        back = lax.all_to_all(synth.reshape(gx, x_local, cols), "gx", split_axis=0, concat_axis=0, tiled=True)
        spec = lax.all_to_all(coarse.reshape(gx, kx, cols), "gx", split_axis=0, concat_axis=0, tiled=True)
        spectrum = merge(spec)[:, :, :ky].astype(jnp.float32).reshape(nf, nz, kx, ky)
        mine = merge(back).reshape(lead * x_local, kpad)
        y_parts = y_tab.reshape(y_local, gy, kpad)
        whole = jnp.zeros((gy, lead * x_local, kpad), jnp.bfloat16)
        whole = lax.dynamic_update_index_in_dim(whole, mine, me_y, 0)
        for shift in range(1, gy):
            got = lax.ppermute(mine, "gy", [(i, (i + shift) % gy) for i in range(gy)])
            whole = lax.dynamic_update_index_in_dim(whole, got, lax.rem(me_y + gy - shift, gy), 0)
        wide = whole.transpose(1, 0, 2).reshape(lead * x_local, gy * kpad)
        low = lax.dot_general(wide, y_tab, (((1,), (1,)), ((), ())), preferred_element_type=jnp.float32)
        return spectrum, low.reshape(nf, nz, x_local, y_local)

    return local


def solution(mesh):
    return jax.shard_map(
        build(mesh.shape["gx"], mesh.shape["gy"]),
        mesh=mesh,
        in_specs=(P(None, None, "gx", "gy"), P(), P()),
        out_specs=(P(None, None, "gx", "gy"), P(None, None, "gx", "gy")),
        check_vma=False,
    )
```

```python
import functools
import math

import jax
import jax.numpy as jnp
from jax import lax
from jax.experimental import pallas as pl
from jax.experimental.pallas import tpu as pltpu
from jax.sharding import PartitionSpec as P

NX = 3072
NY = 3072
BAND = 512
STEP = 64


def angle(freq, position, length):
    phase = freq[None, :] * position[:, None] % length
    return phase.astype(jnp.float32) * (2.0 * math.pi / length)


def mode_parts(picked, first, amount, length, live=None):
    step = 64 if amount % 64 == 0 else 8
    freq = jnp.where(picked <= BAND, picked, picked - BAND)
    coarse_angle = angle(freq, first + step * jnp.arange(amount // step, dtype=jnp.int32), length)
    fine_angle = angle(freq, jnp.arange(step, dtype=jnp.int32), length)
    norm = jnp.where(picked == 0, 1.0 / math.sqrt(length), math.sqrt(2.0 / length)).astype(jnp.float32)
    if live is not None:
        norm = jnp.where(live, norm, 0.0)
    is_cos = (picked <= BAND)[None, :]
    c, s = jnp.cos(coarse_angle), jnp.sin(coarse_angle)
    first_part = jnp.where(is_cos, c, s) * norm[None, :]
    second_part = jnp.where(is_cos, -s, c) * norm[None, :]
    fc, fs = jnp.cos(fine_angle), jnp.sin(fine_angle)
    return lax.optimization_barrier((first_part, second_part, fc, fs))


def mode_table(picked, first, amount, length, live=None):
    first_part, second_part, fc, fs = mode_parts(picked, first, amount, length, live)
    table = first_part[:, None, :] * fc[None] + second_part[:, None, :] * fs[None]
    return table.astype(jnp.bfloat16).reshape(amount, picked.shape[0])


def al(v, m):
    return pl.multiple_of(v, m)


def turn(freq, position, shift, length):
    product = freq * position
    quarter = jnp.floor(product * (4.0 / length) + 0.5)
    x = (product * 4.0 - quarter * length) * (2.0 * math.pi / (4 * length))
    x2 = x * x
    s = x + x * x2 * (-1 / 6 + x2 * (1 / 120 + x2 * (-1 / 5040 + x2 * (1 / 362880))))
    c = 1.0 + x2 * (-0.5 + x2 * (1 / 24 + x2 * (-1 / 720 + x2 * (1 / 40320))))
    quarter = quarter - shift
    q = quarter - 4.0 * jnp.floor(quarter * 0.25)
    odd = (q == 1.0) | (q == 3.0)
    cos_value, sin_value = jnp.where(odd, s, c), jnp.where(odd, c, s)
    cos_value = jnp.where((q == 1.0) | (q == 2.0), -cos_value, cos_value)
    return cos_value, jnp.where(q >= 2.0, -sin_value, sin_value)


LANES = 128


def make_table(code, first, length, table, side, ta, tb, fc, fs):
    amount, codes = table.shape[0], code.shape[1]
    f32 = jnp.float32
    freq = jnp.where(code <= BAND, code, code - BAND).astype(f32)
    shift = jnp.where(code <= BAND, 0, 1).astype(f32)
    norm = jnp.where(code == 0, 1.0 / math.sqrt(length), math.sqrt(2.0 / length)).astype(f32)
    norm = jnp.where(code < 0, 0.0, norm)
    row = lax.broadcasted_iota(jnp.int32, (8, codes), 0)

    @pl.loop(0, amount // STEP // 8)
    def _(i):
        c, s = turn(freq, (first + (row + i * 8) * STEP).astype(f32), shift, length)
        ta[pl.ds(al(i * 8, 8), 8), :] = c * norm
        tb[pl.ds(al(i * 8, 8), 8), :] = s * norm

    @pl.loop(0, STEP // 8)
    def _(i):
        c, s = turn(freq, (row + i * 8).astype(f32), 0.0, length)
        fc[pl.ds(al(i * 8, 8), 8), :] = c
        fs[pl.ds(al(i * 8, 8), 8), :] = s

    @pl.loop(0, amount // STEP)
    def _(h):
        table[pl.ds(al(h * STEP, STEP), STEP), side] = (
            ta[pl.ds(h, 1), :] * fc[...] - tb[pl.ds(h, 1), :] * fs[...]
        ).astype(jnp.bfloat16)


def flipped(spot, t, lead):
    f = spot
    for bit in range(lead.bit_length()):
        if t >> bit & 1:
            f = f + (1 << bit) - (2 << bit) * lax.rem(f // (1 << bit), 2)
    return f


def near_first(lead):
    return sorted(range(lead - 1, 0, -1), key=lambda t: bin(t).count("1"))


def filter_kernel(
    lead, x_local, kx, ky, kpad,
    grid_in, xcode_in, ycode_in, spec_ref, low_ref, wide_last, y_last,
    grid_ref, xcode_ref, ycode_ref, y_raw, y_codes, y_ref, yta, ytb, yfc, yfs, own, other, inc, part, lines, turned, xt, xta, xtb, xfc, xfs,
    s_own, s_out, s_in, coarse, blocks, wide, found, far,
    gs, gr, s1, r1, s2, r2, s3, r3, s4, r4, s5, r5, s6, r6, s7, in_sem,
):
    me = lax.axis_index("gx")
    half = lax.axis_index("gy")
    peer = 1 - half
    bf, f32 = jnp.bfloat16, jnp.float32
    scope = jax.named_scope
    chunks = kpad // LANES
    members = 2 * lead
    modes = xt.shape[1]
    pieces = r2.shape[0] // chunks
    piece = modes // pieces
    rows = lead * x_local
    plane, spot = me // lead, lax.rem(me, lead)
    side = plane // 2
    base = side * members
    mine = me - base
    hub_base = base + (1 - side) * lead
    end_base = base + side * lead
    own_base = plane * lead
    is_hub = plane == 1 + side
    across = (2 - side) * lead + spot

    def grid_copy(f):
        part = pl.ds(al(f * x_local, x_local), x_local)
        return pltpu.make_async_copy(grid_in.at[part, :], grid_ref.at[part, :], in_sem.at[2 + f])

    ycode_copy = pltpu.make_async_copy(ycode_in, ycode_ref, in_sem.at[0])
    xcode_copy = pltpu.make_async_copy(xcode_in, xcode_ref, in_sem.at[1])
    ycode_copy.start()
    for f in range(lead):
        grid_copy(f).start()
    xcode_copy.start()
    barrier = pltpu.get_barrier_semaphore()
    pl.semaphore_signal(barrier, inc=1, device_id={"gy": peer})

    @pl.loop(1, members)
    def _(t):
        pl.semaphore_signal(barrier, inc=1, device_id={"gx": base + lax.rem(mine + t, members)})

    @pl.when(is_hub)
    def _():
        pl.semaphore_signal(barrier, inc=1, device_id={"gx": across})

    def mate(t):
        return flipped(spot, t, lead)

    far_first = near_first(lead)[::-1]
    last = chunks - 1

    def slot(k, i):
        return k if k < last else last + i

    def late(k):
        return pl.ds((k - chunks + 2) * 2 * LANES, 2 * LANES)

    def wide_at(k, who):
        if k >= chunks - 2:
            return wide_last, pl.ds(al((2 * (k - chunks + 2) + who) * LANES, LANES), LANES)
        return wide.at[k], span(who, LANES)

    def wide_row(k, f, who):
        ref, columns = wide_at(k, who)
        return ref.at[f, :, columns]

    def both_halves(k, f):
        return wide_last[f, :, late(k)] if k >= chunks - 2 else wide[k, f]

    def y_place(k):
        return (y_last, late(k)) if k >= chunks - 2 else (y_ref.at[k], slice(None))

    def y_at(k):
        ref, columns = y_place(k)
        return ref[:, columns]

    def span(i, n):
        return pl.ds(al(i * n, n), n)

    def swap(k):
        return pltpu.make_async_remote_copy(
            src_ref=other.at[k], dst_ref=inc.at[k], send_sem=gs, recv_sem=gr.at[k], device_id={"gy": peer})

    def up(k, f):
        return pltpu.make_async_remote_copy(
            src_ref=part.at[k, span(f, x_local), :], dst_ref=lines.at[k, span(mine, x_local), :],
            send_sem=s1, recv_sem=r1.at[k], device_id={"gx": hub_base + f})

    def up_in(k):
        taken = lines.at[k, pl.ds(0, (members - 1) * x_local), :]
        return pltpu.make_async_remote_copy(
            src_ref=taken, dst_ref=taken, send_sem=s1, recv_sem=r1.at[k], device_id={"gx": hub_base})

    def sent(view, sem):
        pltpu.make_async_remote_copy(
            src_ref=view, dst_ref=view, send_sem=sem, recv_sem=gr.at[0], device_id={"gy": peer}).wait_send()

    def cross(k, m):
        return pltpu.make_async_remote_copy(
            src_ref=s_out.at[k, span(m, piece), :], dst_ref=s_in.at[k, span(m, piece), :],
            send_sem=s2, recv_sem=r2.at[k * pieces + m], device_id={"gx": across})

    def relay(k, m):
        view = coarse.at[k, span(m, piece), :]
        return pltpu.make_async_remote_copy(
            src_ref=view, dst_ref=view, send_sem=s5, recv_sem=r5.at[slot(k, m)],
            device_id={"gx": end_base + spot})

    def down(k, f):
        return pltpu.make_async_remote_copy(
            src_ref=blocks.at[k, f], dst_ref=wide_row(k, spot, half),
            send_sem=s3, recv_sem=r3.at[slot(k, spot)], device_id={"gx": own_base + f})

    def show(k, f):
        return pltpu.make_async_remote_copy(
            src_ref=coarse.at[k, span(own_base + f, kx), :], dst_ref=found.at[k, spot],
            send_sem=s6, recv_sem=r6.at[k], device_id={"gx": own_base + f})

    def show_in(k):
        view = found.at[k, pl.ds(0, lead - 1)]
        return pltpu.make_async_remote_copy(
            src_ref=view, dst_ref=view, send_sem=s6, recv_sem=r6.at[k], device_id={"gx": own_base})

    def down_in(k, f):
        return pltpu.make_async_remote_copy(
            src_ref=blocks.at[k, 0], dst_ref=wide_row(k, f, half),
            send_sem=s3, recv_sem=r3.at[slot(k, f)], device_id={"gx": own_base + f})

    def all_down(k):
        ref, columns = wide_at(k, half)
        view = ref.at[pl.ds(0, lead - 1), :, columns]
        return pltpu.make_async_remote_copy(
            src_ref=view, dst_ref=view, send_sem=s3, recv_sem=r3.at[k], device_id={"gx": own_base})

    def all_forward(k, who):
        ref, columns = wide_at(k, who)
        place = ref.at[:, :, columns]
        return pltpu.make_async_remote_copy(
            src_ref=place, dst_ref=place, send_sem=s4, recv_sem=r4.at[k], device_id={"gy": peer})

    def all_relayed(k):
        view = coarse.at[k]
        return pltpu.make_async_remote_copy(
            src_ref=view, dst_ref=view, send_sem=s5, recv_sem=r5.at[k], device_id={"gx": hub_base})

    def forward(k, f, who):
        place = wide_row(k, f, who)
        return pltpu.make_async_remote_copy(
            src_ref=place, dst_ref=place, send_sem=s4, recv_sem=r4.at[slot(k, f)],
            device_id={"gy": peer})

    def local(f):
        return is_hub & (f == spot)

    width = chunks * LANES * 2
    y_raw[...] = jnp.full(y_raw.shape, -1, jnp.int32)
    with scope("codewait"):
        ycode_copy.wait()
    y_raw[:, : 2 * ky] = ycode_ref[...]
    first_half = jnp.broadcast_to(y_raw[...], (8, width))
    second_half = pltpu.roll(first_half, width - ky, 1)
    live = lax.broadcasted_iota(jnp.int32, (8, width), 1) < ky
    first_half = jnp.where(live, first_half, -1)
    second_half = jnp.where(live, second_half, -1)
    for k in range(chunks):
        y_codes[k, :, :LANES] = first_half[:, k * LANES : (k + 1) * LANES]
        y_codes[k, :, LANES:] = second_half[:, k * LANES : (k + 1) * LANES]

    def y_table(k):
        with scope("ytab"):
            make_table(y_codes[k, :1, :], half * grid_ref.shape[1], NY, *y_place(k), yta, ytb, yfc, yfs)

    def field_sums(k, part):
        both = jnp.dot(grid_ref[part, :], y_at(k), preferred_element_type=f32)
        low_part, high_part = both[:, :LANES], both[:, LANES:]
        other[k, part, :] = jnp.where(half == 0, high_part, low_part).astype(bf)
        own[k, part, :] = jnp.where(half == 0, low_part, high_part)

    def sums(k):
        if k == 0:
            @pl.loop(0, lead)
            def _(f):
                with scope("gridwait"):
                    grid_copy(f).wait()
                with scope("dotA"):
                    field_sums(k, span(f, x_local))
        else:
            with scope("dotA"):
                field_sums(k, pl.ds(0, rows))
        if k == 0:
            with scope("barrier"):
                pl.semaphore_wait(barrier, members + jnp.where(is_hub, 1, 0))
        swap(k).start()

    def rise(k):
        with scope("swapwait"):
            swap(k).wait_recv()
        part[k] = (own[k] + inc[k].astype(f32)).astype(bf)

        for t in far_first:
            up(k, mate(t)).start()

        @pl.when(jnp.logical_not(is_hub))
        def _():
            up(k, spot).start()

        @pl.when(is_hub)
        def _():
            lines[k, span(mine, x_local), :] = part[k, span(spot, x_local), :]

    def gather(k):
        with scope("upwait"):
            up_in(k).wait_recv()

        with scope("dotB"):
            turned[...] = lines[k].T

    def partial_sum(k, m, held=1):
        with scope("dotB"):
            got = jnp.dot(turned[...], xt[:, pl.ds(m * piece, piece)], preferred_element_type=f32).T
            s_own[k, pl.ds(m * piece, piece), :] = got
            s_out[k, pl.ds(m * piece, piece), :] = got.astype(bf)

        @pl.when(half <= held)
        def _():
            cross(k, m).start()

    mine_x = span(plane - 2 * side, rows)

    def share(k):
        for t in far_first:
            show(k, mate(t)).start()
        found[k, spot] = coarse[k, span(me, kx), :]

    far_plane = 3 * side
    far_x = span(far_plane - 2 * side, rows)

    def throw(f):
        return pltpu.make_async_remote_copy(
            src_ref=far.at[f], dst_ref=wide_row(last, spot, half),
            send_sem=s7.at[0], recv_sem=r3.at[slot(last, spot)], device_id={"gx": far_plane * lead + f})

    def throw_modes():
        for t in far_first + [0]:
            f = mate(t)
            pltpu.make_async_remote_copy(
                src_ref=coarse.at[last, span(far_plane * lead + f, kx), :], dst_ref=found.at[last, spot],
                send_sem=s7.at[1], recv_sem=r6.at[last], device_id={"gx": far_plane * lead + f}).start()

    def absorb_far(m):
        if m < pieces - 1:
            @pl.when(far_plane == m)
            def _():
                throw_modes()

        with scope("dotF"):
            got = jnp.dot(
                xt[far_x, pl.ds(m * piece, piece)], coarse[last, pl.ds(m * piece, piece), :],
                preferred_element_type=f32)
            if m < pieces - 1:
                own[1] = got if m == 0 else own[1] + got
            else:
                far[...] = (own[1] + got).astype(bf).reshape(lead, x_local, LANES)
                for t in far_first + [0]:
                    throw(mate(t)).start()

                @pl.when(far_plane == m)
                def _():
                    throw_modes()

    def absorb(k, m):
        if m < pieces - 1:
            @pl.when(plane == m)
            def _():
                share(k)

        if k == chunks - 1:
            with scope("dotC"):
                got = jnp.dot(
                    xt[mine_x, pl.ds(m * piece, piece)], coarse[k, pl.ds(m * piece, piece), :],
                    preferred_element_type=f32)
                own[0] = got if m == 0 else own[0] + got

    def meet(k, m):
        with scope("crosswait"):
            cross(k, m).wait_recv()
        part_of = pl.ds(m * piece, piece)
        coarse[k, part_of, :] = (s_own[k, part_of, :] + s_in[k, part_of, :].astype(f32)).astype(bf)
        if k < last:
            relay(k, m).start()
        else:
            @pl.when(half == 0)
            def _():
                relay(k, m).start()

            @pl.when(half == 1)
            def _():
                absorb_far(m)

        absorb(k, m)

    def receive(k):
        if k < last:
            with scope("relaywait"):
                all_relayed(k).wait_recv()
        for m in range(pieces):
            if k == last:
                with scope("relaywait"):
                    relay(k, m).wait_recv()
            absorb(k, m)

    def synthesis(k):
        if k < chunks - 1:
            with scope("dotC"):
                syn = jnp.dot(xt[mine_x, :], coarse[k], preferred_element_type=f32)
        else:
            syn = own[0]
        blocks[k] = syn.astype(bf).reshape(lead, x_local, LANES)

        for t in far_first:
            down(k, mate(t)).start()

        ref, columns = wide_at(k, half)
        ref[spot, :, columns] = blocks[k, spot]

        @pl.when(plane == pieces - 1)
        def _():
            share(k)

    def reveal(k):
        with scope("showwait"):
            show_in(k).wait_recv()
        write_modes(k)

    def write_modes(k):
        columns = min(LANES, ky - k * LANES)
        spec_ref[:, pl.ds(k * LANES, columns)] = (
            found[k].reshape(lead * kx, LANES)[:, :columns].astype(f32))

    def add_field(k, f):
        with scope("dotD"):
            got = lax.dot_general(
                both_halves(k, f), y_at(k), (((1,), (1,)), ((), ())), preferred_element_type=f32)
            if k > 0:
                got = got + low_ref[span(f, x_local), :]
            low_ref[span(f, x_local), :] = got

    def take(k):
        with scope("downwait"):
            all_down(k).wait_recv()
        all_forward(k, half).start()
        reveal(k)

    def expand(k):
        with scope("fwdwait"):
            all_forward(k, peer).wait_recv()

        if k == last - 1:
            add_field(k, spot)
            return

        @pl.loop(0, lead)
        def _(f):
            add_field(k, f)

    def own_first():
        with scope("fwdwait"):
            forward(last, spot, peer).wait_recv()
        add_field(last, spot)

    def pass_on(t):
        with scope("downwait"):
            down_in(last, mate(t)).wait_recv()
        forward(last, mate(t), half).start()

    def others():
        with scope("fwdwait"):
            for t in reversed(far_first):
                forward(last, mate(t), peer).wait_recv()

    def finish():
        @pl.when(half == 0)
        def _():
            for t in reversed(far_first):
                pass_on(t)
            own_first()

        @pl.when(half == 1)
        def _():
            own_first()
            for t in reversed(far_first):
                pass_on(t)

        reveal(last)
        others()

    y_table(0)
    sums(0)
    y_table(1)

    @pl.when(half == 0)
    def _():
        rise(0)

    sums(1)
    y_table(2)
    y_table(3)

    @pl.when(half == 1)
    def _():
        rise(0)

    def x_table():
        with scope("xtab"):
            xcode_copy.wait()
            make_table(xcode_ref[...], side * xt.shape[0], NX, xt, slice(None), xta, xtb, xfc, xfs)

    @pl.when(is_hub)
    def _():
        x_table()
        rise(1)
        sums(2)

        @pl.when(half == 1)
        def _():
            sums(3)

        rise(2)
        gather(0)
        for m in range(pieces):
            partial_sum(0, m)

        @pl.when(half == 0)
        def _():
            sums(3)

        rise(3)
        for k in range(chunks):
            more = k + 1 < chunks
            held = 0 if k + 2 == chunks else 1
            meet(k, 0)
            if k == 0:
                @pl.when(half == 0)
                def _():
                    meet(0, 1)

            if more:
                gather(k + 1)
                for m in range(pieces // 2):
                    partial_sum(k + 1, m, held)
            if k == 0:
                @pl.when(half == 1)
                def _():
                    meet(0, 1)
            else:
                meet(k, 1)
            if more:
                for m in range(pieces // 2, pieces):
                    partial_sum(k + 1, m, held)
            for m in range(2, pieces):
                meet(k, m)
            synthesis(k)
            if k == chunks - 2:
                @pl.when(half == 1)
                def _():
                    @pl.loop(0, pieces)
                    def _(m):
                        cross(chunks - 1, m).start()

            if k == chunks - 2:
                for early in range(chunks - 2):
                    take(early)

                @pl.when(half == 1)
                def _():
                    expand(0)

        forward(chunks - 1, spot, half).start()

        @pl.when(half == 0)
        def _():
            for k in range(chunks - 2):
                expand(k)

        take(chunks - 2)

        @pl.when(half == 1)
        def _():
            for k in range(1, chunks - 2):
                expand(k)

        expand(chunks - 2)
        finish()

    @pl.when(jnp.logical_not(is_hub))
    def _():
        sums(2)
        sums(3)
        rise(1)
        rise(2)
        rise(3)
        x_table()
        for k in range(last):
            receive(k)
            synthesis(k)
            if k > 0:
                take(k - 1)
                if k < last - 1:
                    expand(k - 1)

        @pl.when(half == 1)
        def _():
            expand(last - 2)

        @pl.when(half == 0)
        def _():
            for m in range(pieces):
                with scope("relaywait"):
                    relay(last, m).wait_recv()
                absorb(last, m)
                if m == 0:
                    with scope("fwdwait"):
                        all_forward(last - 2, peer).wait_recv()
                if m < pieces - 1:
                    for f in range(m, min(m + 1, lead)):
                        add_field(last - 2, f)
            synthesis(last)
            forward(last, spot, half).start()
            for f in range(pieces - 1, lead):
                add_field(last - 2, f)

        take(last - 1)
        @pl.when(half == 0)
        def _():
            expand(last - 1)
            for t in reversed(far_first):
                pass_on(t)
            own_first()
            reveal(last)

        @pl.when(half == 1)
        def _():
            for t in [0] + far_first[::-1]:
                pass_on(t)
            expand(last - 1)
            own_first()
            all_found = found.at[last]
            with scope("showwait"):
                pltpu.make_async_remote_copy(
                    src_ref=all_found, dst_ref=all_found, send_sem=s6, recv_sem=r6.at[last],
                    device_id={"gx": own_base}).wait_recv()
            write_modes(last)

        others()

    with scope("drain"):
        sent(other, gs)
        sent(wide.at[:, :, :, pl.ds(0, LANES)], s4)
        sent(wide_last.at[:, :, pl.ds(0, 2 * LANES)], s4)

        @pl.when(is_hub)
        def _():
            sent(part.at[:, pl.ds(0, rows - x_local), :], s1)
            sent(s_out, s2)
            sent(found.at[:, pl.ds(0, lead - 1)], s6)
            sent(blocks.at[:, pl.ds(0, lead - 1)], s3)

            @pl.when(half == 0)
            def _():
                sent(coarse, s5)

            @pl.when(half == 1)
            def _():
                sent(coarse.at[pl.ds(0, last)], s5)
                sent(far, s7.at[0])
                sent(found.at[last], s7.at[1])

        @pl.when(jnp.logical_not(is_hub))
        def _():
            sent(part, s1)

            @pl.when(half == 0)
            def _():
                sent(found.at[:, pl.ds(0, lead - 1)], s6)
                sent(blocks.at[:, pl.ds(0, lead - 1)], s3)

            @pl.when(half == 1)
            def _():
                sent(found.at[pl.ds(0, last), pl.ds(0, lead - 1)], s6)
                sent(blocks.at[pl.ds(0, last), pl.ds(0, lead - 1)], s3)


def spectral_filter(lead, x_local, kx, ky, kpad, *operands):
    bf, f32 = jnp.bfloat16, jnp.float32
    operands = [pltpu.with_memory_space_constraint(a, pltpu.HBM) for a in operands]
    grid, x_codes, y_codes = operands
    y_local = grid.shape[1]
    rows, members, modes = lead * x_local, 2 * lead, x_codes.shape[1]
    chunks, pieces = kpad // LANES, 4
    tall_x, tall_y = members * x_local // STEP, y_local // STEP
    dma = pltpu.SemaphoreType.DMA
    vmem = pl.BlockSpec(memory_space=pltpu.VMEM)
    return pl.pallas_call(
        functools.partial(filter_kernel, lead, x_local, kx, ky, kpad),
        out_shape=(
            jax.ShapeDtypeStruct((lead * kx, ky), f32),
            jax.ShapeDtypeStruct((rows, y_local), f32),
            jax.ShapeDtypeStruct((lead, x_local, 4 * LANES), bf),
            jax.ShapeDtypeStruct((y_local, 4 * LANES), bf),
        ),
        in_specs=[pl.BlockSpec(memory_space=pltpu.HBM)] * 3,
        out_specs=(vmem,) * 4,
        scratch_shapes=[
            pltpu.VMEM((rows, y_local), bf),
            pltpu.VMEM(x_codes.shape, jnp.int32),
            pltpu.VMEM(y_codes.shape, jnp.int32),
            pltpu.VMEM((1, 2 * kpad), jnp.int32),
            pltpu.VMEM((chunks, 8, 2 * LANES), jnp.int32),
            pltpu.VMEM((chunks - 2, y_local, 2 * LANES), bf),
            pltpu.VMEM((tall_y, 2 * LANES), f32),
            pltpu.VMEM((tall_y, 2 * LANES), f32),
            pltpu.VMEM((STEP, 2 * LANES), f32),
            pltpu.VMEM((STEP, 2 * LANES), f32),
            pltpu.VMEM((chunks, rows, LANES), f32),
            pltpu.VMEM((chunks, rows, LANES), bf),
            pltpu.VMEM((chunks, rows, LANES), bf),
            pltpu.VMEM((chunks, rows, LANES), bf),
            pltpu.VMEM((chunks, members * x_local, LANES), bf),
            pltpu.VMEM((LANES, members * x_local), bf),
            pltpu.VMEM((members * x_local, modes), bf),
            pltpu.VMEM((tall_x, modes), f32),
            pltpu.VMEM((tall_x, modes), f32),
            pltpu.VMEM((STEP, modes), f32),
            pltpu.VMEM((STEP, modes), f32),
            pltpu.VMEM((chunks, modes, LANES), f32),
            pltpu.VMEM((chunks, modes, LANES), bf),
            pltpu.VMEM((chunks, modes, LANES), bf),
            pltpu.VMEM((chunks, modes, LANES), bf),
            pltpu.VMEM((chunks, lead, x_local, LANES), bf),
            pltpu.VMEM((chunks - 2, lead, x_local, 2 * LANES), bf),
            pltpu.VMEM((chunks, lead, kx, LANES), bf),
            pltpu.VMEM((lead, x_local, LANES), bf),
            dma, dma((chunks,)),
            dma, dma((chunks,)),
            dma, dma((chunks * pieces,)),
            dma, dma((chunks - 1 + lead,)),
            dma, dma((chunks - 1 + lead,)),
            dma, dma((chunks - 1 + pieces,)),
            dma, dma((chunks,)),
            dma((2,)),
            dma((2 + lead,)),
        ],
        compiler_params=pltpu.CompilerParams(
            collective_id=0, has_side_effects=True, vmem_limit_bytes=44 * 1024 * 1024
        ),
    )(*operands)


def last_sum_kernel(order, spec_in, low_in, wide_in, y_in, spec_out, low_out, total, sem):
    lead, x_local, _ = wide_in.shape
    spot = lax.rem(lax.axis_index("gx"), lead)
    spec_copy = pltpu.make_async_copy(spec_in, spec_out, sem.at[lead])

    def field(source, t):
        part = pl.ds(al(flipped(spot, t, lead) * x_local, x_local), x_local)
        return pltpu.make_async_copy(source.at[part, :], low_out.at[part, :], sem.at[t])

    field(low_in, 0).start()
    spec_copy.start()
    for t in order:
        f = flipped(spot, t, lead)
        part = pl.ds(al(f * x_local, x_local), x_local)
        total[part, :] = low_in[part, :] + lax.dot_general(
            wide_in[f], y_in[...], (((1,), (1,)), ((), ())), preferred_element_type=jnp.float32)
        field(total, t).start()
    field(low_in, 0).wait()
    for t in order:
        field(total, t).wait()
    spec_copy.wait()


def last_sum(spec, low, wide, y_table):
    lead = wide.shape[0]
    vmem, anywhere = pl.BlockSpec(memory_space=pltpu.VMEM), pl.BlockSpec(memory_space=pl.ANY)
    return pl.pallas_call(
        functools.partial(last_sum_kernel, near_first(lead)),
        out_shape=(jax.ShapeDtypeStruct(spec.shape, spec.dtype), jax.ShapeDtypeStruct(low.shape, low.dtype)),
        in_specs=[vmem] * 4,
        out_specs=(anywhere, anywhere),
        scratch_shapes=[pltpu.VMEM(low.shape, low.dtype), pltpu.SemaphoreType.DMA((lead + 1,))],
        compiler_params=pltpu.CompilerParams(vmem_limit_bytes=12 * 1024 * 1024),
    )(spec, low, wide, y_table)


def build(gx, gy):
    def local(fields, x_codes, y_codes):
        nf, nz, x_local, y_local = fields.shape
        lead = nf * nz
        ky = y_codes.shape[0] // gy
        kx = x_codes.shape[0] // gx
        unit = 128 * gx // math.gcd(128 * gx, lead)
        if unit > 2 * ky:
            unit = gx // math.gcd(gx, lead)
        kpad = -(-ky // unit) * unit
        cols = lead * kpad // gx
        me_y = lax.axis_index("gy")
        y_first = me_y * y_local
        grid = fields.reshape(lead * x_local, y_local)
        fits = gy == 2 and gx == 4 * lead and lead & (lead - 1) == 0 and kpad == 4 * LANES and kx % 16 == 0
        fits = fits and x_local % 16 == 0 and 2 * lead * x_local % (8 * STEP) == 0
        fits = fits and y_local % (8 * STEP) == 0 and gx * kx % (4 * LANES) == 0
        if fits:
            spec, low = last_sum(*spectral_filter(
                lead, x_local, kx, ky, kpad, grid, x_codes.reshape(1, -1), y_codes.reshape(1, -1)))
            return spec.reshape(nf, nz, kx, ky), low.reshape(nf, nz, x_local, y_local)
        padded = jnp.pad(y_codes.reshape(gy, ky), ((0, 0), (0, kpad - ky)))
        live = jnp.broadcast_to(jnp.arange(kpad)[None] < ky, (gy, kpad)).reshape(-1)
        x_tab = mode_table(x_codes, 0, x_local * gx, NX)
        y_tab = mode_table(padded.reshape(-1), y_first, y_local, NY, live)
        part = jnp.dot(grid, y_tab, preferred_element_type=jnp.float32).reshape(lead * x_local, gy, kpad)
        own = lax.dynamic_index_in_dim(part, me_y, 1, keepdims=False)
        for shift in range(1, gy):
            there = lax.rem(me_y + shift, gy)
            block = lax.dynamic_index_in_dim(part, there, 1, keepdims=False).astype(jnp.bfloat16)
            got = lax.ppermute(block, "gy", [(i, (i + shift) % gy) for i in range(gy)])
            own = own + got.astype(jnp.float32)
        send = own.astype(jnp.bfloat16).reshape(lead, x_local, kpad)
        if cols <= kpad:
            def spread(a):
                n = a.shape[1]
                return a.reshape(lead, n, kpad // cols, cols).transpose(0, 2, 1, 3).reshape(gx, n, cols)

            def merge(a):
                n = a.shape[1]
                return a.reshape(lead, kpad // cols, n, cols).transpose(0, 2, 1, 3).reshape(lead, n, kpad)
        else:
            def spread(a):
                n = a.shape[1]
                return a.transpose(1, 0, 2).reshape(n, gx, cols).transpose(1, 0, 2)

            def merge(a):
                n = a.shape[1]
                return a.transpose(1, 0, 2).reshape(n, lead, kpad).transpose(1, 0, 2)
        lines = lax.all_to_all(spread(send), "gx", split_axis=0, concat_axis=0, tiled=True)
        lines = lines.reshape(gx * x_local, cols)
        modes = lax.dot_general(x_tab, lines, (((0,), (0,)), ((), ())), preferred_element_type=jnp.float32)
        coarse = modes.astype(jnp.bfloat16)
        synth = jnp.dot(x_tab, coarse, preferred_element_type=jnp.float32).astype(jnp.bfloat16)
        back = lax.all_to_all(synth.reshape(gx, x_local, cols), "gx", split_axis=0, concat_axis=0, tiled=True)
        spec = lax.all_to_all(coarse.reshape(gx, kx, cols), "gx", split_axis=0, concat_axis=0, tiled=True)
        spectrum = merge(spec)[:, :, :ky].astype(jnp.float32).reshape(nf, nz, kx, ky)
        mine = merge(back).reshape(lead * x_local, kpad)
        y_parts = y_tab.reshape(y_local, gy, kpad)
        whole = jnp.zeros((gy, lead * x_local, kpad), jnp.bfloat16)
        whole = lax.dynamic_update_index_in_dim(whole, mine, me_y, 0)
        for shift in range(1, gy):
            got = lax.ppermute(mine, "gy", [(i, (i + shift) % gy) for i in range(gy)])
            whole = lax.dynamic_update_index_in_dim(whole, got, lax.rem(me_y + gy - shift, gy), 0)
        wide = whole.transpose(1, 0, 2).reshape(lead * x_local, gy * kpad)
        low = lax.dot_general(wide, y_tab, (((1,), (1,)), ((), ())), preferred_element_type=jnp.float32)
        return spectrum, low.reshape(nf, nz, x_local, y_local)

    return local


def solution(mesh):
    return jax.shard_map(
        build(mesh.shape["gx"], mesh.shape["gy"]),
        mesh=mesh,
        in_specs=(P(None, None, "gx", "gy"), P(), P()),
        out_specs=(P(None, None, "gx", "gy"), P(None, None, "gx", "gy")),
        check_vma=False,
    )
```
